128 devices in a mesh: dp: 1, tp: 2 (over core), ep: 64 (over z, y, x).
Axes of the slice: x: 4, y: 4, z: 4, core: 2. Of those that a mesh axis runs over, the one named last changes fastest.
Arguments:
- hidden_in: bfloat16 [2048, 2048], P(('dp', 'ep'))
- positions: int32 [2048], P(('dp', 'ep'))
- expert_ids: int32 [2048, 2], P(('dp', 'ep'))
- k_cache: bfloat16 [2048, 32, 4, 128], P(('dp', 'ep'), None, 'tp')
- v_cache: bfloat16 [2048, 32, 4, 128], P(('dp', 'ep'), None, 'tp')
- norm_in: bfloat16 [2048], replicated
- norm_res: bfloat16 [2048], replicated
- norm_post: bfloat16 [2048], replicated
- w_q: bfloat16 [2048, 4096], P(None, 'tp')
- w_k: bfloat16 [2048, 512], P(None, 'tp')
- w_v: bfloat16 [2048, 512], P(None, 'tp')
- w_o: bfloat16 [4096, 2048], P('tp')
- w_gate: bfloat16 [2048, 6144], P(None, 'tp')
- w_up: bfloat16 [2048, 6144], P(None, 'tp')
- w_down: bfloat16 [6144, 2048], P('tp')
- w_router: bfloat16 [2048, 128], replicated
- e_gate: bfloat16 [128, 2048, 768], P('ep', None, 'tp')
- e_up: bfloat16 [128, 2048, 768], P('ep', None, 'tp')
- e_down: bfloat16 [128, 768, 2048], P('ep', 'tp')
Outputs:
- output 1: bfloat16 [2048, 2048], P(('dp', 'ep'))
- output 2: bfloat16 [2048, 32, 4, 128], P(('dp', 'ep'), None, 'tp')
- output 3: bfloat16 [2048, 32, 4, 128], P(('dp', 'ep'), None, 'tp')
All inputs are finite; a program needn't handle non-finite values.
Results may differ from the reference program's by a relative error of at most 0.0124179.
Values are sent between devices in bfloat16 or wider.
A program may use at most 1 GiB of HBM per device.

```python
import jax
import jax.numpy as jnp
from jax import lax

TOKENS = 32
EP_SHARDS = 64
CACHE_LEN = 32
MODEL_DIM = 2048
Q_HEADS = 32
KV_HEADS = 4
HEAD_DIM = 128
DENSE_FF = 6144
EXPERTS = 128
EXPERT_FF = 768
ROPE_BASE = 10000
BATCH = TOKENS * EP_SHARDS
NORM_EPS = 1e-5


def draw_routes(route_key):
    mean_count = 2 * TOKENS // EP_SHARDS
    local_count = EXPERTS // EP_SHARDS
    sub_keys = jax.random.split(route_key, 5)
    shard_perm = jax.random.permutation(sub_keys[0], EP_SHARDS)
    lift_count = jax.random.randint(sub_keys[1], (EP_SHARDS, EP_SHARDS // 2), 0, mean_count + 1)
    lift_count = lift_count.at[0, 0].set(mean_count)
    paired = jnp.stack([lift_count, -lift_count], axis=-1).reshape(EP_SHARDS, EP_SHARDS)
    counts = mean_count + paired[:, jnp.argsort(shard_perm)]
    bounds = jnp.cumsum(counts, axis=1)
    slot_ids = jnp.arange(2 * TOKENS)
    dest_sorted = jnp.sum((bounds[:, None, :] <= slot_ids[None, :, None]).astype(jnp.int32), axis=2)

    def shuffle_tokens(sub_key):
        return jax.random.permutation(sub_key, TOKENS)

    token_perm = jax.vmap(shuffle_tokens)(jax.random.split(sub_keys[2], EP_SHARDS))
    first_dest = jnp.take_along_axis(dest_sorted, token_perm, axis=1)
    second_dest = jnp.take_along_axis(dest_sorted, token_perm + TOKENS, axis=1)
    swap_flag = jax.random.randint(sub_keys[3], (EP_SHARDS, TOKENS), 0, 2) == 1
    dest_pair = jnp.stack([jnp.where(swap_flag, second_dest, first_dest), jnp.where(swap_flag, first_dest, second_dest)], axis=-1)
    within = jax.random.randint(sub_keys[4], (EP_SHARDS, TOKENS, 2), 0, local_count)
    return (dest_pair * local_count + within).reshape(BATCH, 2).astype(jnp.int32)


def draw_matrix(sub_key, mat_shape, fan_in, factor):
    return (jax.random.normal(sub_key, mat_shape, jnp.float32) * (factor * fan_in ** -0.5)).astype(jnp.bfloat16)


def draw_expert_stack(stack_key, fan_in, fan_out):
    def one_expert(sub_key):
        return draw_matrix(sub_key, (fan_in, fan_out), fan_in, 1.0)
    return lax.map(one_expert, jax.random.split(stack_key, EXPERTS))


def draw_gain(sub_key):
    return jax.random.uniform(sub_key, (MODEL_DIM,), jnp.float32, 0.5, 1.5).astype(jnp.bfloat16)


def setup_inputs(seed: int = 0, part: int = 0) -> dict:
    part_key = jax.random.fold_in(jax.random.key(seed), part)
    part_keys = jax.random.split(part_key, 5)
    weight_keys = jax.random.split(jax.random.key(seed + 1), 15)
    attn_width = Q_HEADS * HEAD_DIM
    kv_width = KV_HEADS * HEAD_DIM
    cache_shape = (BATCH, CACHE_LEN, KV_HEADS, HEAD_DIM)
    return {
        'hidden_in': jax.random.normal(part_keys[0], (BATCH, MODEL_DIM), jnp.float32).astype(jnp.bfloat16),
        'positions': jax.random.randint(part_keys[1], (BATCH,), CACHE_LEN // 2, CACHE_LEN).at[0].set(CACHE_LEN - 1).astype(jnp.int32),
        'expert_ids': draw_routes(part_keys[2]),
        'k_cache': jax.random.normal(part_keys[3], cache_shape, jnp.float32).astype(jnp.bfloat16),
        'v_cache': jax.random.normal(part_keys[4], cache_shape, jnp.float32).astype(jnp.bfloat16),
        'norm_in': draw_gain(weight_keys[0]),
        'norm_res': draw_gain(weight_keys[1]),
        'norm_post': draw_gain(weight_keys[2]),
        'w_q': draw_matrix(weight_keys[3], (MODEL_DIM, attn_width), MODEL_DIM, 1.0),
        'w_k': draw_matrix(weight_keys[4], (MODEL_DIM, kv_width), MODEL_DIM, 1.0),
        'w_v': draw_matrix(weight_keys[5], (MODEL_DIM, kv_width), MODEL_DIM, 1.0),
        'w_o': draw_matrix(weight_keys[6], (attn_width, MODEL_DIM), attn_width, 0.5 * CACHE_LEN ** 0.5),
        'w_gate': draw_matrix(weight_keys[7], (MODEL_DIM, DENSE_FF), MODEL_DIM, 1.0),
        'w_up': draw_matrix(weight_keys[8], (MODEL_DIM, DENSE_FF), MODEL_DIM, 1.0),
        'w_down': draw_matrix(weight_keys[9], (DENSE_FF, MODEL_DIM), DENSE_FF, 1.0),
        'w_router': draw_matrix(weight_keys[10], (MODEL_DIM, EXPERTS), MODEL_DIM, 1.0),
        'e_gate': draw_expert_stack(weight_keys[11], MODEL_DIM, EXPERT_FF),
        'e_up': draw_expert_stack(weight_keys[12], MODEL_DIM, EXPERT_FF),
        'e_down': draw_expert_stack(weight_keys[13], EXPERT_FF, MODEL_DIM),
    }


def rms_norm(values, gain_vec):
    wide_vals = values.astype(jnp.float32)
    inv_rms = lax.rsqrt(jnp.mean(wide_vals * wide_vals, axis=-1, keepdims=True) + NORM_EPS)
    return (wide_vals * inv_rms * gain_vec.astype(jnp.float32)).astype(jnp.bfloat16)


def rope_rotate(values, positions):
    half_dim = HEAD_DIM // 2
    inv_freq = 1.0 / (ROPE_BASE ** (jnp.arange(0, HEAD_DIM, 2, dtype=jnp.float32) / HEAD_DIM))
    angles = positions.astype(jnp.float32)[:, None] * inv_freq[None, :]
    cosine = jnp.cos(angles)[:, None, :]
    sine_part = jnp.sin(angles)[:, None, :]
    first_half = values[..., :half_dim]
    second_half = values[..., half_dim:]
    return jnp.concatenate([first_half * cosine - second_half * sine_part, second_half * cosine + first_half * sine_part], axis=-1)


def reference(hidden_in, positions, expert_ids, k_cache, v_cache, norm_in, norm_res, norm_post, w_q, w_k, w_v, w_o, w_gate, w_up, w_down, w_router, e_gate, e_up, e_down):
    group_size = Q_HEADS // KV_HEADS
    normed = rms_norm(hidden_in, norm_in)
    q_proj = jnp.dot(normed, w_q, preferred_element_type=jnp.float32).reshape(BATCH, Q_HEADS, HEAD_DIM)
    k_proj = jnp.dot(normed, w_k, preferred_element_type=jnp.float32).reshape(BATCH, KV_HEADS, HEAD_DIM)
    v_new = jnp.dot(normed, w_v, preferred_element_type=jnp.float32).astype(jnp.bfloat16).reshape(BATCH, KV_HEADS, HEAD_DIM)
    q_rot = rope_rotate(q_proj, positions).astype(jnp.bfloat16)
    k_rot = rope_rotate(k_proj, positions).astype(jnp.bfloat16)
    slot_hit = (jnp.arange(CACHE_LEN)[None, :] == positions[:, None])[:, :, None, None]
    k_out = jnp.where(slot_hit, k_rot[:, None], k_cache)
    v_out = jnp.where(slot_hit, v_new[:, None], v_cache)

    def attend_token(operands):
        q_tok, k_tok, v_tok, pos_tok = operands
        q_grp = q_tok.reshape(KV_HEADS, group_size, HEAD_DIM).astype(jnp.float32)
        scores = jnp.einsum('kgd,tkd->kgt', q_grp, k_tok.astype(jnp.float32)) * (HEAD_DIM ** -0.5)
        visible = jnp.arange(CACHE_LEN)[None, None, :] <= pos_tok
        attn_probs = jax.nn.softmax(jnp.where(visible, scores, -jnp.inf), axis=-1)
        attn_probs = attn_probs.astype(jnp.bfloat16).astype(jnp.float32)
        mixed_vals = jnp.einsum('kgt,tkd->kgd', attn_probs, v_tok.astype(jnp.float32))
        return mixed_vals.astype(jnp.bfloat16).reshape(Q_HEADS * HEAD_DIM)

    attn_mix = lax.map(attend_token, (q_rot, k_out, v_out, positions))
    hidden_mid = (hidden_in.astype(jnp.float32) + jnp.dot(attn_mix, w_o, preferred_element_type=jnp.float32)).astype(jnp.bfloat16)
    res_in = rms_norm(hidden_mid, norm_res)
    gate_val = jnp.dot(res_in, w_gate, preferred_element_type=jnp.float32)
    up_val = jnp.dot(res_in, w_up, preferred_element_type=jnp.float32)
    dense_out = jnp.dot((jax.nn.silu(gate_val) * up_val).astype(jnp.bfloat16), w_down, preferred_element_type=jnp.float32)
    moe_in = rms_norm(hidden_in, norm_post)
    gate_probs = jax.nn.softmax(jnp.dot(moe_in, w_router, preferred_element_type=jnp.float32), axis=-1)
    picked = jnp.take_along_axis(gate_probs, expert_ids, axis=1)
    route_wts = picked / jnp.sum(picked, axis=1, keepdims=True)

    def expert_token(operands):
        row_vec, id_pair, wt_pair = operands
        moe_sum = jnp.zeros((MODEL_DIM,), jnp.float32)
        for choice in range(2):
            expert = id_pair[choice]
            gate_e = jnp.dot(row_vec[None, :], e_gate[expert], preferred_element_type=jnp.float32)
            up_e = jnp.dot(row_vec[None, :], e_up[expert], preferred_element_type=jnp.float32)
            act_e = (jax.nn.silu(gate_e) * up_e).astype(jnp.bfloat16)
            moe_sum = moe_sum + wt_pair[choice] * jnp.dot(act_e, e_down[expert], preferred_element_type=jnp.float32)[0]
        return moe_sum

    moe_out = lax.map(expert_token, (moe_in, expert_ids, route_wts))
    hidden_out = (hidden_mid.astype(jnp.float32) + dense_out + moe_out).astype(jnp.bfloat16)
    return (hidden_out, k_out, v_out)
```

```python
import functools
import math

import jax
import jax.numpy as jnp
from jax import lax
from jax.experimental import pallas as pl
from jax.experimental.pallas import tpu as pltpu
from jax.sharding import PartitionSpec as P

NORM_EPS = 1e-5
ROPE_BASE = 10000.0
MESH = pl.DeviceIdType.MESH
F32 = jnp.float32
BF16 = jnp.bfloat16


def iota(shape, axis):
    return lax.broadcasted_iota(jnp.int32, shape, axis)


def gain_row(ref):
    tile = ref[...].astype(F32)
    return jnp.concatenate([tile[i:i + 1, :] for i in range(tile.shape[0])], axis=1)


def inv_rms(wide):
    return lax.rsqrt(jnp.mean(wide * wide, axis=-1, keepdims=True) + NORM_EPS)


def silu_mul(gate, up):
    return ((gate * jax.nn.sigmoid(gate)) * up).astype(BF16)


def layer_kernel(dims, x_h, pos_h, ids_h, kc_h, vc_h, gin_h, gres_h, gpost_h, wq_h, wk_h, wv_h, wo_h, wg_h, wu_h, wd_h, wr_h,
                 eg_h, eu_h, ed_h, out_h, ko_h, vo_h,
                 x_v, pos_v, ids_v, kc_v, vc_v, gin_v, gres_v, gpost_v, wq_v, wk_v, wv_v, wo_v, wg_v, wu_v, wr_v,
                 eg_v, eu_v, ed_v, ko_v, vo_v, a_v, q_v, mix_v, as_v, ar_v, h_v, c_v, act_v, den_v,
                 ds_v, dr_v, rows_v, z_v, rs_v, rr_v, ret_v, fs_v, fr_v, out_v,
                 small_sem, w_sem, out_sem, tp_sem, ep_sem):
    T, D, L, KV, HD, QH, F, EL, EF, EP, CAP, TILE = dims
    group = QH // KV
    slots = EP * CAP
    me = lax.axis_index('ep')
    other = 1 - lax.axis_index('tp')

    barrier = pltpu.get_barrier_semaphore()

    def signal_peer(i, carry):
        pl.semaphore_signal(barrier, inc=1, device_id={'ep': lax.rem(me + i, EP)}, device_id_type=MESH)
        return carry

    lax.fori_loop(1, EP, signal_peer, 0)
    pl.semaphore_signal(barrier, inc=1, device_id={'tp': other}, device_id_type=MESH)

    small = [(x_h, x_v), (pos_h, pos_v), (ids_h, ids_v), (gin_h, gin_v), (gres_h, gres_v), (gpost_h, gpost_v)]
    for i, (src, dst) in enumerate(small):
        pltpu.make_async_copy(src, dst, small_sem.at[i]).start()

    def fetch(src, dst, sem, parts):
        step = dst.shape[0] // parts
        for i in range(parts):
            rows = pl.ds(i * step, step)
            pltpu.make_async_copy(src.at[rows], dst.at[rows], sem).start()

    def arrive(dst, sem):
        pltpu.make_async_copy(dst, dst, sem).wait()

    fetch(wr_h, wr_v, w_sem.at[0], 1)
    fetch(wk_h, wk_v, w_sem.at[1], 1)
    fetch(wv_h, wv_v, w_sem.at[2], 1)
    fetch(wq_h, wq_v, w_sem.at[3], 4)
    fetch(kc_h, kc_v, w_sem.at[4], 1)
    fetch(vc_h, vc_v, w_sem.at[5], 1)
    fetch(wo_h, wo_v, w_sem.at[6], 4)
    fetch(eg_h, eg_v, w_sem.at[7], EL)
    fetch(eu_h, eu_v, w_sem.at[8], EL)
    fetch(ed_h, ed_v, w_sem.at[9], EL)

    for i, (src, dst) in enumerate(small):
        pltpu.make_async_copy(src, dst, small_sem.at[i]).wait()

    wide = x_v[...].astype(F32)
    scaled = wide * inv_rms(wide)
    a_v[...] = (scaled * gain_row(gin_v)).astype(BF16)
    moe_in = (scaled * gain_row(gpost_v)).astype(BF16)

    eye = iota((T, T), 0) == iota((T, T), 1)
    before = iota((T, T), 0) < iota((T, T), 1)

    def to_col(row):
        return jnp.sum(jnp.where(eye, row, 0.0), axis=1, keepdims=True)

    ids = ids_v[...]
    pos_row = pos_v[...].astype(F32)
    pos_col = to_col(pos_row)
    id_rows = [ids[k:k + 1, :].astype(F32) for k in range(2)]
    dest_rows = [jnp.floor(r * (1.0 / EL)) for r in id_rows]
    bit_rows = [r - EL * d for r, d in zip(id_rows, dest_rows)]
    dest_cols = [to_col(d) for d in dest_rows]
    rank0 = jnp.sum(jnp.where((dest_cols[0] == dest_rows[0]) & before, 1.0, 0.0), axis=0, keepdims=True)
    rank1 = (jnp.sum(jnp.where(dest_cols[0] == dest_rows[1], 1.0, 0.0), axis=0, keepdims=True)
             + jnp.sum(jnp.where((dest_cols[1] == dest_rows[1]) & before, 1.0, 0.0), axis=0, keepdims=True))
    slot_rows = [dest_rows[0] * CAP + rank0, dest_rows[1] * CAP + rank1]
    slot_cols = [to_col(s) for s in slot_rows]
    slot_iota = iota((slots, T), 0).astype(F32)
    hot = [jnp.where(slot_iota == s, 1.0, 0.0) for s in slot_rows]
    which = jnp.sum(hot[0] * bit_rows[0] + hot[1] * bit_rows[1], axis=1, keepdims=True)
    sent = jnp.dot((hot[0] + hot[1]).astype(BF16), moe_in, preferred_element_type=F32).astype(BF16)
    ds_v[:, :, :D] = sent.reshape(EP, CAP, D)
    ds_v[:, :, D:] = jnp.broadcast_to(which, (slots, 128)).astype(BF16).reshape(EP, CAP, 128)
    dr_v[me] = ds_v[me]

    arrive(wr_v, w_sem.at[0])
    logits = jnp.dot(moe_in, wr_v[...], preferred_element_type=F32)
    expd = jnp.exp(logits - jnp.max(logits, axis=-1, keepdims=True))
    probs = expd / jnp.sum(expd, axis=-1, keepdims=True)
    lane = iota(logits.shape, 1).astype(F32)
    picked = [jnp.sum(jnp.where(lane == to_col(r), probs, 0.0), axis=1, keepdims=True) for r in id_rows]
    total = picked[0] + picked[1]
    weights = [pk / total for pk in picked]

    pl.semaphore_wait(barrier, EP)

    def send_rows(i, carry):
        peer = lax.rem(me + i, EP)
        pltpu.make_async_remote_copy(src_ref=ds_v.at[peer], dst_ref=dr_v.at[me], send_sem=ep_sem.at[0], recv_sem=ep_sem.at[1],
                                     device_id={'ep': peer}, device_id_type=MESH).start()
        return carry

    lax.fori_loop(1, EP, send_rows, 0)

    def tiled(width, body, tile=TILE):
        tile = min(tile, width)

        def step(i, carry):
            body(pl.ds(pl.multiple_of(i * tile, tile), tile))
            return carry

        lax.fori_loop(0, width // tile, step, 0)

    inv_freq = jnp.exp((iota((1, HD), 1) & (HD // 2 - 1)).astype(F32) * (-2.0 / HD * math.log(ROPE_BASE)))
    angles = pos_col * inv_freq
    cosine = jnp.cos(angles)
    sine = jnp.where(iota((1, HD), 1) < HD // 2, -1.0, 1.0) * jnp.sin(angles)

    def rope(head):
        return (head * cosine + pltpu.roll(head, HD // 2, 1) * sine).astype(BF16)

    arrive(wk_v, w_sem.at[1])
    k_proj = jnp.dot(a_v[...], wk_v[...], preferred_element_type=F32)
    k_new = jnp.concatenate([rope(k_proj[:, g * HD:(g + 1) * HD]) for g in range(KV)], axis=0)
    arrive(wv_v, w_sem.at[2])
    v_proj = jnp.dot(a_v[...], wv_v[...], preferred_element_type=F32).astype(BF16)
    v_new = jnp.concatenate([v_proj[:, g * HD:(g + 1) * HD] for g in range(KV)], axis=0)

    arrive(wq_v, w_sem.at[3])

    def q_tile(cols):
        q_v[:, cols] = jnp.dot(a_v[...], wq_v[:, cols], preferred_element_type=F32)

    tiled(QH * HD, q_tile)
    fetch(wg_h, wg_v, w_sem.at[10], 4)
    fetch(wu_h, wu_v, w_sem.at[11], 4)
    half = min(wd_h.shape[0], wq_v.shape[0])
    rest = wd_h.shape[0] - half
    pltpu.make_async_copy(wd_h.at[pl.ds(0, half)], wq_v.at[pl.ds(0, half)], w_sem.at[12]).start()

    arrive(kc_v, w_sem.at[4])
    arrive(vc_v, w_sem.at[5])
    tok_i = iota((T, KV * T), 0)
    lane_j = iota((T, KV * T), 1)
    target = jnp.sum(jnp.where(lax.rem(lane_j, T) == tok_i, (tok_i.astype(F32) * L + pos_col) * KV, 0.0), axis=0, keepdims=True)
    target = target + jnp.floor(iota((1, KV * T), 1).astype(F32) * (1.0 / T))
    new_rows = jnp.concatenate([k_new, v_new, jnp.ones((KV * T, HD), BF16)], axis=1)
    q_heads = [rope(q_v[:, h * HD:(h + 1) * HD]) for h in range(QH)]
    TC = min(16, T)
    width = TC * L * KV
    for c in range(T // TC):
        rows = pl.ds(c * width, width)
        place = jnp.where(iota((width, KV * T), 0).astype(F32) + float(c * width) == target, 1.0, 0.0).astype(BF16)
        placed = jnp.dot(place, new_rows, preferred_element_type=F32)
        hit = placed[:, 2 * HD:] > 0.5
        k_all = jnp.where(hit, placed[:, :HD], kc_v[rows, :].astype(F32)).astype(BF16)
        v_all = jnp.where(hit, placed[:, HD:2 * HD], vc_v[rows, :].astype(F32)).astype(BF16)
        ko_v[rows, :] = k_all
        vo_v[rows, :] = v_all
        q_rows = jnp.concatenate([q[c * TC:(c + 1) * TC] for q in q_heads], axis=0)
        scores = lax.dot_general(q_rows, k_all, (((1,), (1,)), ((), ())), preferred_element_type=F32) * (HD ** -0.5)
        head_kv = iota((QH * TC, 1), 0) // (group * TC)
        base = lax.rem(iota((QH * TC, 1), 0), TC) * (L * KV) + head_kv
        pos_rows = jnp.concatenate([pos_col[c * TC:(c + 1) * TC]] * QH, axis=0).astype(jnp.int32)
        last = base + KV * pos_rows
        col = iota((QH * TC, width), 1)
        visible = (col >= base) & (col <= last) & (lax.rem(col, KV) == head_kv)
        scores = jnp.where(visible, scores, -jnp.inf)
        expo = jnp.exp(scores - jnp.max(scores, axis=-1, keepdims=True))
        attn = (expo / jnp.sum(expo, axis=-1, keepdims=True)).astype(BF16)
        mixed = jnp.dot(attn, v_all, preferred_element_type=F32).astype(BF16)
        mix_v[c * TC:(c + 1) * TC, :] = jnp.concatenate([mixed[h * TC:(h + 1) * TC] for h in range(QH)], axis=1)
    cache_out = [pltpu.make_async_copy(ko_v, ko_h, out_sem.at[0]), pltpu.make_async_copy(vo_v, vo_h, out_sem.at[1])]
    for copy in cache_out:
        copy.start()

    arrive(wo_v, w_sem.at[6])

    def o_tile(cols):
        as_v[:, cols] = jnp.dot(mix_v[...], wo_v[:, cols], preferred_element_type=F32).astype(BF16)

    tiled(D, o_tile)
    if rest:
        pltpu.make_async_copy(wd_h.at[pl.ds(half, rest)], wo_v.at[pl.ds(0, rest)], w_sem.at[13]).start()
    attn_copy = pltpu.make_async_remote_copy(src_ref=as_v, dst_ref=ar_v, send_sem=tp_sem.at[0], recv_sem=tp_sem.at[1],
                                             device_id={'tp': other}, device_id_type=MESH)
    attn_copy.start()
    attn_copy.wait()
    mid = (x_v[...].astype(F32) + (as_v[...].astype(F32) + ar_v[...].astype(F32))).astype(BF16)
    h_v[...] = mid
    mid = mid.astype(F32)
    c_v[...] = (mid * inv_rms(mid) * gain_row(gres_v)).astype(BF16)

    arrive(wg_v, w_sem.at[10])
    arrive(wu_v, w_sem.at[11])

    def ff_tile(cols):
        gate = jnp.dot(c_v[...], wg_v[:, cols], preferred_element_type=F32)
        up = jnp.dot(c_v[...], wu_v[:, cols], preferred_element_type=F32)
        act_v[:, cols] = silu_mul(gate, up)

    tiled(F, ff_tile)

    arrive(eg_v, w_sem.at[7])
    arrive(eu_v, w_sem.at[8])
    arrive(ed_v, w_sem.at[9])
    others = pl.ds(0, EP - 1)
    pltpu.make_async_copy(dr_v.at[others], dr_v.at[others], ep_sem.at[1]).wait()
    rows_v[...] = dr_v[...].reshape(slots, D + 128)
    for e in range(EL):
        gate = jnp.dot(rows_v[:, :D], eg_v[e], preferred_element_type=F32)
        up = jnp.dot(rows_v[:, :D], eu_v[e], preferred_element_type=F32)
        mine = rows_v[:, D:D + 1].astype(F32) == float(e)
        z_v[:, e * EF:(e + 1) * EF] = jnp.where(mine, silu_mul(gate, up).astype(F32), 0.0).astype(BF16)

    def back_tile(cols):
        part = jnp.dot(z_v[:, :EF], ed_v[0, :, cols], preferred_element_type=F32)
        for e in range(1, EL):
            part += jnp.dot(z_v[:, e * EF:(e + 1) * EF], ed_v[e, :, cols], preferred_element_type=F32)
        rs_v[:, :, cols] = part.astype(BF16).reshape(EP, CAP, part.shape[1])

    tiled(D, back_tile)
    rr_v[me] = rs_v[me]

    def send_back(i, carry):
        peer = lax.rem(me + i, EP)
        pltpu.make_async_remote_copy(src_ref=rs_v.at[peer], dst_ref=rr_v.at[me], send_sem=ep_sem.at[2], recv_sem=ep_sem.at[3],
                                     device_id={'ep': peer}, device_id_type=MESH).start()
        return carry

    lax.fori_loop(1, EP, send_back, 0)

    arrive(wq_v.at[pl.ds(0, half)], w_sem.at[12])
    if rest:
        arrive(wo_v.at[pl.ds(0, rest)], w_sem.at[13])

    def down_tile(cols):
        part = jnp.dot(act_v[:, :half], wq_v[:half, cols], preferred_element_type=F32)
        if rest:
            part += jnp.dot(act_v[:, half:], wo_v[:rest, cols], preferred_element_type=F32)
        den_v[:, cols] = part

    tiled(D, down_tile)

    pltpu.make_async_copy(rr_v.at[others], rr_v.at[others], ep_sem.at[3]).wait()
    ret_v[...] = rr_v[...].reshape(slots, D)
    slot_lane = iota((T, slots), 1).astype(F32)
    take = [jnp.where(slot_lane == s, 1.0, 0.0).astype(BF16) for s in slot_cols]

    def sum_tile(cols):
        moe = weights[0] * jnp.dot(take[0], ret_v[:, cols], preferred_element_type=F32)
        moe += weights[1] * jnp.dot(take[1], ret_v[:, cols], preferred_element_type=F32)
        fs_v[:, cols] = (den_v[:, cols] + moe).astype(BF16)

    tiled(D, sum_tile)
    last_copy = pltpu.make_async_remote_copy(src_ref=fs_v, dst_ref=fr_v, send_sem=tp_sem.at[2], recv_sem=tp_sem.at[3],
                                             device_id={'tp': other}, device_id_type=MESH)
    last_copy.start()
    last_copy.wait()
    out_v[...] = (h_v[...].astype(F32) + (fs_v[...].astype(F32) + fr_v[...].astype(F32))).astype(BF16)
    done = pltpu.make_async_copy(out_v, out_h, out_sem.at[2])
    done.start()
    for sem, ref in ((0, ds_v), (2, rs_v)):
        pltpu.make_async_copy(ref.at[others], ref.at[others], ep_sem.at[sem]).wait()
    for copy in cache_out:
        copy.wait()
    done.wait()


def solution(mesh):
    EP = mesh.shape['ep']
    row_spec = P(('dp', 'ep'), None)
    cache_spec = P(('dp', 'ep'), None, 'tp', None)
    col_split = P(None, 'tp')
    row_split = P('tp', None)
    in_specs = (row_spec, P(('dp', 'ep')), row_spec, cache_spec, cache_spec, P(None), P(None), P(None), col_split, col_split, col_split, row_split, col_split, col_split, row_split, P(None, None), P('ep', None, 'tp'), P('ep', None, 'tp'), P('ep', 'tp', None))
    out_specs = (row_spec, cache_spec, cache_spec)

    def local_layer(hidden_in, positions, expert_ids, k_cache, v_cache, norm_in, norm_res, norm_post, w_q, w_k, w_v, w_o, w_gate, w_up, w_down, w_router, e_gate, e_up, e_down):
        T, D = hidden_in.shape
        _, L, KV, HD = k_cache.shape
        QH = w_q.shape[1] // HD
        F = w_gate.shape[1]
        EL, _, EF = e_gate.shape
        CAP = 4 * T // EP
        dims = (T, D, L, KV, HD, QH, F, EL, EF, EP, CAP, 512)
        slots = EP * CAP
        cache_rows = (T * L * KV, HD)
        args = (hidden_in, positions.reshape(1, T), expert_ids.T, k_cache.reshape(cache_rows), v_cache.reshape(cache_rows),
                norm_in.reshape(D // 128, 128), norm_res.reshape(D // 128, 128), norm_post.reshape(D // 128, 128),
                w_q, w_k, w_v, w_o, w_gate, w_up, w_down, w_router, e_gate, e_up, e_down)
        mirror = [pltpu.VMEM(a.shape, a.dtype) for i, a in enumerate(args) if i != 14]
        work = [
            pltpu.VMEM(cache_rows, BF16), pltpu.VMEM(cache_rows, BF16),
            pltpu.VMEM((T, D), BF16), pltpu.VMEM((T, QH * HD), F32), pltpu.VMEM((T, QH * HD), BF16),
            pltpu.VMEM((T, D), BF16), pltpu.VMEM((T, D), BF16), pltpu.VMEM((T, D), BF16), pltpu.VMEM((T, D), BF16),
            pltpu.VMEM((T, F), BF16), pltpu.VMEM((T, D), F32),
            pltpu.VMEM((EP, CAP, D + 128), BF16), pltpu.VMEM((EP, CAP, D + 128), BF16), pltpu.VMEM((slots, D + 128), BF16),
            pltpu.VMEM((slots, EL * EF), BF16), pltpu.VMEM((EP, CAP, D), BF16), pltpu.VMEM((EP, CAP, D), BF16), pltpu.VMEM((slots, D), BF16),
            pltpu.VMEM((T, D), BF16), pltpu.VMEM((T, D), BF16), pltpu.VMEM((T, D), BF16),
            pltpu.SemaphoreType.DMA((6,)), pltpu.SemaphoreType.DMA((14,)), pltpu.SemaphoreType.DMA((3,)),
            pltpu.SemaphoreType.DMA((4,)), pltpu.SemaphoreType.DMA((4,)),
        ]
        hbm = pl.BlockSpec(memory_space=pl.ANY)
        out, k_out, v_out = pl.pallas_call(
            functools.partial(layer_kernel, dims),
            out_shape=(jax.ShapeDtypeStruct((T, D), BF16), jax.ShapeDtypeStruct(cache_rows, BF16), jax.ShapeDtypeStruct(cache_rows, BF16)),
            in_specs=[hbm] * len(args),
            out_specs=(hbm, hbm, hbm),
            scratch_shapes=mirror + work,
            compiler_params=pltpu.CompilerParams(collective_id=0, has_side_effects=True, vmem_limit_bytes=67043328),
            name='layer',
        )(*args)
        return out, k_out.reshape(k_cache.shape), v_out.reshape(v_cache.shape)

    return jax.shard_map(local_layer, mesh=mesh, in_specs=in_specs, out_specs=out_specs, check_vma=False)
```

```python
import functools
import math

import jax
import jax.numpy as jnp
from jax import lax
from jax.experimental import pallas as pl
from jax.experimental.pallas import tpu as pltpu
from jax.sharding import PartitionSpec as P

NORM_EPS = 1e-5
ROPE_BASE = 10000.0
MESH = pl.DeviceIdType.MESH
F32 = jnp.float32
BF16 = jnp.bfloat16


def iota(shape, axis):
    return lax.broadcasted_iota(jnp.int32, shape, axis)


def gain_row(ref):
    tile = ref[...].astype(F32)
    return jnp.concatenate([tile[i:i + 1, :] for i in range(tile.shape[0])], axis=1)


def inv_rms(wide):
    return lax.rsqrt(jnp.mean(wide * wide, axis=-1, keepdims=True) + NORM_EPS)


def silu_mul(gate, up):
    return ((gate * jax.nn.sigmoid(gate)) * up).astype(BF16)


def layer_kernel(dims, x_h, pos_h, ids_h, kc_h, vc_h, gin_h, gres_h, gpost_h, wq_h, wk_h, wv_h, wo_h, wg_h, wu_h, wd_h, wr_h,
                 eg_h, eu_h, ed_h, out_h, ko_h, vo_h,
                 x_v, pos_v, ids_v, kc_v, vc_v, gin_v, gres_v, gpost_v, wq_v, wk_v, wv_v, wo_v, wg_v, wu_v, wr_v,
                 eg_v, eu_v, ed_v, ko_v, vo_v, a_v, m_v, q_v, mix_v, as_v, ar_v, h_v, c_v, act_v, den_v,
                 ds_v, dr_v, dp_v, near_v, far_v, gu_v, z_v, xs_v, xr_v, own_v, rs_v, rr_v, ret_v, fs_v, fr_v, out_v,
                 small_sem, w_sem, out_sem, tp_sem, ep_sem):
    T, D, L, KV, HD, QH, F, EL, EF, EP, CAP, TILE = dims
    group = QH // KV
    slots = EP * CAP
    me = lax.axis_index('ep')
    mine = lax.axis_index('tp')
    other = 1 - mine
    HALF = D // 2

    barrier = pltpu.get_barrier_semaphore()

    def signal_peer(i, carry):
        pl.semaphore_signal(barrier, inc=1, device_id={'ep': lax.rem(me + i, EP)}, device_id_type=MESH)
        return carry

    lax.fori_loop(1, EP, signal_peer, 0)
    pl.semaphore_signal(barrier, inc=1, device_id={'tp': other}, device_id_type=MESH)

    small = [(x_h, x_v), (pos_h, pos_v), (ids_h, ids_v), (gin_h, gin_v), (gres_h, gres_v), (gpost_h, gpost_v)]
    for i, (src, dst) in enumerate(small):
        pltpu.make_async_copy(src, dst, small_sem.at[i]).start()

    def fetch(src, dst, sem, parts):
        step = dst.shape[0] // parts
        for i in range(parts):
            rows = pl.ds(i * step, step)
            pltpu.make_async_copy(src.at[rows], dst.at[rows], sem).start()

    def arrive(dst, sem):
        pltpu.make_async_copy(dst, dst, sem).wait()

    fetch(wr_h, wr_v, w_sem.at[0], 1)
    fetch(wk_h, wk_v, w_sem.at[1], 1)
    fetch(wv_h, wv_v, w_sem.at[2], 1)
    fetch(wq_h, wq_v, w_sem.at[3], 4)
    fetch(kc_h, kc_v, w_sem.at[4], 1)
    fetch(vc_h, vc_v, w_sem.at[5], 1)
    fetch(wo_h, wo_v, w_sem.at[6], 4)
    fetch(eg_h, eg_v, w_sem.at[7], EL)
    fetch(eu_h, eu_v, w_sem.at[8], EL)
    fetch(ed_h, ed_v, w_sem.at[9], EL)

    for i, (src, dst) in enumerate(small):
        pltpu.make_async_copy(src, dst, small_sem.at[i]).wait()

    wide = x_v[...].astype(F32)
    scaled = wide * inv_rms(wide)
    a_v[...] = (scaled * gain_row(gin_v)).astype(BF16)
    moe_in = (scaled * gain_row(gpost_v)).astype(BF16)
    m_v[...] = moe_in
    mine_half = pl.ds(pl.multiple_of(mine * HALF, HALF), HALF)
    other_half = pl.ds(pl.multiple_of(other * HALF, HALF), HALF)

    eye = iota((T, T), 0) == iota((T, T), 1)
    before = iota((T, T), 0) < iota((T, T), 1)

    def to_col(row):
        return jnp.sum(jnp.where(eye, row, 0.0), axis=1, keepdims=True)

    ids = ids_v[...]
    pos_row = pos_v[...].astype(F32)
    pos_col = to_col(pos_row)
    id_rows = [ids[k:k + 1, :].astype(F32) for k in range(2)]
    dest_rows = [jnp.floor(r * (1.0 / EL)) for r in id_rows]
    bit_rows = [r - EL * d for r, d in zip(id_rows, dest_rows)]
    dest_cols = [to_col(d) for d in dest_rows]
    rank0 = jnp.sum(jnp.where((dest_cols[0] == dest_rows[0]) & before, 1.0, 0.0), axis=0, keepdims=True)
    rank1 = (jnp.sum(jnp.where(dest_cols[0] == dest_rows[1], 1.0, 0.0), axis=0, keepdims=True)
             + jnp.sum(jnp.where((dest_cols[1] == dest_rows[1]) & before, 1.0, 0.0), axis=0, keepdims=True))
    slot_rows = [dest_rows[0] * CAP + rank0, dest_rows[1] * CAP + rank1]
    slot_cols = [to_col(s) for s in slot_rows]
    slot_iota = iota((slots, T), 0).astype(F32)
    hot = [jnp.where(slot_iota == s, 1.0, 0.0) for s in slot_rows]
    which = jnp.sum(hot[0] * bit_rows[0] + hot[1] * bit_rows[1], axis=1, keepdims=True)
    sent = jnp.dot((hot[0] + hot[1]).astype(BF16), m_v[:, mine_half], preferred_element_type=F32).astype(BF16)
    ds_v[:, :, :HALF] = sent.reshape(EP, CAP, HALF)
    ds_v[:, :, HALF:] = jnp.broadcast_to(which, (slots, 128)).astype(BF16).reshape(EP, CAP, 128)
    dr_v[me] = ds_v[me]

    arrive(wr_v, w_sem.at[0])
    logits = jnp.dot(moe_in, wr_v[...], preferred_element_type=F32)
    expd = jnp.exp(logits - jnp.max(logits, axis=-1, keepdims=True))
    probs = expd / jnp.sum(expd, axis=-1, keepdims=True)
    lane = iota(logits.shape, 1).astype(F32)
    picked = [jnp.sum(jnp.where(lane == to_col(r), probs, 0.0), axis=1, keepdims=True) for r in id_rows]
    total = picked[0] + picked[1]
    weights = [pk / total for pk in picked]

    pl.semaphore_wait(barrier, EP)

    def send_rows(i, carry):
        peer = lax.rem(me + i, EP)
        pltpu.make_async_remote_copy(src_ref=ds_v.at[peer], dst_ref=dr_v.at[me], send_sem=ep_sem.at[0], recv_sem=ep_sem.at[1],
                                     device_id={'ep': peer}, device_id_type=MESH).start()
        return carry

    lax.fori_loop(1, EP, send_rows, 0)

    def tiled(width, body, tile=TILE):
        tile = min(tile, width)

        def step(i, carry):
            body(pl.ds(pl.multiple_of(i * tile, tile), tile))
            return carry

        lax.fori_loop(0, width // tile, step, 0)

    inv_freq = jnp.exp((iota((1, HD), 1) & (HD // 2 - 1)).astype(F32) * (-2.0 / HD * math.log(ROPE_BASE)))
    angles = pos_col * inv_freq
    cosine = jnp.cos(angles)
    sine = jnp.where(iota((1, HD), 1) < HD // 2, -1.0, 1.0) * jnp.sin(angles)

    def rope(head):
        return (head * cosine + pltpu.roll(head, HD // 2, 1) * sine).astype(BF16)

    arrive(wk_v, w_sem.at[1])
    k_proj = jnp.dot(a_v[...], wk_v[...], preferred_element_type=F32)
    k_new = jnp.concatenate([rope(k_proj[:, g * HD:(g + 1) * HD]) for g in range(KV)], axis=0)
    arrive(wv_v, w_sem.at[2])
    v_proj = jnp.dot(a_v[...], wv_v[...], preferred_element_type=F32).astype(BF16)
    v_new = jnp.concatenate([v_proj[:, g * HD:(g + 1) * HD] for g in range(KV)], axis=0)

    arrive(wq_v, w_sem.at[3])

    def q_tile(cols):
        q_v[:, cols] = jnp.dot(a_v[...], wq_v[:, cols], preferred_element_type=F32)

    tiled(QH * HD, q_tile)
    fetch(wg_h, wg_v, w_sem.at[10], 4)
    fetch(wu_h, wu_v, w_sem.at[11], 4)
    half = min(wd_h.shape[0], wq_v.shape[0])
    rest = wd_h.shape[0] - half
    pltpu.make_async_copy(wd_h.at[pl.ds(0, half)], wq_v.at[pl.ds(0, half)], w_sem.at[12]).start()

    arrive(kc_v, w_sem.at[4])
    arrive(vc_v, w_sem.at[5])
    tok_i = iota((T, KV * T), 0)
    lane_j = iota((T, KV * T), 1)
    target = jnp.sum(jnp.where(lax.rem(lane_j, T) == tok_i, (tok_i.astype(F32) * L + pos_col) * KV, 0.0), axis=0, keepdims=True)
    target = target + jnp.floor(iota((1, KV * T), 1).astype(F32) * (1.0 / T))
    new_rows = jnp.concatenate([k_new, v_new, jnp.ones((KV * T, HD), BF16)], axis=1)
    q_heads = [rope(q_v[:, h * HD:(h + 1) * HD]) for h in range(QH)]
    TC = min(16, T)
    width = TC * L * KV
    for c in range(T // TC):
        rows = pl.ds(c * width, width)
        place = jnp.where(iota((width, KV * T), 0).astype(F32) + float(c * width) == target, 1.0, 0.0).astype(BF16)
        placed = jnp.dot(place, new_rows, preferred_element_type=F32)
        hit = placed[:, 2 * HD:] > 0.5
        k_all = jnp.where(hit, placed[:, :HD], kc_v[rows, :].astype(F32)).astype(BF16)
        v_all = jnp.where(hit, placed[:, HD:2 * HD], vc_v[rows, :].astype(F32)).astype(BF16)
        ko_v[rows, :] = k_all
        vo_v[rows, :] = v_all
        q_rows = jnp.concatenate([q[c * TC:(c + 1) * TC] for q in q_heads], axis=0)
        scores = lax.dot_general(q_rows, k_all, (((1,), (1,)), ((), ())), preferred_element_type=F32) * (HD ** -0.5)
        head_kv = iota((QH * TC, 1), 0) // (group * TC)
        base = lax.rem(iota((QH * TC, 1), 0), TC) * (L * KV) + head_kv
        pos_rows = jnp.concatenate([pos_col[c * TC:(c + 1) * TC]] * QH, axis=0).astype(jnp.int32)
        last = base + KV * pos_rows
        col = iota((QH * TC, width), 1)
        visible = (col >= base) & (col <= last) & (lax.rem(col, KV) == head_kv)
        scores = jnp.where(visible, scores, -jnp.inf)
        expo = jnp.exp(scores - jnp.max(scores, axis=-1, keepdims=True))
        attn = (expo / jnp.sum(expo, axis=-1, keepdims=True)).astype(BF16)
        mixed = jnp.dot(attn, v_all, preferred_element_type=F32).astype(BF16)
        mix_v[c * TC:(c + 1) * TC, :] = jnp.concatenate([mixed[h * TC:(h + 1) * TC] for h in range(QH)], axis=1)
    cache_out = [pltpu.make_async_copy(ko_v, ko_h, out_sem.at[0]), pltpu.make_async_copy(vo_v, vo_h, out_sem.at[1])]
    for copy in cache_out:
        copy.start()

    arrive(wo_v, w_sem.at[6])

    def o_tile(cols):
        as_v[:, cols] = jnp.dot(mix_v[...], wo_v[:, cols], preferred_element_type=F32).astype(BF16)

    tiled(D, o_tile)
    if rest:
        pltpu.make_async_copy(wd_h.at[pl.ds(half, rest)], wo_v.at[pl.ds(0, rest)], w_sem.at[13]).start()
    attn_copy = pltpu.make_async_remote_copy(src_ref=as_v, dst_ref=ar_v, send_sem=tp_sem.at[0], recv_sem=tp_sem.at[1],
                                             device_id={'tp': other}, device_id_type=MESH)
    attn_copy.start()
    attn_copy.wait()
    mid = (x_v[...].astype(F32) + (as_v[...].astype(F32) + ar_v[...].astype(F32))).astype(BF16)
    h_v[...] = mid
    mid = mid.astype(F32)
    c_v[...] = (mid * inv_rms(mid) * gain_row(gres_v)).astype(BF16)

    arrive(eg_v, w_sem.at[7])
    arrive(eu_v, w_sem.at[8])
    others = pl.ds(0, EP - 1)
    pltpu.make_async_copy(dr_v.at[others], dr_v.at[others], ep_sem.at[1]).wait()
    rows_copy = pltpu.make_async_remote_copy(src_ref=dr_v, dst_ref=dp_v, send_sem=tp_sem.at[4], recv_sem=tp_sem.at[5],
                                             device_id={'tp': other}, device_id_type=MESH)
    rows_copy.start()
    near_v[...] = dr_v[...].reshape(slots, HALF + 128)
    for e in range(EL):
        gu_v[2 * e] = jnp.dot(near_v[:, :HALF], eg_v[e, mine_half, :], preferred_element_type=F32)
        gu_v[2 * e + 1] = jnp.dot(near_v[:, :HALF], eu_v[e, mine_half, :], preferred_element_type=F32)
    rows_copy.wait()
    far_v[...] = dp_v[:, :, :HALF].reshape(slots, HALF)
    for e in range(EL):
        gate = gu_v[2 * e] + jnp.dot(far_v[...], eg_v[e, other_half, :], preferred_element_type=F32)
        up = gu_v[2 * e + 1] + jnp.dot(far_v[...], eu_v[e, other_half, :], preferred_element_type=F32)
        chosen = near_v[:, HALF:HALF + 1].astype(F32) == float(e)
        z_v[:, e * EF:(e + 1) * EF] = jnp.where(chosen, silu_mul(gate, up).astype(F32), 0.0).astype(BF16)
    arrive(ed_v, w_sem.at[9])

    def expert_down(half):
        part = jnp.dot(z_v[:, :EF], ed_v[0, :, half], preferred_element_type=F32)
        for e in range(1, EL):
            part += jnp.dot(z_v[:, e * EF:(e + 1) * EF], ed_v[e, :, half], preferred_element_type=F32)
        return part

    xs_v[...] = expert_down(other_half).astype(BF16)
    sum_copy = pltpu.make_async_remote_copy(src_ref=xs_v, dst_ref=xr_v, send_sem=tp_sem.at[6], recv_sem=tp_sem.at[7],
                                            device_id={'tp': other}, device_id_type=MESH)
    sum_copy.start()
    own_v[...] = expert_down(mine_half)
    sum_copy.wait()
    rs_v[...] = (own_v[...] + xr_v[...].astype(F32)).astype(BF16).reshape(EP, CAP, HALF)
    rr_v[me] = rs_v[me]

    def send_back(i, carry):
        peer = lax.rem(me + i, EP)
        pltpu.make_async_remote_copy(src_ref=rs_v.at[peer], dst_ref=rr_v.at[me], send_sem=ep_sem.at[2], recv_sem=ep_sem.at[3],
                                     device_id={'ep': peer}, device_id_type=MESH).start()
        return carry

    lax.fori_loop(1, EP, send_back, 0)

    arrive(wg_v, w_sem.at[10])
    arrive(wu_v, w_sem.at[11])

    def ff_tile(cols):
        gate = jnp.dot(c_v[...], wg_v[:, cols], preferred_element_type=F32)
        up = jnp.dot(c_v[...], wu_v[:, cols], preferred_element_type=F32)
        act_v[:, cols] = silu_mul(gate, up)

    tiled(F, ff_tile)

    arrive(wq_v.at[pl.ds(0, half)], w_sem.at[12])
    if rest:
        arrive(wo_v.at[pl.ds(0, rest)], w_sem.at[13])

    def down_tile(cols):
        part = jnp.dot(act_v[:, :half], wq_v[:half, cols], preferred_element_type=F32)
        if rest:
            part += jnp.dot(act_v[:, half:], wo_v[:rest, cols], preferred_element_type=F32)
        den_v[:, cols] = part
        fs_v[:, cols] = part.astype(BF16)

    tiled(D, down_tile)

    pltpu.make_async_copy(rr_v.at[others], rr_v.at[others], ep_sem.at[3]).wait()
    ret_v[...] = rr_v[...].reshape(slots, HALF)
    slot_lane = iota((T, slots), 1).astype(F32)
    take = [jnp.where(slot_lane == s, 1.0, 0.0).astype(BF16) for s in slot_cols]
    moe = weights[0] * jnp.dot(take[0], ret_v[...], preferred_element_type=F32)
    moe += weights[1] * jnp.dot(take[1], ret_v[...], preferred_element_type=F32)
    fs_v[:, mine_half] = (den_v[:, mine_half] + moe).astype(BF16)
    last_copy = pltpu.make_async_remote_copy(src_ref=fs_v, dst_ref=fr_v, send_sem=tp_sem.at[2], recv_sem=tp_sem.at[3],
                                             device_id={'tp': other}, device_id_type=MESH)
    last_copy.start()
    last_copy.wait()
    out_v[...] = (h_v[...].astype(F32) + (fs_v[...].astype(F32) + fr_v[...].astype(F32))).astype(BF16)
    done = pltpu.make_async_copy(out_v, out_h, out_sem.at[2])
    done.start()
    for sem, ref in ((0, ds_v), (2, rs_v)):
        pltpu.make_async_copy(ref.at[others], ref.at[others], ep_sem.at[sem]).wait()
    for copy in cache_out:
        copy.wait()
    done.wait()


def settle_kernel(*refs):
    n = (len(refs) - 1) // 3
    src, dst, buf, sem = refs[:n], refs[n:2 * n], refs[2 * n:3 * n], refs[-1]
    loads = [pltpu.make_async_copy(s, b, sem.at[i]) for i, (s, b) in enumerate(zip(src, buf))]
    stores = [pltpu.make_async_copy(b, d, sem.at[n + i]) for i, (b, d) in enumerate(zip(buf, dst))]
    for copy in loads:
        copy.start()
    for load, store in zip(loads, stores):
        load.wait()
        store.start()
    for copy in stores:
        copy.wait()


def settle(arrays):
    hbm = pl.BlockSpec(memory_space=pl.ANY)
    return pl.pallas_call(
        settle_kernel,
        out_shape=tuple(jax.ShapeDtypeStruct(a.shape, a.dtype) for a in arrays),
        in_specs=[hbm] * len(arrays),
        out_specs=(hbm,) * len(arrays),
        scratch_shapes=[pltpu.VMEM(a.shape, a.dtype) for a in arrays] + [pltpu.SemaphoreType.DMA((2 * len(arrays),))],
        compiler_params=pltpu.CompilerParams(vmem_limit_bytes=67043328),
        name='settle',
    )(*arrays)


def solution(mesh):
    EP = mesh.shape['ep']
    row_spec = P(('dp', 'ep'), None)
    cache_spec = P(('dp', 'ep'), None, 'tp', None)
    col_split = P(None, 'tp')
    row_split = P('tp', None)
    in_specs = (row_spec, P(('dp', 'ep')), row_spec, cache_spec, cache_spec, P(None), P(None), P(None), col_split, col_split, col_split, row_split, col_split, col_split, row_split, P(None, None), P('ep', None, 'tp'), P('ep', None, 'tp'), P('ep', 'tp', None))
    out_specs = (row_spec, cache_spec, cache_spec)

    def local_layer(hidden_in, positions, expert_ids, k_cache, v_cache, norm_in, norm_res, norm_post, w_q, w_k, w_v, w_o, w_gate, w_up, w_down, w_router, e_gate, e_up, e_down):
        T, D = hidden_in.shape
        _, L, KV, HD = k_cache.shape
        QH = w_q.shape[1] // HD
        F = w_gate.shape[1]
        EL, _, EF = e_gate.shape
        CAP = 4 * T // EP
        dims = (T, D, L, KV, HD, QH, F, EL, EF, EP, CAP, 512)
        slots = EP * CAP
        HALF = D // 2
        cache_rows = (T * L * KV, HD)
        args = (hidden_in, positions.reshape(1, T), expert_ids.T, k_cache.reshape(cache_rows), v_cache.reshape(cache_rows),
                norm_in.reshape(D // 128, 128), norm_res.reshape(D // 128, 128), norm_post.reshape(D // 128, 128),
                w_q, w_k, w_v, w_o, w_gate, w_up, w_down, w_router, e_gate, e_up, e_down)
        mirror = [pltpu.VMEM(a.shape, a.dtype) for i, a in enumerate(args) if i != 14]
        work = [
            pltpu.VMEM(cache_rows, BF16), pltpu.VMEM(cache_rows, BF16),
            pltpu.VMEM((T, D), BF16), pltpu.VMEM((T, D), BF16), pltpu.VMEM((T, QH * HD), F32), pltpu.VMEM((T, QH * HD), BF16),
            pltpu.VMEM((T, D), BF16), pltpu.VMEM((T, D), BF16), pltpu.VMEM((T, D), BF16), pltpu.VMEM((T, D), BF16),
            pltpu.VMEM((T, F), BF16), pltpu.VMEM((T, D), F32),
            pltpu.VMEM((EP, CAP, HALF + 128), BF16), pltpu.VMEM((EP, CAP, HALF + 128), BF16), pltpu.VMEM((EP, CAP, HALF + 128), BF16),
            pltpu.VMEM((slots, HALF + 128), BF16), pltpu.VMEM((slots, HALF), BF16), pltpu.VMEM((2 * EL, slots, EF), F32),
            pltpu.VMEM((slots, EL * EF), BF16), pltpu.VMEM((slots, HALF), BF16), pltpu.VMEM((slots, HALF), BF16), pltpu.VMEM((slots, HALF), F32),
            pltpu.VMEM((EP, CAP, HALF), BF16), pltpu.VMEM((EP, CAP, HALF), BF16), pltpu.VMEM((slots, HALF), BF16),
            pltpu.VMEM((T, D), BF16), pltpu.VMEM((T, D), BF16), pltpu.VMEM((T, D), BF16),
            pltpu.SemaphoreType.DMA((6,)), pltpu.SemaphoreType.DMA((14,)), pltpu.SemaphoreType.DMA((3,)),
            pltpu.SemaphoreType.DMA((8,)), pltpu.SemaphoreType.DMA((4,)),
        ]
        hbm = pl.BlockSpec(memory_space=pl.ANY)
        out, k_out, v_out = pl.pallas_call(
            functools.partial(layer_kernel, dims),
            out_shape=(jax.ShapeDtypeStruct((T, D), BF16), jax.ShapeDtypeStruct(cache_rows, BF16), jax.ShapeDtypeStruct(cache_rows, BF16)),
            in_specs=[hbm] * len(args),
            out_specs=(hbm, hbm, hbm),
            scratch_shapes=mirror + work,
            compiler_params=pltpu.CompilerParams(collective_id=0, has_side_effects=True, vmem_limit_bytes=67043328),
            name='layer',
        )(*args)
        out, k_out, v_out = settle((out, k_out, v_out))
        return out, k_out.reshape(k_cache.shape), v_out.reshape(v_cache.shape)

    return jax.shard_map(local_layer, mesh=mesh, in_specs=in_specs, out_specs=out_specs, check_vma=False)
```

```python
import functools
import math
import random

import jax
import jax.numpy as jnp
from jax import lax
from jax.experimental import pallas as pl
from jax.experimental.pallas import tpu as pltpu
from jax.sharding import PartitionSpec as P

NORM_EPS = 1e-5
ROPE_BASE = 10000.0
MESH = pl.DeviceIdType.MESH
F32 = jnp.float32
BF16 = jnp.bfloat16


def iota(shape, axis):
    return lax.broadcasted_iota(jnp.int32, shape, axis)


def peer_steps(n):
    side = round(n ** (1 / 3))
    if side ** 3 != n:
        return n, [(0, 0, i) for i in range(1, n)]
    steps = [(a, b, c) for a in range(side) for b in range(side) for c in range(side)][1:]
    random.Random(1).shuffle(steps)
    return side, sorted(steps, key=lambda s: -sum(min(d, side - d) for d in s))


def gain_row(ref):
    tile = ref[...].astype(F32)
    return jnp.concatenate([tile[i:i + 1, :] for i in range(tile.shape[0])], axis=1)


def inv_rms(wide):
    return lax.rsqrt(jnp.mean(wide * wide, axis=-1, keepdims=True) + NORM_EPS)


def silu_mul(gate, up):
    return ((gate * jax.nn.sigmoid(gate)) * up).astype(BF16)


def layer_kernel(dims, x_h, pos_h, ids_h, kc_h, vc_h, gin_h, gres_h, gpost_h, wq_h, wk_h, wv_h, wo_h, wg_h, wu_h, wd_h, wr_h,
                 eg_h, eu_h, ed_h, out_h, ko_h, vo_h,
                 x_v, pos_v, ids_v, kc_v, vc_v, gin_v, gres_v, gpost_v, wq_v, wk_v, wv_v, wo_v, wg_v, wu_v, wr_v,
                 eg_v, eu_v, ed_v, ko_v, vo_v, a_v, m_v, q_v, mix_v, as_v, ar_v, h_v, c_v, act_v, den_v,
                 ds_v, dr_v, dp_v, near_v, far_v, gu_v, z_v, xs_v, xr_v, own_v, rs_v, rr_v, ret_v, fs_v, fr_v, out_v,
                 small_sem, w_sem, out_sem, tp_sem, ep_sem):
    T, D, L, KV, HD, QH, F, EL, EF, EP, CAP, TILE = dims
    group = QH // KV
    slots = EP * CAP
    me = lax.axis_index('ep')
    mine = lax.axis_index('tp')
    other = 1 - mine
    HALF = D // 2

    barrier = pltpu.get_barrier_semaphore()

    side, steps = peer_steps(EP)
    at = (lax.div(me, side * side), lax.rem(lax.div(me, side), side), lax.rem(me, side))
    digit = [[lax.rem(p + d, side) * side ** (2 - axis) for d in range(side)] for axis, p in enumerate(at)]
    peers = [digit[0][i] + digit[1][j] + digit[2][k] for i, j, k in steps]

    for peer in peers:
        pl.semaphore_signal(barrier, inc=1, device_id={'ep': peer}, device_id_type=MESH)
    pl.semaphore_signal(barrier, inc=1, device_id={'tp': other}, device_id_type=MESH)

    small = [(x_h, x_v), (pos_h, pos_v), (ids_h, ids_v), (gin_h, gin_v), (gres_h, gres_v), (gpost_h, gpost_v)]
    for i, (src, dst) in enumerate(small):
        pltpu.make_async_copy(src, dst, small_sem.at[i]).start()

    def fetch(src, dst, sem, parts):
        step = dst.shape[0] // parts
        for i in range(parts):
            rows = pl.ds(i * step, step)
            pltpu.make_async_copy(src.at[rows], dst.at[rows], sem).start()

    def arrive(dst, sem):
        pltpu.make_async_copy(dst, dst, sem).wait()

    fetch(wr_h, wr_v, w_sem.at[0], 1)
    fetch(wk_h, wk_v, w_sem.at[1], 1)
    fetch(wv_h, wv_v, w_sem.at[2], 1)
    fetch(wq_h, wq_v, w_sem.at[3], 4)
    fetch(kc_h, kc_v, w_sem.at[4], 1)
    fetch(vc_h, vc_v, w_sem.at[5], 1)
    fetch(wo_h, wo_v, w_sem.at[6], 4)
    fetch(eg_h, eg_v, w_sem.at[7], EL)
    fetch(eu_h, eu_v, w_sem.at[8], EL)
    fetch(ed_h, ed_v, w_sem.at[9], EL)

    for i, (src, dst) in enumerate(small):
        pltpu.make_async_copy(src, dst, small_sem.at[i]).wait()

    wide = x_v[...].astype(F32)
    scaled = wide * inv_rms(wide)
    a_v[...] = (scaled * gain_row(gin_v)).astype(BF16)
    moe_in = (scaled * gain_row(gpost_v)).astype(BF16)
    m_v[...] = moe_in
    mine_half = pl.ds(pl.multiple_of(mine * HALF, HALF), HALF)
    other_half = pl.ds(pl.multiple_of(other * HALF, HALF), HALF)

    eye = iota((T, T), 0) == iota((T, T), 1)
    before = iota((T, T), 0) < iota((T, T), 1)

    def to_col(row):
        return jnp.sum(jnp.where(eye, row, 0.0), axis=1, keepdims=True)

    ids = ids_v[...]
    pos_row = pos_v[...].astype(F32)
    pos_col = to_col(pos_row)
    id_rows = [ids[k:k + 1, :].astype(F32) for k in range(2)]
    dest_rows = [jnp.floor(r * (1.0 / EL)) for r in id_rows]
    bit_rows = [r - EL * d for r, d in zip(id_rows, dest_rows)]
    dest_cols = [to_col(d) for d in dest_rows]
    rank0 = jnp.sum(jnp.where((dest_cols[0] == dest_rows[0]) & before, 1.0, 0.0), axis=0, keepdims=True)
    rank1 = (jnp.sum(jnp.where(dest_cols[0] == dest_rows[1], 1.0, 0.0), axis=0, keepdims=True)
             + jnp.sum(jnp.where((dest_cols[1] == dest_rows[1]) & before, 1.0, 0.0), axis=0, keepdims=True))
    slot_rows = [dest_rows[0] * CAP + rank0, dest_rows[1] * CAP + rank1]
    slot_cols = [to_col(s) for s in slot_rows]
    slot_iota = iota((slots, T), 0).astype(F32)
    hot = [jnp.where(slot_iota == s, 1.0, 0.0) for s in slot_rows]
    which = jnp.sum(hot[0] * bit_rows[0] + hot[1] * bit_rows[1], axis=1, keepdims=True)
    sent = jnp.dot((hot[0] + hot[1]).astype(BF16), m_v[:, mine_half], preferred_element_type=F32).astype(BF16)
    ds_v[:, :, :HALF] = sent.reshape(EP, CAP, HALF)
    ds_v[:, :, HALF:] = jnp.broadcast_to(which, (slots, 128)).astype(BF16).reshape(EP, CAP, 128)

    arrive(wr_v, w_sem.at[0])
    logits = jnp.dot(moe_in, wr_v[...], preferred_element_type=F32)
    expd = jnp.exp(logits - jnp.max(logits, axis=-1, keepdims=True))
    probs = expd / jnp.sum(expd, axis=-1, keepdims=True)
    lane = iota(logits.shape, 1).astype(F32)
    picked = [jnp.sum(jnp.where(lane == to_col(r), probs, 0.0), axis=1, keepdims=True) for r in id_rows]
    total = picked[0] + picked[1]
    weights = [pk / total for pk in picked]

    pl.semaphore_wait(barrier, EP)

    def exchange(src, dst, sem):
        for peer in peers:
            pltpu.make_async_remote_copy(src_ref=src.at[peer], dst_ref=dst.at[me], send_sem=ep_sem.at[sem], recv_sem=ep_sem.at[sem + 1],
                                         device_id={'ep': peer}, device_id_type=MESH).start()

    exchange(ds_v, dr_v, 0)
    dr_v[me] = ds_v[me]

    def tiled(width, body, tile=TILE):
        tile = min(tile, width)

        def step(i, carry):
            body(pl.ds(pl.multiple_of(i * tile, tile), tile))
            return carry

        lax.fori_loop(0, width // tile, step, 0)

    inv_freq = jnp.exp((iota((1, HD), 1) & (HD // 2 - 1)).astype(F32) * (-2.0 / HD * math.log(ROPE_BASE)))
    angles = pos_col * inv_freq
    cosine = jnp.cos(angles)
    sine = jnp.where(iota((1, HD), 1) < HD // 2, -1.0, 1.0) * jnp.sin(angles)

    def rope(head):
        return (head * cosine + pltpu.roll(head, HD // 2, 1) * sine).astype(BF16)

    arrive(wk_v, w_sem.at[1])
    k_proj = jnp.dot(a_v[...], wk_v[...], preferred_element_type=F32)
    k_new = jnp.concatenate([rope(k_proj[:, g * HD:(g + 1) * HD]) for g in range(KV)], axis=0)
    arrive(wv_v, w_sem.at[2])
    v_proj = jnp.dot(a_v[...], wv_v[...], preferred_element_type=F32).astype(BF16)
    v_new = jnp.concatenate([v_proj[:, g * HD:(g + 1) * HD] for g in range(KV)], axis=0)

    arrive(wq_v, w_sem.at[3])

    def q_tile(cols):
        q_v[:, cols] = jnp.dot(a_v[...], wq_v[:, cols], preferred_element_type=F32)

    tiled(QH * HD, q_tile)
    fetch(wg_h, wg_v, w_sem.at[10], 4)
    fetch(wu_h, wu_v, w_sem.at[11], 4)
    half = min(wd_h.shape[0], wq_v.shape[0])
    rest = wd_h.shape[0] - half
    pltpu.make_async_copy(wd_h.at[pl.ds(0, half)], wq_v.at[pl.ds(0, half)], w_sem.at[12]).start()

    arrive(kc_v, w_sem.at[4])
    arrive(vc_v, w_sem.at[5])
    tok_i = iota((T, KV * T), 0)
    lane_j = iota((T, KV * T), 1)
    target = jnp.sum(jnp.where(lax.rem(lane_j, T) == tok_i, (tok_i.astype(F32) * L + pos_col) * KV, 0.0), axis=0, keepdims=True)
    target = target + jnp.floor(iota((1, KV * T), 1).astype(F32) * (1.0 / T))
    new_rows = jnp.concatenate([k_new, v_new, jnp.ones((KV * T, HD), BF16)], axis=1)
    q_heads = [rope(q_v[:, h * HD:(h + 1) * HD]) for h in range(QH)]
    TC = min(16, T)
    width = TC * L * KV
    for c in range(T // TC):
        rows = pl.ds(c * width, width)
        place = jnp.where(iota((width, KV * T), 0).astype(F32) + float(c * width) == target, 1.0, 0.0).astype(BF16)
        placed = jnp.dot(place, new_rows, preferred_element_type=F32)
        hit = placed[:, 2 * HD:] > 0.5
        k_all = jnp.where(hit, placed[:, :HD], kc_v[rows, :].astype(F32)).astype(BF16)
        v_all = jnp.where(hit, placed[:, HD:2 * HD], vc_v[rows, :].astype(F32)).astype(BF16)
        ko_v[rows, :] = k_all
        vo_v[rows, :] = v_all
        q_rows = jnp.concatenate([q[c * TC:(c + 1) * TC] for q in q_heads], axis=0)
        scores = lax.dot_general(q_rows, k_all, (((1,), (1,)), ((), ())), preferred_element_type=F32) * (HD ** -0.5)
        head_kv = iota((QH * TC, 1), 0) // (group * TC)
        base = lax.rem(iota((QH * TC, 1), 0), TC) * (L * KV) + head_kv
        pos_rows = jnp.concatenate([pos_col[c * TC:(c + 1) * TC]] * QH, axis=0).astype(jnp.int32)
        last = base + KV * pos_rows
        col = iota((QH * TC, width), 1)
        visible = (col >= base) & (col <= last) & (lax.rem(col, KV) == head_kv)
        scores = jnp.where(visible, scores, -jnp.inf)
        expo = jnp.exp(scores - jnp.max(scores, axis=-1, keepdims=True))
        attn = (expo / jnp.sum(expo, axis=-1, keepdims=True)).astype(BF16)
        mixed = jnp.dot(attn, v_all, preferred_element_type=F32).astype(BF16)
        mix_v[c * TC:(c + 1) * TC, :] = jnp.concatenate([mixed[h * TC:(h + 1) * TC] for h in range(QH)], axis=1)
    cache_out = [pltpu.make_async_copy(ko_v, ko_h, out_sem.at[0]), pltpu.make_async_copy(vo_v, vo_h, out_sem.at[1])]
    for copy in cache_out:
        copy.start()

    arrive(wo_v, w_sem.at[6])

    def o_tile(cols):
        as_v[:, cols] = jnp.dot(mix_v[...], wo_v[:, cols], preferred_element_type=F32).astype(BF16)

    tiled(D, o_tile)
    if rest:
        pltpu.make_async_copy(wd_h.at[pl.ds(half, rest)], wo_v.at[pl.ds(0, rest)], w_sem.at[13]).start()
    attn_copy = pltpu.make_async_remote_copy(src_ref=as_v, dst_ref=ar_v, send_sem=tp_sem.at[0], recv_sem=tp_sem.at[1],
                                             device_id={'tp': other}, device_id_type=MESH)
    attn_copy.start()
    attn_copy.wait()
    mid = (x_v[...].astype(F32) + (as_v[...].astype(F32) + ar_v[...].astype(F32))).astype(BF16)
    h_v[...] = mid
    mid = mid.astype(F32)
    c_v[...] = (mid * inv_rms(mid) * gain_row(gres_v)).astype(BF16)

    arrive(eg_v, w_sem.at[7])
    arrive(eu_v, w_sem.at[8])
    others = pl.ds(0, EP - 1)
    pltpu.make_async_copy(dr_v.at[others], dr_v.at[others], ep_sem.at[1]).wait()
    rows_copy = pltpu.make_async_remote_copy(src_ref=dr_v, dst_ref=dp_v, send_sem=tp_sem.at[4], recv_sem=tp_sem.at[5],
                                             device_id={'tp': other}, device_id_type=MESH)
    rows_copy.start()
    near_v[...] = dr_v[...].reshape(slots, HALF + 128)
    for e in range(EL):
        gu_v[2 * e] = jnp.dot(near_v[:, :HALF], eg_v[e, mine_half, :], preferred_element_type=F32)
        gu_v[2 * e + 1] = jnp.dot(near_v[:, :HALF], eu_v[e, mine_half, :], preferred_element_type=F32)
    rows_copy.wait()
    far_v[...] = dp_v[:, :, :HALF].reshape(slots, HALF)
    for e in range(EL):
        gate = gu_v[2 * e] + jnp.dot(far_v[...], eg_v[e, other_half, :], preferred_element_type=F32)
        up = gu_v[2 * e + 1] + jnp.dot(far_v[...], eu_v[e, other_half, :], preferred_element_type=F32)
        chosen = near_v[:, HALF:HALF + 1].astype(F32) == float(e)
        z_v[:, e * EF:(e + 1) * EF] = jnp.where(chosen, silu_mul(gate, up).astype(F32), 0.0).astype(BF16)
    arrive(ed_v, w_sem.at[9])

    def expert_down(half):
        part = jnp.dot(z_v[:, :EF], ed_v[0, :, half], preferred_element_type=F32)
        for e in range(1, EL):
            part += jnp.dot(z_v[:, e * EF:(e + 1) * EF], ed_v[e, :, half], preferred_element_type=F32)
        return part

    xs_v[...] = expert_down(other_half).astype(BF16)
    sum_copy = pltpu.make_async_remote_copy(src_ref=xs_v, dst_ref=xr_v, send_sem=tp_sem.at[6], recv_sem=tp_sem.at[7],
                                            device_id={'tp': other}, device_id_type=MESH)
    sum_copy.start()
    own_v[...] = expert_down(mine_half)
    sum_copy.wait()
    rs_v[...] = (own_v[...] + xr_v[...].astype(F32)).astype(BF16).reshape(EP, CAP, HALF)
    exchange(rs_v, rr_v, 2)
    rr_v[me] = rs_v[me]

    arrive(wg_v, w_sem.at[10])
    arrive(wu_v, w_sem.at[11])

    def ff_tile(cols):
        gate = jnp.dot(c_v[...], wg_v[:, cols], preferred_element_type=F32)
        up = jnp.dot(c_v[...], wu_v[:, cols], preferred_element_type=F32)
        act_v[:, cols] = silu_mul(gate, up)

    tiled(F, ff_tile)

    arrive(wq_v.at[pl.ds(0, half)], w_sem.at[12])
    if rest:
        arrive(wo_v.at[pl.ds(0, rest)], w_sem.at[13])

    def down_tile(cols):
        part = jnp.dot(act_v[:, :half], wq_v[:half, cols], preferred_element_type=F32)
        if rest:
            part += jnp.dot(act_v[:, half:], wo_v[:rest, cols], preferred_element_type=F32)
        fs_v[:, cols] = part.astype(BF16)

    tiled(D, down_tile)

    dense_copy = pltpu.make_async_remote_copy(src_ref=fs_v, dst_ref=fr_v, send_sem=tp_sem.at[2], recv_sem=tp_sem.at[3],
                                              device_id={'tp': other}, device_id_type=MESH)
    dense_copy.start()
    dense_copy.wait()
    den_v[...] = h_v[:, mine_half].astype(F32) + (fs_v[:, mine_half].astype(F32) + fr_v[:, mine_half].astype(F32))
    slot_lane = iota((T, slots), 1).astype(F32)
    take = [jnp.where(slot_lane == s, 1.0, 0.0).astype(BF16) for s in slot_cols]

    pltpu.make_async_copy(rr_v.at[others], rr_v.at[others], ep_sem.at[3]).wait()
    ret_v[...] = rr_v[...].reshape(slots, HALF)
    moe = weights[0] * jnp.dot(take[0], ret_v[...], preferred_element_type=F32)
    moe += weights[1] * jnp.dot(take[1], ret_v[...], preferred_element_type=F32)
    out_v[...] = (den_v[...] + moe).astype(BF16)
    last_copy = pltpu.make_async_remote_copy(src_ref=out_v, dst_ref=out_h.at[mine], send_sem=tp_sem.at[8], recv_sem=tp_sem.at[9],
                                             device_id={'tp': other}, device_id_type=MESH)
    last_copy.start()
    done = pltpu.make_async_copy(out_v, out_h.at[mine], out_sem.at[2])
    done.start()
    for sem, ref in ((0, ds_v), (2, rs_v)):
        pltpu.make_async_copy(ref.at[others], ref.at[others], ep_sem.at[sem]).wait()
    for copy in cache_out:
        copy.wait()
    last_copy.wait()
    done.wait()


def settle_kernel(half_h, ki_h, vi_h, out_h, ko_h, vo_h, out_v, k_v, v_v, sem):
    T, D = out_v.shape
    cols = [pl.ds(0, D // 2), pl.ds(D // 2, D // 2)]
    halves = [pltpu.make_async_copy(half_h.at[i], out_v.at[:, c], sem.at[i]) for i, c in enumerate(cols)]
    loads = [pltpu.make_async_copy(ki_h, k_v, sem.at[2]), pltpu.make_async_copy(vi_h, v_v, sem.at[3])]
    stores = [pltpu.make_async_copy(k_v, ko_h, sem.at[4]), pltpu.make_async_copy(v_v, vo_h, sem.at[5])]
    last = pltpu.make_async_copy(out_v, out_h, sem.at[6])
    for copy in loads + halves:
        copy.start()
    for load, store in zip(loads, stores):
        load.wait()
        store.start()
    for copy in halves:
        copy.wait()
    last.start()
    for copy in stores + [last]:
        copy.wait()


def settle(halves, k_rows, v_rows):
    hbm = pl.BlockSpec(memory_space=pl.ANY)
    T, D = halves.shape[1], 2 * halves.shape[2]
    shapes = ((T, D), k_rows.shape, v_rows.shape)
    return pl.pallas_call(
        settle_kernel,
        out_shape=tuple(jax.ShapeDtypeStruct(s, BF16) for s in shapes),
        in_specs=[hbm] * 3,
        out_specs=(hbm,) * 3,
        scratch_shapes=[pltpu.VMEM(s, BF16) for s in shapes] + [pltpu.SemaphoreType.DMA((7,))],
        compiler_params=pltpu.CompilerParams(vmem_limit_bytes=67043328),
        name='settle',
    )(halves, k_rows, v_rows)


def solution(mesh):
    EP = mesh.shape['ep']
    row_spec = P(('dp', 'ep'), None)
    cache_spec = P(('dp', 'ep'), None, 'tp', None)
    col_split = P(None, 'tp')
    row_split = P('tp', None)
    in_specs = (row_spec, P(('dp', 'ep')), row_spec, cache_spec, cache_spec, P(None), P(None), P(None), col_split, col_split, col_split, row_split, col_split, col_split, row_split, P(None, None), P('ep', None, 'tp'), P('ep', None, 'tp'), P('ep', 'tp', None))
    out_specs = (row_spec, cache_spec, cache_spec)

    def local_layer(hidden_in, positions, expert_ids, k_cache, v_cache, norm_in, norm_res, norm_post, w_q, w_k, w_v, w_o, w_gate, w_up, w_down, w_router, e_gate, e_up, e_down):
        T, D = hidden_in.shape
        _, L, KV, HD = k_cache.shape
        QH = w_q.shape[1] // HD
        F = w_gate.shape[1]
        EL, _, EF = e_gate.shape
        CAP = 4 * T // EP
        dims = (T, D, L, KV, HD, QH, F, EL, EF, EP, CAP, 512)
        slots = EP * CAP
        HALF = D // 2
        cache_rows = (T * L * KV, HD)
        args = (hidden_in, positions.reshape(1, T), expert_ids.T, k_cache.reshape(cache_rows), v_cache.reshape(cache_rows),
                norm_in.reshape(D // 128, 128), norm_res.reshape(D // 128, 128), norm_post.reshape(D // 128, 128),
                w_q, w_k, w_v, w_o, w_gate, w_up, w_down, w_router, e_gate, e_up, e_down)
        mirror = [pltpu.VMEM(a.shape, a.dtype) for i, a in enumerate(args) if i != 14]
        work = [
            pltpu.VMEM(cache_rows, BF16), pltpu.VMEM(cache_rows, BF16),
            pltpu.VMEM((T, D), BF16), pltpu.VMEM((T, D), BF16), pltpu.VMEM((T, QH * HD), F32), pltpu.VMEM((T, QH * HD), BF16),
            pltpu.VMEM((T, D), BF16), pltpu.VMEM((T, D), BF16), pltpu.VMEM((T, D), BF16), pltpu.VMEM((T, D), BF16),
            pltpu.VMEM((T, F), BF16), pltpu.VMEM((T, HALF), F32),
            pltpu.VMEM((EP, CAP, HALF + 128), BF16), pltpu.VMEM((EP, CAP, HALF + 128), BF16), pltpu.VMEM((EP, CAP, HALF + 128), BF16),
            pltpu.VMEM((slots, HALF + 128), BF16), pltpu.VMEM((slots, HALF), BF16), pltpu.VMEM((2 * EL, slots, EF), F32),
            pltpu.VMEM((slots, EL * EF), BF16), pltpu.VMEM((slots, HALF), BF16), pltpu.VMEM((slots, HALF), BF16), pltpu.VMEM((slots, HALF), F32),
            pltpu.VMEM((EP, CAP, HALF), BF16), pltpu.VMEM((EP, CAP, HALF), BF16), pltpu.VMEM((slots, HALF), BF16),
            pltpu.VMEM((T, D), BF16), pltpu.VMEM((T, D), BF16), pltpu.VMEM((T, HALF), BF16),
            pltpu.SemaphoreType.DMA((6,)), pltpu.SemaphoreType.DMA((14,)), pltpu.SemaphoreType.DMA((3,)),
            pltpu.SemaphoreType.DMA((10,)), pltpu.SemaphoreType.DMA((4,)),
        ]
        hbm = pl.BlockSpec(memory_space=pl.ANY)
        out, k_out, v_out = pl.pallas_call(
            functools.partial(layer_kernel, dims),
            out_shape=(jax.ShapeDtypeStruct((2, T, HALF), BF16), jax.ShapeDtypeStruct(cache_rows, BF16), jax.ShapeDtypeStruct(cache_rows, BF16)),
            in_specs=[hbm] * len(args),
            out_specs=(hbm, hbm, hbm),
            scratch_shapes=mirror + work,
            compiler_params=pltpu.CompilerParams(collective_id=0, has_side_effects=True, vmem_limit_bytes=67043328),
            name='layer',
        )(*args)
        out, k_out, v_out = settle(out, k_out, v_out)
        return out, k_out.reshape(k_cache.shape), v_out.reshape(v_cache.shape)

    return jax.shard_map(local_layer, mesh=mesh, in_specs=in_specs, out_specs=out_specs, check_vma=False)
```

```python
import functools
import math
import random

import jax
import jax.numpy as jnp
from jax import lax
from jax.experimental import pallas as pl
from jax.experimental.pallas import tpu as pltpu
from jax.sharding import PartitionSpec as P

NORM_EPS = 1e-5
ROPE_BASE = 10000.0
MESH = pl.DeviceIdType.MESH
F32 = jnp.float32
BF16 = jnp.bfloat16


def iota(shape, axis):
    return lax.broadcasted_iota(jnp.int32, shape, axis)


def peer_steps(n):
    side = round(n ** (1 / 3))
    if side ** 3 != n:
        return n, [(0, 0, i) for i in range(1, n)]
    steps = [(a, b, c) for a in range(side) for b in range(side) for c in range(side)][1:]
    random.Random(1).shuffle(steps)
    return side, sorted(steps, key=lambda s: -sum(min(d, side - d) for d in s))


def gain_row(ref):
    tile = ref[...].astype(F32)
    return jnp.concatenate([tile[i:i + 1, :] for i in range(tile.shape[0])], axis=1)


def inv_rms(wide):
    return lax.rsqrt(jnp.mean(wide * wide, axis=-1, keepdims=True) + NORM_EPS)


def silu_mul(gate, up):
    return ((gate * jax.nn.sigmoid(gate)) * up).astype(BF16)


def layer_kernel(dims, x_h, pos_h, ids_h, kc_h, vc_h, gin_h, gres_h, gpost_h, wq_h, wk_h, wv_h, wo_h, wg_h, wu_h, wd_h, wr_h,
                 eg_h, eu_h, ed_h, out_h, ko_h, vo_h,
                 x_v, pos_v, ids_v, kc_v, vc_v, gin_v, gres_v, gpost_v, wq_v, wk_v, wv_v, wo_v, wg_v, wu_v, wr_v,
                 eg_v, eu_v, ed_v, ko_v, vo_v, a_v, m_v, q_v, mix_v, as_v, ar_v, h_v, c_v, act_v, den_v,
                 ds_v, dr_v, dp_v, near_v, far_v, gu_v, z_v, xs_v, xr_v, own_v, rs_v, rr_v, ret_v, fs_v, fr_v, out_v,
                 small_sem, w_sem, ff_sem, out_sem, tp_sem, ep_sem):
    T, D, L, KV, HD, QH, F, EL, EF, EP, CAP, TILE = dims
    group = QH // KV
    slots = EP * CAP
    me = lax.axis_index('ep')
    mine = lax.axis_index('tp')
    other = 1 - mine
    HALF = D // 2

    barrier = pltpu.get_barrier_semaphore()

    side, steps = peer_steps(EP)
    at = (lax.div(me, side * side), lax.rem(lax.div(me, side), side), lax.rem(me, side))
    digit = [[lax.rem(p + d, side) * side ** (2 - axis) for d in range(side)] for axis, p in enumerate(at)]
    peers = [digit[0][i] + digit[1][j] + digit[2][k] for i, j, k in steps]

    small = [(x_h, x_v), (ids_h, ids_v), (gpost_h, gpost_v), (gin_h, gin_v), (pos_h, pos_v), (gres_h, gres_v)]
    for i, (src, dst) in enumerate(small):
        pltpu.make_async_copy(src, dst, small_sem.at[i]).start()

    for peer in peers:
        pl.semaphore_signal(barrier, inc=1, device_id={'ep': peer}, device_id_type=MESH)
    pl.semaphore_signal(barrier, inc=1, device_id={'tp': other}, device_id_type=MESH)

    def fetch(src, dst, sem, parts):
        step = dst.shape[0] // parts
        for i in range(parts):
            rows = pl.ds(i * step, step)
            pltpu.make_async_copy(src.at[rows], dst.at[rows], sem).start()

    def arrive(dst, sem):
        pltpu.make_async_copy(dst, dst, sem).wait()

    for i, (src, dst) in enumerate(small):
        pltpu.make_async_copy(src, dst, small_sem.at[i]).wait()

    fetch(wk_h, wk_v, w_sem.at[1], 1)
    fetch(wv_h, wv_v, w_sem.at[2], 1)
    fetch(wq_h, wq_v, w_sem.at[3], 2)

    wide = x_v[...].astype(F32)
    scaled = wide * inv_rms(wide)
    a_v[...] = (scaled * gain_row(gin_v)).astype(BF16)
    moe_in = (scaled * gain_row(gpost_v)).astype(BF16)
    m_v[...] = moe_in
    mine_half = pl.ds(pl.multiple_of(mine * HALF, HALF), HALF)
    other_half = pl.ds(pl.multiple_of(other * HALF, HALF), HALF)

    eye = iota((T, T), 0) == iota((T, T), 1)
    before = iota((T, T), 0) < iota((T, T), 1)

    def to_col(row):
        return jnp.sum(jnp.where(eye, row, 0.0), axis=1, keepdims=True)

    ids = ids_v[...]
    pos_row = pos_v[...].astype(F32)
    pos_col = to_col(pos_row)
    id_rows = [ids[k:k + 1, :].astype(F32) for k in range(2)]
    dest_rows = [jnp.floor(r * (1.0 / EL)) for r in id_rows]
    bit_rows = [r - EL * d for r, d in zip(id_rows, dest_rows)]
    dest_cols = [to_col(d) for d in dest_rows]
    rank0 = jnp.sum(jnp.where((dest_cols[0] == dest_rows[0]) & before, 1.0, 0.0), axis=0, keepdims=True)
    rank1 = (jnp.sum(jnp.where(dest_cols[0] == dest_rows[1], 1.0, 0.0), axis=0, keepdims=True)
             + jnp.sum(jnp.where((dest_cols[1] == dest_rows[1]) & before, 1.0, 0.0), axis=0, keepdims=True))
    slot_rows = [dest_rows[0] * CAP + rank0, dest_rows[1] * CAP + rank1]
    slot_cols = [to_col(s) for s in slot_rows]
    slot_iota = iota((slots, T), 0).astype(F32)
    hot = [jnp.where(slot_iota == s, 1.0, 0.0) for s in slot_rows]
    which = jnp.sum(hot[0] * bit_rows[0] + hot[1] * bit_rows[1], axis=1, keepdims=True)
    sent = jnp.dot((hot[0] + hot[1]).astype(BF16), m_v[:, mine_half], preferred_element_type=F32).astype(BF16)
    ds_v[:, :, :HALF] = sent.reshape(EP, CAP, HALF)
    ds_v[:, :, HALF:] = jnp.broadcast_to(which, (slots, 128)).astype(BF16).reshape(EP, CAP, 128)

    def tiled(width, body, tile=TILE, first=0):
        tile = min(tile, width)

        def step(i, carry):
            body(pl.ds(pl.multiple_of(first + i * tile, tile), tile))
            return carry

        lax.fori_loop(0, width // tile, step, 0)

    inv_freq = jnp.exp((iota((1, HD), 1) & (HD // 2 - 1)).astype(F32) * (-2.0 / HD * math.log(ROPE_BASE)))
    angles = pos_col * inv_freq
    cosine = jnp.cos(angles)
    sine = jnp.where(iota((1, HD), 1) < HD // 2, -1.0, 1.0) * jnp.sin(angles)

    def rope(head):
        return (head * cosine + pltpu.roll(head, HD // 2, 1) * sine).astype(BF16)

    arrive(wk_v, w_sem.at[1])
    k_proj = jnp.dot(a_v[...], wk_v[...], preferred_element_type=F32)
    k_new = jnp.concatenate([rope(k_proj[:, g * HD:(g + 1) * HD]) for g in range(KV)], axis=0)
    arrive(wv_v, w_sem.at[2])
    v_proj = jnp.dot(a_v[...], wv_v[...], preferred_element_type=F32).astype(BF16)
    v_new = jnp.concatenate([v_proj[:, g * HD:(g + 1) * HD] for g in range(KV)], axis=0)

    fetch(kc_h, kc_v, w_sem.at[4], 1)
    fetch(vc_h, vc_v, w_sem.at[5], 1)
    fetch(wo_h, wo_v, w_sem.at[6], 2)

    pl.semaphore_wait(barrier, EP)

    def exchange(src, dst, sem):
        for peer in peers:
            pltpu.make_async_remote_copy(src_ref=src.at[peer], dst_ref=dst.at[me], send_sem=ep_sem.at[sem], recv_sem=ep_sem.at[sem + 1],
                                         device_id={'ep': peer}, device_id_type=MESH).start()

    exchange(ds_v, dr_v, 0)
    dr_v[me] = ds_v[me]
    fetch(eg_h, eg_v, w_sem.at[7], 1)
    fetch(eu_h, eu_v, w_sem.at[8], 1)
    fetch(ed_h, ed_v, w_sem.at[9], 1)
    fetch(wr_h, wr_v, w_sem.at[0], 1)

    arrive(wq_v, w_sem.at[3])

    def q_tile(cols):
        q_v[:, cols] = jnp.dot(a_v[...], wq_v[:, cols], preferred_element_type=F32)

    tiled(QH * HD, q_tile)
    blocks = 3 if F % (3 * TILE) == 0 else 1
    ff_cols = [pl.ds(i * (F // blocks), F // blocks) for i in range(blocks)]
    for i, cols in enumerate(ff_cols):
        pltpu.make_async_copy(wg_h.at[:, cols], wg_v.at[:, cols], ff_sem.at[2 * i]).start()
        pltpu.make_async_copy(wu_h.at[:, cols], wu_v.at[:, cols], ff_sem.at[2 * i + 1]).start()
    half = min(wd_h.shape[0], wq_v.shape[0])
    rest = wd_h.shape[0] - half
    pltpu.make_async_copy(wd_h.at[pl.ds(0, half)], wq_v.at[pl.ds(0, half)], w_sem.at[12]).start()

    arrive(kc_v, w_sem.at[4])
    arrive(vc_v, w_sem.at[5])
    tok_i = iota((T, KV * T), 0)
    lane_j = iota((T, KV * T), 1)
    target = jnp.sum(jnp.where(lax.rem(lane_j, T) == tok_i, (tok_i.astype(F32) * L + pos_col) * KV, 0.0), axis=0, keepdims=True)
    target = target + jnp.floor(iota((1, KV * T), 1).astype(F32) * (1.0 / T))
    new_rows = jnp.concatenate([k_new, v_new, jnp.ones((KV * T, HD), BF16)], axis=1)
    q_heads = [rope(q_v[:, h * HD:(h + 1) * HD]) for h in range(QH)]
    TC = min(16, T)
    width = TC * L * KV
    for c in range(T // TC):
        rows = pl.ds(c * width, width)
        place = jnp.where(iota((width, KV * T), 0).astype(F32) + float(c * width) == target, 1.0, 0.0).astype(BF16)
        placed = jnp.dot(place, new_rows, preferred_element_type=F32)
        hit = placed[:, 2 * HD:] > 0.5
        k_all = jnp.where(hit, placed[:, :HD], kc_v[rows, :].astype(F32)).astype(BF16)
        v_all = jnp.where(hit, placed[:, HD:2 * HD], vc_v[rows, :].astype(F32)).astype(BF16)
        ko_v[rows, :] = k_all
        vo_v[rows, :] = v_all
        q_rows = jnp.concatenate([q[c * TC:(c + 1) * TC] for q in q_heads], axis=0)
        scores = lax.dot_general(q_rows, k_all, (((1,), (1,)), ((), ())), preferred_element_type=F32) * (HD ** -0.5)
        head_kv = iota((QH * TC, 1), 0) // (group * TC)
        base = lax.rem(iota((QH * TC, 1), 0), TC) * (L * KV) + head_kv
        pos_rows = jnp.concatenate([pos_col[c * TC:(c + 1) * TC]] * QH, axis=0).astype(jnp.int32)
        last = base + KV * pos_rows
        col = iota((QH * TC, width), 1)
        visible = (col >= base) & (col <= last) & (lax.rem(col, KV) == head_kv)
        scores = jnp.where(visible, scores, -jnp.inf)
        expo = jnp.exp(scores - jnp.max(scores, axis=-1, keepdims=True))
        attn = (expo / jnp.sum(expo, axis=-1, keepdims=True)).astype(BF16)
        mixed = jnp.dot(attn, v_all, preferred_element_type=F32).astype(BF16)
        mix_v[c * TC:(c + 1) * TC, :] = jnp.concatenate([mixed[h * TC:(h + 1) * TC] for h in range(QH)], axis=1)
    cache_out = [pltpu.make_async_copy(ko_v, ko_h, out_sem.at[0]), pltpu.make_async_copy(vo_v, vo_h, out_sem.at[1])]
    for copy in cache_out:
        copy.start()

    arrive(wo_v, w_sem.at[6])

    def o_tile(cols):
        as_v[:, cols] = jnp.dot(mix_v[...], wo_v[:, cols], preferred_element_type=F32).astype(BF16)

    tiled(D, o_tile)
    if rest:
        pltpu.make_async_copy(wd_h.at[pl.ds(half, rest)], wo_v.at[pl.ds(0, rest)], w_sem.at[13]).start()
    attn_copy = pltpu.make_async_remote_copy(src_ref=as_v, dst_ref=ar_v, send_sem=tp_sem.at[0], recv_sem=tp_sem.at[1],
                                             device_id={'tp': other}, device_id_type=MESH)
    attn_copy.start()

    arrive(eg_v, w_sem.at[7])
    arrive(eu_v, w_sem.at[8])
    others = pl.ds(0, EP - 1)
    pltpu.make_async_copy(dr_v.at[others], dr_v.at[others], ep_sem.at[1]).wait()
    rows_copy = pltpu.make_async_remote_copy(src_ref=dr_v, dst_ref=dp_v, send_sem=tp_sem.at[4], recv_sem=tp_sem.at[5],
                                             device_id={'tp': other}, device_id_type=MESH)
    rows_copy.start()
    near_v[...] = dr_v[...].reshape(slots, HALF + 128)
    for e in range(EL):
        gu_v[2 * e] = jnp.dot(near_v[:, :HALF], eg_v[e, mine_half, :], preferred_element_type=F32)
        gu_v[2 * e + 1] = jnp.dot(near_v[:, :HALF], eu_v[e, mine_half, :], preferred_element_type=F32)
    rows_copy.wait()
    far_v[...] = dp_v[:, :, :HALF].reshape(slots, HALF)
    for e in range(EL):
        gate = gu_v[2 * e] + jnp.dot(far_v[...], eg_v[e, other_half, :], preferred_element_type=F32)
        up = gu_v[2 * e + 1] + jnp.dot(far_v[...], eu_v[e, other_half, :], preferred_element_type=F32)
        chosen = near_v[:, HALF:HALF + 1].astype(F32) == float(e)
        z_v[:, e * EF:(e + 1) * EF] = jnp.where(chosen, silu_mul(gate, up).astype(F32), 0.0).astype(BF16)
    arrive(ed_v, w_sem.at[9])

    def expert_down(half):
        part = jnp.dot(z_v[:, :EF], ed_v[0, :, half], preferred_element_type=F32)
        for e in range(1, EL):
            part += jnp.dot(z_v[:, e * EF:(e + 1) * EF], ed_v[e, :, half], preferred_element_type=F32)
        return part

    xs_v[...] = expert_down(other_half).astype(BF16)
    sum_copy = pltpu.make_async_remote_copy(src_ref=xs_v, dst_ref=xr_v, send_sem=tp_sem.at[6], recv_sem=tp_sem.at[7],
                                            device_id={'tp': other}, device_id_type=MESH)
    sum_copy.start()
    own_v[...] = expert_down(mine_half)
    attn_copy.wait()
    mid = (x_v[...].astype(F32) + (as_v[...].astype(F32) + ar_v[...].astype(F32))).astype(BF16)
    h_v[...] = mid
    mid = mid.astype(F32)
    c_v[...] = (mid * inv_rms(mid) * gain_row(gres_v)).astype(BF16)
    sum_copy.wait()
    rs_v[...] = (own_v[...] + xr_v[...].astype(F32)).astype(BF16).reshape(EP, CAP, HALF)
    exchange(rs_v, rr_v, 2)
    rr_v[me] = rs_v[me]

    def ff_tile(cols):
        gate = jnp.dot(c_v[...], wg_v[:, cols], preferred_element_type=F32)
        up = jnp.dot(c_v[...], wu_v[:, cols], preferred_element_type=F32)
        act_v[:, cols] = silu_mul(gate, up)

    for i, cols in enumerate(ff_cols):
        arrive(wg_v.at[:, cols], ff_sem.at[2 * i])
        arrive(wu_v.at[:, cols], ff_sem.at[2 * i + 1])
        tiled(F // blocks, ff_tile, first=i * (F // blocks))

    arrive(wq_v.at[pl.ds(0, half)], w_sem.at[12])
    if rest:
        arrive(wo_v.at[pl.ds(0, rest)], w_sem.at[13])

    def down_tile(cols):
        part = jnp.dot(act_v[:, :half], wq_v[:half, cols], preferred_element_type=F32)
        if rest:
            part += jnp.dot(act_v[:, half:], wo_v[:rest, cols], preferred_element_type=F32)
        fs_v[:, cols] = part.astype(BF16)

    tiled(D, down_tile)

    dense_copy = pltpu.make_async_remote_copy(src_ref=fs_v, dst_ref=fr_v, send_sem=tp_sem.at[2], recv_sem=tp_sem.at[3],
                                              device_id={'tp': other}, device_id_type=MESH)
    dense_copy.start()
    dense_copy.wait()
    den_v[...] = h_v[:, mine_half].astype(F32) + (fs_v[:, mine_half].astype(F32) + fr_v[:, mine_half].astype(F32))
    arrive(wr_v, w_sem.at[0])
    logits = jnp.dot(m_v[...], wr_v[...], preferred_element_type=F32)
    expd = jnp.exp(logits - jnp.max(logits, axis=-1, keepdims=True))
    probs = expd / jnp.sum(expd, axis=-1, keepdims=True)
    lane = iota(logits.shape, 1).astype(F32)
    picked = [jnp.sum(jnp.where(lane == to_col(r), probs, 0.0), axis=1, keepdims=True) for r in id_rows]
    total = picked[0] + picked[1]
    weights = [pk / total for pk in picked]
    slot_lane = iota((T, slots), 1).astype(F32)
    take = [jnp.where(slot_lane == s, 1.0, 0.0).astype(BF16) for s in slot_cols]

    pltpu.make_async_copy(rr_v.at[others], rr_v.at[others], ep_sem.at[3]).wait()
    ret_v[...] = rr_v[...].reshape(slots, HALF)
    moe = weights[0] * jnp.dot(take[0], ret_v[...], preferred_element_type=F32)
    moe += weights[1] * jnp.dot(take[1], ret_v[...], preferred_element_type=F32)
    out_v[...] = (den_v[...] + moe).astype(BF16)
    last_copy = pltpu.make_async_remote_copy(src_ref=out_v, dst_ref=out_h.at[mine], send_sem=tp_sem.at[8], recv_sem=tp_sem.at[9],
                                             device_id={'tp': other}, device_id_type=MESH)
    last_copy.start()
    done = pltpu.make_async_copy(out_v, out_h.at[mine], out_sem.at[2])
    done.start()
    for sem, ref in ((0, ds_v), (2, rs_v)):
        pltpu.make_async_copy(ref.at[others], ref.at[others], ep_sem.at[sem]).wait()
    for copy in cache_out:
        copy.wait()
    last_copy.wait()
    done.wait()


def settle_kernel(half_h, ki_h, vi_h, out_h, ko_h, vo_h, out_v, k_v, v_v, sem):
    T, D = out_v.shape
    cols = [pl.ds(0, D // 2), pl.ds(D // 2, D // 2)]
    halves = [pltpu.make_async_copy(half_h.at[i], out_v.at[:, c], sem.at[i]) for i, c in enumerate(cols)]
    loads = [pltpu.make_async_copy(ki_h, k_v, sem.at[2]), pltpu.make_async_copy(vi_h, v_v, sem.at[3])]
    stores = [pltpu.make_async_copy(k_v, ko_h, sem.at[4]), pltpu.make_async_copy(v_v, vo_h, sem.at[5])]
    last = pltpu.make_async_copy(out_v, out_h, sem.at[6])
    for copy in loads + halves:
        copy.start()
    for load, store in zip(loads, stores):
        load.wait()
        store.start()
    for copy in halves:
        copy.wait()
    last.start()
    for copy in stores + [last]:
        copy.wait()


def settle(halves, k_rows, v_rows):
    hbm = pl.BlockSpec(memory_space=pl.ANY)
    T, D = halves.shape[1], 2 * halves.shape[2]
    shapes = ((T, D), k_rows.shape, v_rows.shape)
    return pl.pallas_call(
        settle_kernel,
        out_shape=tuple(jax.ShapeDtypeStruct(s, BF16) for s in shapes),
        in_specs=[hbm] * 3,
        out_specs=(hbm,) * 3,
        scratch_shapes=[pltpu.VMEM(s, BF16) for s in shapes] + [pltpu.SemaphoreType.DMA((7,))],
        compiler_params=pltpu.CompilerParams(vmem_limit_bytes=67043328),
        name='settle',
    )(halves, k_rows, v_rows)


def solution(mesh):
    EP = mesh.shape['ep']
    row_spec = P(('dp', 'ep'), None)
    cache_spec = P(('dp', 'ep'), None, 'tp', None)
    col_split = P(None, 'tp')
    row_split = P('tp', None)
    in_specs = (row_spec, P(('dp', 'ep')), row_spec, cache_spec, cache_spec, P(None), P(None), P(None), col_split, col_split, col_split, row_split, col_split, col_split, row_split, P(None, None), P('ep', None, 'tp'), P('ep', None, 'tp'), P('ep', 'tp', None))
    out_specs = (row_spec, cache_spec, cache_spec)

    def local_layer(hidden_in, positions, expert_ids, k_cache, v_cache, norm_in, norm_res, norm_post, w_q, w_k, w_v, w_o, w_gate, w_up, w_down, w_router, e_gate, e_up, e_down):
        T, D = hidden_in.shape
        _, L, KV, HD = k_cache.shape
        QH = w_q.shape[1] // HD
        F = w_gate.shape[1]
        EL, _, EF = e_gate.shape
        CAP = 4 * T // EP
        dims = (T, D, L, KV, HD, QH, F, EL, EF, EP, CAP, 512)
        slots = EP * CAP
        HALF = D // 2
        cache_rows = (T * L * KV, HD)
        args = (hidden_in, positions.reshape(1, T), expert_ids.T, k_cache.reshape(cache_rows), v_cache.reshape(cache_rows),
                norm_in.reshape(D // 128, 128), norm_res.reshape(D // 128, 128), norm_post.reshape(D // 128, 128),
                w_q, w_k, w_v, w_o, w_gate, w_up, w_down, w_router, e_gate, e_up, e_down)
        mirror = [pltpu.VMEM(a.shape, a.dtype) for i, a in enumerate(args) if i != 14]
        work = [
            pltpu.VMEM(cache_rows, BF16), pltpu.VMEM(cache_rows, BF16),
            pltpu.VMEM((T, D), BF16), pltpu.VMEM((T, D), BF16), pltpu.VMEM((T, QH * HD), F32), pltpu.VMEM((T, QH * HD), BF16),
            pltpu.VMEM((T, D), BF16), pltpu.VMEM((T, D), BF16), pltpu.VMEM((T, D), BF16), pltpu.VMEM((T, D), BF16),
            pltpu.VMEM((T, F), BF16), pltpu.VMEM((T, HALF), F32),
            pltpu.VMEM((EP, CAP, HALF + 128), BF16), pltpu.VMEM((EP, CAP, HALF + 128), BF16), pltpu.VMEM((EP, CAP, HALF + 128), BF16),
            pltpu.VMEM((slots, HALF + 128), BF16), pltpu.VMEM((slots, HALF), BF16), pltpu.VMEM((2 * EL, slots, EF), F32),
            pltpu.VMEM((slots, EL * EF), BF16), pltpu.VMEM((slots, HALF), BF16), pltpu.VMEM((slots, HALF), BF16), pltpu.VMEM((slots, HALF), F32),
            pltpu.VMEM((EP, CAP, HALF), BF16), pltpu.VMEM((EP, CAP, HALF), BF16), pltpu.VMEM((slots, HALF), BF16),
            pltpu.VMEM((T, D), BF16), pltpu.VMEM((T, D), BF16), pltpu.VMEM((T, HALF), BF16),
            pltpu.SemaphoreType.DMA((6,)), pltpu.SemaphoreType.DMA((14,)), pltpu.SemaphoreType.DMA((6,)), pltpu.SemaphoreType.DMA((3,)),
            pltpu.SemaphoreType.DMA((10,)), pltpu.SemaphoreType.DMA((4,)),
        ]
        hbm = pl.BlockSpec(memory_space=pl.ANY)
        out, k_out, v_out = pl.pallas_call(
            functools.partial(layer_kernel, dims),
            out_shape=(jax.ShapeDtypeStruct((2, T, HALF), BF16), jax.ShapeDtypeStruct(cache_rows, BF16), jax.ShapeDtypeStruct(cache_rows, BF16)),
            in_specs=[hbm] * len(args),
            out_specs=(hbm, hbm, hbm),
            scratch_shapes=mirror + work,
            compiler_params=pltpu.CompilerParams(collective_id=0, has_side_effects=True, vmem_limit_bytes=67043328),
            name='layer',
        )(*args)
        out, k_out, v_out = settle(out, k_out, v_out)
        return out, k_out.reshape(k_cache.shape), v_out.reshape(v_cache.shape)

    return jax.shard_map(local_layer, mesh=mesh, in_specs=in_specs, out_specs=out_specs, check_vma=False)
```

```python
import functools
import math
import random

import jax
import jax.numpy as jnp
from jax import lax
from jax.experimental import pallas as pl
from jax.experimental.pallas import tpu as pltpu
from jax.sharding import PartitionSpec as P

NORM_EPS = 1e-5
ROPE_BASE = 10000.0
MESH = pl.DeviceIdType.MESH
F32 = jnp.float32
BF16 = jnp.bfloat16


def iota(shape, axis):
    return lax.broadcasted_iota(jnp.int32, shape, axis)


def peer_steps(n):
    side = round(n ** (1 / 3))
    if side ** 3 != n:
        return n, [(0, 0, i) for i in range(1, n)]
    steps = [(a, b, c) for a in range(side) for b in range(side) for c in range(side)][1:]
    random.Random(1).shuffle(steps)
    return side, sorted(steps, key=lambda s: -sum(min(d, side - d) for d in s))


def gain_row(ref):
    tile = ref[...].astype(F32)
    return jnp.concatenate([tile[i:i + 1, :] for i in range(tile.shape[0])], axis=1)


def inv_rms(wide):
    return lax.rsqrt(jnp.mean(wide * wide, axis=-1, keepdims=True) + NORM_EPS)


def silu_mul(gate, up):
    return ((gate * jax.nn.sigmoid(gate)) * up).astype(BF16)


def layer_kernel(dims, x_h, pos_h, ids_h, kc_h, vc_h, gin_h, gres_h, gpost_h, wq_h, wk_h, wv_h, wo_h, wg_h, wu_h, wd_h, wr_h,
                 eg_h, eu_h, ed_h, out_h, ko_h, vo_h,
                 x_v, pos_v, ids_v, kc_v, vc_v, gin_v, gres_v, gpost_v, wq_v, wk_v, wv_v, wo_v, wg_v, wu_v, wr_v,
                 eg_v, eu_v, ed_v, ko_v, vo_v, a_v, m_v, q_v, mix_v, as_v, ar_v, h_v, c_v, act_v, den_v,
                 ds_v, dr_v, dp_v, near_v, far_v, gu_v, z_v, xs_v, xr_v, own_v, rs_v, rr_v, ret_v, fs_v, fr_v, out_v,
                 small_sem, w_sem, ff_sem, out_sem, tp_sem, ep_sem):
    T, D, L, KV, HD, QH, F, EL, EF, EP, CAP, TILE = dims
    group = QH // KV
    slots = EP * CAP
    me = lax.axis_index('ep')
    mine = lax.axis_index('tp')
    other = 1 - mine
    HALF = D // 2

    barrier = pltpu.get_barrier_semaphore()

    side, steps = peer_steps(EP)
    at = (lax.div(me, side * side), lax.rem(lax.div(me, side), side), lax.rem(me, side))
    digit = [[lax.rem(p + d, side) * side ** (2 - axis) for d in range(side)] for axis, p in enumerate(at)]
    peers = [digit[0][i] + digit[1][j] + digit[2][k] for i, j, k in steps]

    small = [(x_h, x_v), (ids_h, ids_v), (gpost_h, gpost_v), (gin_h, gin_v), (pos_h, pos_v), (gres_h, gres_v)]
    for i, (src, dst) in enumerate(small):
        pltpu.make_async_copy(src, dst, small_sem.at[i]).start()

    def fetch(src, dst, sem, parts):
        step = dst.shape[0] // parts
        for i in range(parts):
            rows = pl.ds(i * step, step)
            pltpu.make_async_copy(src.at[rows], dst.at[rows], sem).start()

    def arrive(dst, sem):
        pltpu.make_async_copy(dst, dst, sem).wait()

    fetch(wk_h, wk_v, w_sem.at[1], 1)
    fetch(wv_h, wv_v, w_sem.at[2], 1)

    for peer in peers:
        pl.semaphore_signal(barrier, inc=1, device_id={'ep': peer}, device_id_type=MESH)
    pl.semaphore_signal(barrier, inc=1, device_id={'tp': other}, device_id_type=MESH)

    for i, (src, dst) in enumerate(small):
        pltpu.make_async_copy(src, dst, small_sem.at[i]).wait()

    fetch(wq_h, wq_v, w_sem.at[3], 2)

    wide = x_v[...].astype(F32)
    scaled = wide * inv_rms(wide)
    a_v[...] = (scaled * gain_row(gin_v)).astype(BF16)
    moe_in = (scaled * gain_row(gpost_v)).astype(BF16)
    m_v[...] = moe_in
    mine_half = pl.ds(pl.multiple_of(mine * HALF, HALF), HALF)
    other_half = pl.ds(pl.multiple_of(other * HALF, HALF), HALF)

    eye = iota((T, T), 0) == iota((T, T), 1)
    before = iota((T, T), 0) < iota((T, T), 1)

    def to_col(row):
        return jnp.sum(jnp.where(eye, row, 0.0), axis=1, keepdims=True)

    ids = ids_v[...]
    pos_row = pos_v[...].astype(F32)
    pos_col = to_col(pos_row)
    id_rows = [ids[k:k + 1, :].astype(F32) for k in range(2)]
    dest_rows = [jnp.floor(r * (1.0 / EL)) for r in id_rows]
    bit_rows = [r - EL * d for r, d in zip(id_rows, dest_rows)]
    dest_cols = [to_col(d) for d in dest_rows]
    rank0 = jnp.sum(jnp.where((dest_cols[0] == dest_rows[0]) & before, 1.0, 0.0), axis=0, keepdims=True)
    rank1 = (jnp.sum(jnp.where(dest_cols[0] == dest_rows[1], 1.0, 0.0), axis=0, keepdims=True)
             + jnp.sum(jnp.where((dest_cols[1] == dest_rows[1]) & before, 1.0, 0.0), axis=0, keepdims=True))
    slot_rows = [dest_rows[0] * CAP + rank0, dest_rows[1] * CAP + rank1]
    slot_cols = [to_col(s) for s in slot_rows]
    slot_iota = iota((slots, T), 0).astype(F32)
    hot = [jnp.where(slot_iota == s, 1.0, 0.0) for s in slot_rows]
    which = jnp.sum(hot[0] * bit_rows[0] + hot[1] * bit_rows[1], axis=1, keepdims=True)
    sent = jnp.dot((hot[0] + hot[1]).astype(BF16), m_v[:, mine_half], preferred_element_type=F32).astype(BF16)
    ds_v[:, :, :HALF] = sent.reshape(EP, CAP, HALF)
    ds_v[:, :, HALF:] = jnp.broadcast_to(which, (slots, 128)).astype(BF16).reshape(EP, CAP, 128)

    inv_freq = jnp.exp((iota((1, HD), 1) & (HD // 2 - 1)).astype(F32) * (-2.0 / HD * math.log(ROPE_BASE)))
    angles = pos_col * inv_freq
    cosine = jnp.cos(angles)
    sine = jnp.where(iota((1, HD), 1) < HD // 2, -1.0, 1.0) * jnp.sin(angles)

    def rope(head):
        return (head * cosine + pltpu.roll(head, HD // 2, 1) * sine).astype(BF16)

    arrive(wk_v, w_sem.at[1])
    k_proj = jnp.dot(a_v[...], wk_v[...], preferred_element_type=F32)
    k_new = jnp.concatenate([rope(k_proj[:, g * HD:(g + 1) * HD]) for g in range(KV)], axis=0)
    arrive(wv_v, w_sem.at[2])
    v_proj = jnp.dot(a_v[...], wv_v[...], preferred_element_type=F32).astype(BF16)
    v_new = jnp.concatenate([v_proj[:, g * HD:(g + 1) * HD] for g in range(KV)], axis=0)

    fetch(kc_h, kc_v, w_sem.at[4], 1)
    fetch(vc_h, vc_v, w_sem.at[5], 1)
    fetch(wo_h, wo_v, w_sem.at[6], 2)

    pl.semaphore_wait(barrier, EP)

    def exchange(src, dst, sem):
        for peer in peers:
            pltpu.make_async_remote_copy(src_ref=src.at[peer], dst_ref=dst.at[me], send_sem=ep_sem.at[sem], recv_sem=ep_sem.at[sem + 1],
                                         device_id={'ep': peer}, device_id_type=MESH).start()

    exchange(ds_v, dr_v, 0)
    dr_v[me] = ds_v[me]
    fetch(eg_h, eg_v, w_sem.at[7], 1)
    fetch(eu_h, eu_v, w_sem.at[8], 1)
    fetch(ed_h, ed_v, w_sem.at[9], 1)
    fetch(wr_h, wr_v, w_sem.at[0], 1)

    arrive(wq_v, w_sem.at[3])

    q_v[...] = jnp.dot(a_v[...], wq_v[...], preferred_element_type=F32)
    blocks = 3 if F % (3 * TILE) == 0 else 1
    ff_cols = [pl.ds(i * (F // blocks), F // blocks) for i in range(blocks)]
    for i, cols in enumerate(ff_cols):
        pltpu.make_async_copy(wg_h.at[:, cols], wg_v.at[:, cols], ff_sem.at[2 * i]).start()
        pltpu.make_async_copy(wu_h.at[:, cols], wu_v.at[:, cols], ff_sem.at[2 * i + 1]).start()
    half = min(wd_h.shape[0], wq_v.shape[0])
    rest = wd_h.shape[0] - half
    pltpu.make_async_copy(wd_h.at[pl.ds(0, half)], wq_v.at[pl.ds(0, half)], w_sem.at[12]).start()

    arrive(kc_v, w_sem.at[4])
    arrive(vc_v, w_sem.at[5])
    tok_i = iota((T, KV * T), 0)
    lane_j = iota((T, KV * T), 1)
    target = jnp.sum(jnp.where(lax.rem(lane_j, T) == tok_i, (tok_i.astype(F32) * L + pos_col) * KV, 0.0), axis=0, keepdims=True)
    target = target + jnp.floor(iota((1, KV * T), 1).astype(F32) * (1.0 / T))
    new_rows = jnp.concatenate([k_new, v_new, jnp.ones((KV * T, HD), BF16)], axis=1)
    q_heads = [rope(q_v[:, h * HD:(h + 1) * HD]) for h in range(QH)]
    TC = min(16, T)
    width = TC * L * KV
    for c in range(T // TC):
        rows = pl.ds(c * width, width)
        place = jnp.where(iota((width, KV * T), 0).astype(F32) + float(c * width) == target, 1.0, 0.0).astype(BF16)
        placed = jnp.dot(place, new_rows, preferred_element_type=F32)
        hit = placed[:, 2 * HD:] > 0.5
        k_all = jnp.where(hit, placed[:, :HD], kc_v[rows, :].astype(F32)).astype(BF16)
        v_all = jnp.where(hit, placed[:, HD:2 * HD], vc_v[rows, :].astype(F32)).astype(BF16)
        ko_v[rows, :] = k_all
        vo_v[rows, :] = v_all
        q_rows = jnp.concatenate([q[c * TC:(c + 1) * TC] for q in q_heads], axis=0)
        scores = lax.dot_general(q_rows, k_all, (((1,), (1,)), ((), ())), preferred_element_type=F32) * (HD ** -0.5)
        base = lax.rem(iota((QH * TC, 1), 0), TC) * (L * KV)
        pos_rows = jnp.concatenate([pos_col[c * TC:(c + 1) * TC]] * QH, axis=0).astype(jnp.int32)
        last = base + KV * pos_rows + (KV - 1)
        col = iota((1, width), 1)
        attn = []
        for g in range(KV):
            part = slice(g * group * TC, (g + 1) * group * TC)
            own_col = jnp.where(lax.rem(col, KV) == g, col, -1)
            visible = (own_col >= base[part]) & (own_col <= last[part])
            sub = jnp.where(visible, scores[part], -jnp.inf)
            expo = jnp.exp(sub - jnp.max(sub, axis=-1, keepdims=True))
            attn.append((expo * (1.0 / jnp.sum(expo, axis=-1, keepdims=True))).astype(BF16))
        attn = jnp.concatenate(attn, axis=0)
        mixed = jnp.dot(attn, v_all, preferred_element_type=F32).astype(BF16)
        mix_v[c * TC:(c + 1) * TC, :] = jnp.concatenate([mixed[h * TC:(h + 1) * TC] for h in range(QH)], axis=1)
    cache_out = [pltpu.make_async_copy(ko_v, ko_h, out_sem.at[0]), pltpu.make_async_copy(vo_v, vo_h, out_sem.at[1])]
    for copy in cache_out:
        copy.start()

    others = pl.ds(0, EP - 1)
    pltpu.make_async_copy(dr_v.at[others], dr_v.at[others], ep_sem.at[1]).wait()
    rows_copy = pltpu.make_async_remote_copy(src_ref=dr_v, dst_ref=dp_v, send_sem=tp_sem.at[4], recv_sem=tp_sem.at[5],
                                             device_id={'tp': other}, device_id_type=MESH)
    rows_copy.start()

    arrive(wo_v, w_sem.at[6])

    as_v[...] = jnp.dot(mix_v[...], wo_v[...], preferred_element_type=F32).astype(BF16)
    if rest:
        pltpu.make_async_copy(wd_h.at[pl.ds(half, rest)], wo_v.at[pl.ds(0, rest)], w_sem.at[13]).start()
    attn_copy = pltpu.make_async_remote_copy(src_ref=as_v, dst_ref=ar_v, send_sem=tp_sem.at[0], recv_sem=tp_sem.at[1],
                                             device_id={'tp': other}, device_id_type=MESH)
    attn_copy.start()

    arrive(eg_v, w_sem.at[7])
    arrive(eu_v, w_sem.at[8])
    near_v[...] = dr_v[...].reshape(slots, HALF + 128)
    for e in range(EL):
        gu_v[2 * e] = jnp.dot(near_v[:, :HALF], eg_v[e, mine_half, :], preferred_element_type=F32)
        gu_v[2 * e + 1] = jnp.dot(near_v[:, :HALF], eu_v[e, mine_half, :], preferred_element_type=F32)
    rows_copy.wait()
    far_v[...] = dp_v[:, :, :HALF].reshape(slots, HALF)
    for e in range(EL):
        gate = gu_v[2 * e] + jnp.dot(far_v[...], eg_v[e, other_half, :], preferred_element_type=F32)
        up = gu_v[2 * e + 1] + jnp.dot(far_v[...], eu_v[e, other_half, :], preferred_element_type=F32)
        chosen = near_v[:, HALF:HALF + 1].astype(F32) == float(e)
        z_v[:, e * EF:(e + 1) * EF] = jnp.where(chosen, silu_mul(gate, up).astype(F32), 0.0).astype(BF16)
    arrive(ed_v, w_sem.at[9])

    def expert_down(half):
        part = jnp.dot(z_v[:, :EF], ed_v[0, :, half], preferred_element_type=F32)
        for e in range(1, EL):
            part += jnp.dot(z_v[:, e * EF:(e + 1) * EF], ed_v[e, :, half], preferred_element_type=F32)
        return part

    xs_v[...] = expert_down(other_half).astype(BF16)
    sum_copy = pltpu.make_async_remote_copy(src_ref=xs_v, dst_ref=xr_v, send_sem=tp_sem.at[6], recv_sem=tp_sem.at[7],
                                            device_id={'tp': other}, device_id_type=MESH)
    sum_copy.start()
    own_v[...] = expert_down(mine_half)
    attn_copy.wait()
    mid = (x_v[...].astype(F32) + (as_v[...].astype(F32) + ar_v[...].astype(F32))).astype(BF16)
    h_v[...] = mid
    mid = mid.astype(F32)
    c_v[...] = (mid * inv_rms(mid) * gain_row(gres_v)).astype(BF16)
    arrive(wr_v, w_sem.at[0])
    logits = jnp.dot(m_v[...], wr_v[...], preferred_element_type=F32)
    expd = jnp.exp(logits - jnp.max(logits, axis=-1, keepdims=True))
    probs = expd / jnp.sum(expd, axis=-1, keepdims=True)
    lane = iota(logits.shape, 1).astype(F32)
    picked = [jnp.sum(jnp.where(lane == to_col(r), probs, 0.0), axis=1, keepdims=True) for r in id_rows]
    total = picked[0] + picked[1]
    weights = [pk / total for pk in picked]
    slot_lane = iota((T, slots), 1).astype(F32)
    take = [jnp.where(slot_lane == s, 1.0, 0.0).astype(BF16) for s in slot_cols]

    sum_copy.wait()
    rs_v[...] = (own_v[...] + xr_v[...].astype(F32)).astype(BF16).reshape(EP, CAP, HALF)
    exchange(rs_v, rr_v, 2)
    rr_v[me] = rs_v[me]

    for i, cols in enumerate(ff_cols):
        arrive(wg_v.at[:, cols], ff_sem.at[2 * i])
        arrive(wu_v.at[:, cols], ff_sem.at[2 * i + 1])
        gate = jnp.dot(c_v[...], wg_v[:, cols], preferred_element_type=F32)
        up = jnp.dot(c_v[...], wu_v[:, cols], preferred_element_type=F32)
        act_v[:, cols] = silu_mul(gate, up)

    arrive(wq_v.at[pl.ds(0, half)], w_sem.at[12])
    if rest:
        arrive(wo_v.at[pl.ds(0, rest)], w_sem.at[13])

    def down(cols):
        part = jnp.dot(act_v[:, :half], wq_v[:half, cols], preferred_element_type=F32)
        if rest:
            part += jnp.dot(act_v[:, half:], wo_v[:rest, cols], preferred_element_type=F32)
        return part

    fs_v[...] = down(other_half).astype(BF16)
    dense_copy = pltpu.make_async_remote_copy(src_ref=fs_v, dst_ref=fr_v, send_sem=tp_sem.at[2], recv_sem=tp_sem.at[3],
                                              device_id={'tp': other}, device_id_type=MESH)
    dense_copy.start()
    den_v[...] = h_v[:, mine_half].astype(F32) + down(mine_half)

    pltpu.make_async_copy(rr_v.at[others], rr_v.at[others], ep_sem.at[3]).wait()
    ret_v[...] = rr_v[...].reshape(slots, HALF)
    moe = weights[0] * jnp.dot(take[0], ret_v[...], preferred_element_type=F32)
    moe += weights[1] * jnp.dot(take[1], ret_v[...], preferred_element_type=F32)
    dense_copy.wait()
    out_v[...] = (den_v[...] + fr_v[...].astype(F32) + moe).astype(BF16)
    last_copy = pltpu.make_async_remote_copy(src_ref=out_v, dst_ref=out_h.at[mine], send_sem=tp_sem.at[8], recv_sem=tp_sem.at[9],
                                             device_id={'tp': other}, device_id_type=MESH)
    last_copy.start()
    done = pltpu.make_async_copy(out_v, out_h.at[mine], out_sem.at[2])
    done.start()
    for sem, ref in ((0, ds_v), (2, rs_v)):
        pltpu.make_async_copy(ref.at[others], ref.at[others], ep_sem.at[sem]).wait()
    for copy in cache_out:
        copy.wait()
    last_copy.wait()
    done.wait()


def settle_kernel(half_h, ki_h, vi_h, out_h, ko_h, vo_h, out_v, k_v, v_v, sem):
    T, D = out_v.shape
    cols = [pl.ds(0, D // 2), pl.ds(D // 2, D // 2)]
    halves = [pltpu.make_async_copy(half_h.at[i], out_v.at[:, c], sem.at[i]) for i, c in enumerate(cols)]
    loads = [pltpu.make_async_copy(ki_h, k_v, sem.at[2]), pltpu.make_async_copy(vi_h, v_v, sem.at[3])]
    stores = [pltpu.make_async_copy(k_v, ko_h, sem.at[4]), pltpu.make_async_copy(v_v, vo_h, sem.at[5])]
    last = pltpu.make_async_copy(out_v, out_h, sem.at[6])
    for copy in loads + halves:
        copy.start()
    for load, store in zip(loads, stores):
        load.wait()
        store.start()
    for copy in halves:
        copy.wait()
    last.start()
    for copy in stores + [last]:
        copy.wait()


def settle(halves, k_rows, v_rows):
    hbm = pl.BlockSpec(memory_space=pl.ANY)
    T, D = halves.shape[1], 2 * halves.shape[2]
    shapes = ((T, D), k_rows.shape, v_rows.shape)
    return pl.pallas_call(
        settle_kernel,
        out_shape=tuple(jax.ShapeDtypeStruct(s, BF16) for s in shapes),
        in_specs=[hbm] * 3,
        out_specs=(hbm,) * 3,
        scratch_shapes=[pltpu.VMEM(s, BF16) for s in shapes] + [pltpu.SemaphoreType.DMA((7,))],
        compiler_params=pltpu.CompilerParams(vmem_limit_bytes=67043328),
        name='settle',
    )(halves, k_rows, v_rows)


def solution(mesh):
    EP = mesh.shape['ep']
    row_spec = P(('dp', 'ep'), None)
    cache_spec = P(('dp', 'ep'), None, 'tp', None)
    col_split = P(None, 'tp')
    row_split = P('tp', None)
    in_specs = (row_spec, P(('dp', 'ep')), row_spec, cache_spec, cache_spec, P(None), P(None), P(None), col_split, col_split, col_split, row_split, col_split, col_split, row_split, P(None, None), P('ep', None, 'tp'), P('ep', None, 'tp'), P('ep', 'tp', None))
    out_specs = (row_spec, cache_spec, cache_spec)

    def local_layer(hidden_in, positions, expert_ids, k_cache, v_cache, norm_in, norm_res, norm_post, w_q, w_k, w_v, w_o, w_gate, w_up, w_down, w_router, e_gate, e_up, e_down):
        T, D = hidden_in.shape
        _, L, KV, HD = k_cache.shape
        QH = w_q.shape[1] // HD
        F = w_gate.shape[1]
        EL, _, EF = e_gate.shape
        CAP = 4 * T // EP
        dims = (T, D, L, KV, HD, QH, F, EL, EF, EP, CAP, 512)
        slots = EP * CAP
        HALF = D // 2
        cache_rows = (T * L * KV, HD)
        args = (hidden_in, positions.reshape(1, T), expert_ids.T, k_cache.reshape(cache_rows), v_cache.reshape(cache_rows),
                norm_in.reshape(D // 128, 128), norm_res.reshape(D // 128, 128), norm_post.reshape(D // 128, 128),
                w_q, w_k, w_v, w_o, w_gate, w_up, w_down, w_router, e_gate, e_up, e_down)
        mirror = [pltpu.VMEM(a.shape, a.dtype) for i, a in enumerate(args) if i != 14]
        work = [
            pltpu.VMEM(cache_rows, BF16), pltpu.VMEM(cache_rows, BF16),
            pltpu.VMEM((T, D), BF16), pltpu.VMEM((T, D), BF16), pltpu.VMEM((T, QH * HD), F32), pltpu.VMEM((T, QH * HD), BF16),
            pltpu.VMEM((T, D), BF16), pltpu.VMEM((T, D), BF16), pltpu.VMEM((T, D), BF16), pltpu.VMEM((T, D), BF16),
            pltpu.VMEM((T, F), BF16), pltpu.VMEM((T, HALF), F32),
            pltpu.VMEM((EP, CAP, HALF + 128), BF16), pltpu.VMEM((EP, CAP, HALF + 128), BF16), pltpu.VMEM((EP, CAP, HALF + 128), BF16),
            pltpu.VMEM((slots, HALF + 128), BF16), pltpu.VMEM((slots, HALF), BF16), pltpu.VMEM((2 * EL, slots, EF), F32),
            pltpu.VMEM((slots, EL * EF), BF16), pltpu.VMEM((slots, HALF), BF16), pltpu.VMEM((slots, HALF), BF16), pltpu.VMEM((slots, HALF), F32),
            pltpu.VMEM((EP, CAP, HALF), BF16), pltpu.VMEM((EP, CAP, HALF), BF16), pltpu.VMEM((slots, HALF), BF16),
            pltpu.VMEM((T, HALF), BF16), pltpu.VMEM((T, HALF), BF16), pltpu.VMEM((T, HALF), BF16),
            pltpu.SemaphoreType.DMA((6,)), pltpu.SemaphoreType.DMA((14,)), pltpu.SemaphoreType.DMA((6,)), pltpu.SemaphoreType.DMA((3,)),
            pltpu.SemaphoreType.DMA((10,)), pltpu.SemaphoreType.DMA((4,)),
        ]
        hbm = pl.BlockSpec(memory_space=pl.ANY)
        out, k_out, v_out = pl.pallas_call(
            functools.partial(layer_kernel, dims),
            out_shape=(jax.ShapeDtypeStruct((2, T, HALF), BF16), jax.ShapeDtypeStruct(cache_rows, BF16), jax.ShapeDtypeStruct(cache_rows, BF16)),
            in_specs=[hbm] * len(args),
            out_specs=(hbm, hbm, hbm),
            scratch_shapes=mirror + work,
            compiler_params=pltpu.CompilerParams(collective_id=0, has_side_effects=True, vmem_limit_bytes=67043328),
            name='layer',
        )(*args)
        out, k_out, v_out = settle(out, k_out, v_out)
        return out, k_out.reshape(k_cache.shape), v_out.reshape(v_cache.shape)

    return jax.shard_map(local_layer, mesh=mesh, in_specs=in_specs, out_specs=out_specs, check_vma=False)
```

```python
import functools
import math
import random

import jax
import jax.numpy as jnp
from jax import lax
from jax.experimental import pallas as pl
from jax.experimental.pallas import tpu as pltpu
from jax.sharding import PartitionSpec as P

NORM_EPS = 1e-5
ROPE_BASE = 10000.0
MESH = pl.DeviceIdType.MESH
F32 = jnp.float32
BF16 = jnp.bfloat16


def iota(shape, axis):
    return lax.broadcasted_iota(jnp.int32, shape, axis)


def peer_steps(n):
    side = round(n ** (1 / 3))
    if side ** 3 != n:
        return n, [(0, 0, i) for i in range(1, n)]
    steps = [(a, b, c) for a in range(side) for b in range(side) for c in range(side)][1:]
    random.Random(1).shuffle(steps)
    return side, sorted(steps, key=lambda s: -sum(min(d, side - d) for d in s))


def entry_level(at, side):
    if side != 4:
        return 0 * at[2]
    cost = 0
    for place, table in zip(at, ((0, 8, 17, 23), (0, 5, 10, 13), (0, 4, 9, 11))):
        for i in range(1, 4):
            cost = cost + jnp.where(place == i, table[i], 0)
    return jnp.where(cost <= 12, 2, jnp.where(cost <= 22, 1, 0))


def gain_row(ref):
    tile = ref[...].astype(F32)
    return jnp.concatenate([tile[i:i + 1, :] for i in range(tile.shape[0])], axis=1)


def inv_rms(wide):
    return lax.rsqrt(jnp.mean(wide * wide, axis=-1, keepdims=True) + NORM_EPS)


def silu_mul(gate, up):
    return ((gate * jax.nn.sigmoid(gate)) * up).astype(BF16)


def layer_kernel(dims, x_h, pos_h, ids_h, kc_h, vc_h, gin_h, gres_h, gpost_h, wq_h, wk_h, wv_h, wo_h, wg_h, wu_h, wd_h, wr_h,
                 eg_h, eu_h, ed_h, out_h, ko_h, vo_h,
                 x_v, pos_v, ids_v, kc_v, vc_v, gin_v, gres_v, gpost_v, wq_v, wk_v, wv_v, wo_v, wg_v, wu_v, wr_v,
                 eg_v, eu_v, ed_v, ko_v, vo_v, a_v, m_v, q_v, mix_v, as_v, ar_v, h_v, c_v, act_v, den_v,
                 ds_v, dr_v, dp_v, near_v, far_v, gu_v, z_v, xs_v, xr_v, own_v, rs_v, rr_v, ret_v, fs_v, fr_v, out_v,
                 small_sem, w_sem, ff_sem, out_sem, tp_sem, ep_sem):
    T, D, L, KV, HD, QH, F, EL, EF, EP, CAP, TILE = dims
    group = QH // KV
    slots = EP * CAP
    me = lax.axis_index('ep')
    mine = lax.axis_index('tp')
    other = 1 - mine
    HALF = D // 2

    barrier = pltpu.get_barrier_semaphore()

    side, steps = peer_steps(EP)
    at = (lax.div(me, side * side), lax.rem(lax.div(me, side), side), lax.rem(me, side))
    digit = [[lax.rem(p + d, side) * side ** (2 - axis) for d in range(side)] for axis, p in enumerate(at)]
    peers = [digit[0][i] + digit[1][j] + digit[2][k] for i, j, k in steps]

    small = [(x_h, x_v), (ids_h, ids_v), (gpost_h, gpost_v), (gin_h, gin_v), (pos_h, pos_v), (gres_h, gres_v)]
    for i, (src, dst) in enumerate(small):
        pltpu.make_async_copy(src, dst, small_sem.at[i]).start()

    def fetch(src, dst, sem, parts):
        step = dst.shape[0] // parts
        for i in range(parts):
            rows = pl.ds(i * step, step)
            pltpu.make_async_copy(src.at[rows], dst.at[rows], sem).start()

    def arrive(dst, sem):
        pltpu.make_async_copy(dst, dst, sem).wait()

    fetch(wk_h, wk_v, w_sem.at[1], 1)
    fetch(wv_h, wv_v, w_sem.at[2], 1)

    for peer in peers:
        pl.semaphore_signal(barrier, inc=1, device_id={'ep': peer}, device_id_type=MESH)
    pl.semaphore_signal(barrier, inc=1, device_id={'tp': other}, device_id_type=MESH)

    for i, (src, dst) in enumerate(small):
        pltpu.make_async_copy(src, dst, small_sem.at[i]).wait()

    fetch(wq_h, wq_v, w_sem.at[3], 2)

    wide = x_v[...].astype(F32)
    scaled = wide * inv_rms(wide)
    a_v[...] = (scaled * gain_row(gin_v)).astype(BF16)
    moe_in = (scaled * gain_row(gpost_v)).astype(BF16)
    m_v[...] = moe_in
    mine_half = pl.ds(pl.multiple_of(mine * HALF, HALF), HALF)
    other_half = pl.ds(pl.multiple_of(other * HALF, HALF), HALF)

    eye = iota((T, T), 0) == iota((T, T), 1)
    before = iota((T, T), 0) < iota((T, T), 1)

    def to_col(row):
        return jnp.sum(jnp.where(eye, row, 0.0), axis=1, keepdims=True)

    ids = ids_v[...]
    pos_row = pos_v[...].astype(F32)
    pos_col = to_col(pos_row)
    id_rows = [ids[k:k + 1, :].astype(F32) for k in range(2)]
    dest_rows = [jnp.floor(r * (1.0 / EL)) for r in id_rows]
    bit_rows = [r - EL * d for r, d in zip(id_rows, dest_rows)]
    dest_cols = [to_col(d) for d in dest_rows]
    rank0 = jnp.sum(jnp.where((dest_cols[0] == dest_rows[0]) & before, 1.0, 0.0), axis=0, keepdims=True)
    rank1 = (jnp.sum(jnp.where(dest_cols[0] == dest_rows[1], 1.0, 0.0), axis=0, keepdims=True)
             + jnp.sum(jnp.where((dest_cols[1] == dest_rows[1]) & before, 1.0, 0.0), axis=0, keepdims=True))
    slot_rows = [dest_rows[0] * CAP + rank0, dest_rows[1] * CAP + rank1]
    slot_cols = [to_col(s) for s in slot_rows]
    slot_iota = iota((slots, T), 0).astype(F32)
    hot = [jnp.where(slot_iota == s, 1.0, 0.0) for s in slot_rows]
    which = jnp.sum(hot[0] * bit_rows[0] + hot[1] * bit_rows[1], axis=1, keepdims=True)
    sent = jnp.dot((hot[0] + hot[1]).astype(BF16), m_v[:, mine_half], preferred_element_type=F32).astype(BF16)
    ds_v[:, :, :HALF] = sent.reshape(EP, CAP, HALF)
    ds_v[:, :, HALF:] = jnp.broadcast_to(which, (slots, 128)).astype(BF16).reshape(EP, CAP, 128)

    inv_freq = jnp.exp((iota((1, HD), 1) & (HD // 2 - 1)).astype(F32) * (-2.0 / HD * math.log(ROPE_BASE)))
    angles = pos_col * inv_freq
    cosine = jnp.cos(angles)
    sine = jnp.where(iota((1, HD), 1) < HD // 2, -1.0, 1.0) * jnp.sin(angles)

    def rope(head):
        return (head * cosine + pltpu.roll(head, HD // 2, 1) * sine).astype(BF16)

    arrive(wk_v, w_sem.at[1])
    k_proj = jnp.dot(a_v[...], wk_v[...], preferred_element_type=F32)
    k_new = jnp.concatenate([rope(k_proj[:, g * HD:(g + 1) * HD]) for g in range(KV)], axis=0)
    arrive(wv_v, w_sem.at[2])
    v_proj = jnp.dot(a_v[...], wv_v[...], preferred_element_type=F32).astype(BF16)
    v_new = jnp.concatenate([v_proj[:, g * HD:(g + 1) * HD] for g in range(KV)], axis=0)

    fetch(kc_h, kc_v, w_sem.at[4], 1)
    fetch(vc_h, vc_v, w_sem.at[5], 1)
    fetch(wo_h, wo_v, w_sem.at[6], 2)

    blocks = 3 if F % (3 * TILE) == 0 else 1
    ff_cols = [pl.ds(i * (F // blocks), F // blocks) for i in range(blocks)]
    half = min(wd_h.shape[0], wq_v.shape[0])
    rest = wd_h.shape[0] - half
    cache_out = [pltpu.make_async_copy(ko_v, ko_h, out_sem.at[0]), pltpu.make_async_copy(vo_v, vo_h, out_sem.at[1])]
    level = entry_level(at, side)

    def queries():
        arrive(wq_v, w_sem.at[3])
        fetch(eg_h, eg_v, w_sem.at[7], 1)
        fetch(eu_h, eu_v, w_sem.at[8], 1)
        fetch(ed_h, ed_v, w_sem.at[9], 1)
        fetch(wr_h, wr_v, w_sem.at[0], 1)
        q_v[...] = jnp.dot(a_v[...], wq_v[...], preferred_element_type=F32)
        for i, cols in enumerate(ff_cols):
            pltpu.make_async_copy(wg_h.at[:, cols], wg_v.at[:, cols], ff_sem.at[2 * i]).start()
            pltpu.make_async_copy(wu_h.at[:, cols], wu_v.at[:, cols], ff_sem.at[2 * i + 1]).start()
        pltpu.make_async_copy(wd_h.at[pl.ds(0, half)], wq_v.at[pl.ds(0, half)], w_sem.at[12]).start()

    def attention():
        arrive(kc_v, w_sem.at[4])
        arrive(vc_v, w_sem.at[5])
        tok_i = iota((T, KV * T), 0)
        lane_j = iota((T, KV * T), 1)
        target = jnp.sum(jnp.where(lax.rem(lane_j, T) == tok_i, (tok_i.astype(F32) * L + pos_col) * KV, 0.0), axis=0, keepdims=True)
        target = target + jnp.floor(iota((1, KV * T), 1).astype(F32) * (1.0 / T))
        new_rows = jnp.concatenate([k_new, v_new, jnp.ones((KV * T, HD), BF16)], axis=1)
        q_heads = [rope(q_v[:, h * HD:(h + 1) * HD]) for h in range(QH)]
        TC = min(16, T)
        width = TC * L * KV
        for c in range(T // TC):
            rows = pl.ds(c * width, width)
            place = jnp.where(iota((width, KV * T), 0).astype(F32) + float(c * width) == target, 1.0, 0.0).astype(BF16)
            placed = jnp.dot(place, new_rows, preferred_element_type=F32)
            hit = placed[:, 2 * HD:] > 0.5
            k_all = jnp.where(hit, placed[:, :HD], kc_v[rows, :].astype(F32)).astype(BF16)
            v_all = jnp.where(hit, placed[:, HD:2 * HD], vc_v[rows, :].astype(F32)).astype(BF16)
            ko_v[rows, :] = k_all
            vo_v[rows, :] = v_all
            q_rows = jnp.concatenate([q[c * TC:(c + 1) * TC] for q in q_heads], axis=0)
            scores = lax.dot_general(q_rows, k_all, (((1,), (1,)), ((), ())), preferred_element_type=F32) * (HD ** -0.5)
            base = lax.rem(iota((QH * TC, 1), 0), TC) * (L * KV)
            pos_rows = jnp.concatenate([pos_col[c * TC:(c + 1) * TC]] * QH, axis=0).astype(jnp.int32)
            last = base + KV * pos_rows + (KV - 1)
            col = iota((1, width), 1)
            attn = []
            for g in range(KV):
                part = slice(g * group * TC, (g + 1) * group * TC)
                own_col = jnp.where(lax.rem(col, KV) == g, col, -1)
                visible = (own_col >= base[part]) & (own_col <= last[part])
                sub = jnp.where(visible, scores[part], -jnp.inf)
                expo = jnp.exp(sub - jnp.max(sub, axis=-1, keepdims=True))
                attn.append((expo * (1.0 / jnp.sum(expo, axis=-1, keepdims=True))).astype(BF16))
            attn = jnp.concatenate(attn, axis=0)
            mixed = jnp.dot(attn, v_all, preferred_element_type=F32).astype(BF16)
            mix_v[c * TC:(c + 1) * TC, :] = jnp.concatenate([mixed[h * TC:(h + 1) * TC] for h in range(QH)], axis=1)
        for copy in cache_out:
            copy.start()

    pl.when(level >= 1)(queries)
    pl.when(level >= 2)(attention)

    pl.semaphore_wait(barrier, EP)

    def exchange(src, dst, sem):
        for peer in peers:
            pltpu.make_async_remote_copy(src_ref=src.at[peer], dst_ref=dst.at[me], send_sem=ep_sem.at[sem], recv_sem=ep_sem.at[sem + 1],
                                         device_id={'ep': peer}, device_id_type=MESH).start()

    exchange(ds_v, dr_v, 0)
    dr_v[me] = ds_v[me]

    pl.when(level < 1)(queries)
    pl.when(level < 2)(attention)


    attn_copy = pltpu.make_async_remote_copy(src_ref=as_v, dst_ref=ar_v, send_sem=tp_sem.at[0], recv_sem=tp_sem.at[1],
                                             device_id={'tp': other}, device_id_type=MESH)

    def project():
        arrive(wo_v, w_sem.at[6])

        as_v[...] = jnp.dot(mix_v[...], wo_v[...], preferred_element_type=F32).astype(BF16)
        if rest:
            pltpu.make_async_copy(wd_h.at[pl.ds(half, rest)], wo_v.at[pl.ds(0, rest)], w_sem.at[13]).start()
        attn_copy.start()

    pl.when(level >= 2)(project)

    others = pl.ds(0, EP - 1)
    pltpu.make_async_copy(dr_v.at[others], dr_v.at[others], ep_sem.at[1]).wait()
    rows_copy = pltpu.make_async_remote_copy(src_ref=dr_v, dst_ref=dp_v, send_sem=tp_sem.at[4], recv_sem=tp_sem.at[5],
                                             device_id={'tp': other}, device_id_type=MESH)
    rows_copy.start()

    pl.when(level < 2)(project)

    arrive(eg_v, w_sem.at[7])
    arrive(eu_v, w_sem.at[8])
    near_v[...] = dr_v[...].reshape(slots, HALF + 128)
    for e in range(EL):
        gu_v[2 * e] = jnp.dot(near_v[:, :HALF], eg_v[e, mine_half, :], preferred_element_type=F32)
        gu_v[2 * e + 1] = jnp.dot(near_v[:, :HALF], eu_v[e, mine_half, :], preferred_element_type=F32)
    rows_copy.wait()
    far_v[...] = dp_v[:, :, :HALF].reshape(slots, HALF)
    for e in range(EL):
        gate = gu_v[2 * e] + jnp.dot(far_v[...], eg_v[e, other_half, :], preferred_element_type=F32)
        up = gu_v[2 * e + 1] + jnp.dot(far_v[...], eu_v[e, other_half, :], preferred_element_type=F32)
        chosen = near_v[:, HALF:HALF + 1].astype(F32) == float(e)
        z_v[:, e * EF:(e + 1) * EF] = jnp.where(chosen, silu_mul(gate, up).astype(F32), 0.0).astype(BF16)
    arrive(ed_v, w_sem.at[9])

    def expert_down(half):
        part = jnp.dot(z_v[:, :EF], ed_v[0, :, half], preferred_element_type=F32)
        for e in range(1, EL):
            part += jnp.dot(z_v[:, e * EF:(e + 1) * EF], ed_v[e, :, half], preferred_element_type=F32)
        return part

    xs_v[...] = expert_down(other_half).astype(BF16)
    sum_copy = pltpu.make_async_remote_copy(src_ref=xs_v, dst_ref=xr_v, send_sem=tp_sem.at[6], recv_sem=tp_sem.at[7],
                                            device_id={'tp': other}, device_id_type=MESH)
    sum_copy.start()
    own_v[...] = expert_down(mine_half)
    attn_copy.wait()
    mid = (x_v[...].astype(F32) + (as_v[...].astype(F32) + ar_v[...].astype(F32))).astype(BF16)
    h_v[...] = mid
    mid = mid.astype(F32)
    c_v[...] = (mid * inv_rms(mid) * gain_row(gres_v)).astype(BF16)
    arrive(wr_v, w_sem.at[0])
    logits = jnp.dot(m_v[...], wr_v[...], preferred_element_type=F32)
    expd = jnp.exp(logits - jnp.max(logits, axis=-1, keepdims=True))
    probs = expd / jnp.sum(expd, axis=-1, keepdims=True)
    lane = iota(logits.shape, 1).astype(F32)
    picked = [jnp.sum(jnp.where(lane == to_col(r), probs, 0.0), axis=1, keepdims=True) for r in id_rows]
    total = picked[0] + picked[1]
    weights = [pk / total for pk in picked]
    slot_lane = iota((T, slots), 1).astype(F32)
    take = [jnp.where(slot_lane == s, 1.0, 0.0).astype(BF16) for s in slot_cols]

    sum_copy.wait()
    rs_v[...] = (own_v[...] + xr_v[...].astype(F32)).astype(BF16).reshape(EP, CAP, HALF)
    exchange(rs_v, rr_v, 2)
    rr_v[me] = rs_v[me]

    for i, cols in enumerate(ff_cols):
        arrive(wg_v.at[:, cols], ff_sem.at[2 * i])
        arrive(wu_v.at[:, cols], ff_sem.at[2 * i + 1])
        gate = jnp.dot(c_v[...], wg_v[:, cols], preferred_element_type=F32)
        up = jnp.dot(c_v[...], wu_v[:, cols], preferred_element_type=F32)
        act_v[:, cols] = silu_mul(gate, up)

    arrive(wq_v.at[pl.ds(0, half)], w_sem.at[12])
    if rest:
        arrive(wo_v.at[pl.ds(0, rest)], w_sem.at[13])

    def down(cols):
        part = jnp.dot(act_v[:, :half], wq_v[:half, cols], preferred_element_type=F32)
        if rest:
            part += jnp.dot(act_v[:, half:], wo_v[:rest, cols], preferred_element_type=F32)
        return part

    fs_v[...] = down(other_half).astype(BF16)
    dense_copy = pltpu.make_async_remote_copy(src_ref=fs_v, dst_ref=fr_v, send_sem=tp_sem.at[2], recv_sem=tp_sem.at[3],
                                              device_id={'tp': other}, device_id_type=MESH)
    dense_copy.start()
    den_v[...] = h_v[:, mine_half].astype(F32) + down(mine_half)

    pltpu.make_async_copy(rr_v.at[others], rr_v.at[others], ep_sem.at[3]).wait()
    ret_v[...] = rr_v[...].reshape(slots, HALF)
    moe = weights[0] * jnp.dot(take[0], ret_v[...], preferred_element_type=F32)
    moe += weights[1] * jnp.dot(take[1], ret_v[...], preferred_element_type=F32)
    dense_copy.wait()
    out_v[...] = (den_v[...] + fr_v[...].astype(F32) + moe).astype(BF16)
    last_copy = pltpu.make_async_remote_copy(src_ref=out_v, dst_ref=out_h.at[mine], send_sem=tp_sem.at[8], recv_sem=tp_sem.at[9],
                                             device_id={'tp': other}, device_id_type=MESH)
    last_copy.start()
    done = pltpu.make_async_copy(out_v, out_h.at[mine], out_sem.at[2])
    done.start()
    for sem, ref in ((0, ds_v), (2, rs_v)):
        pltpu.make_async_copy(ref.at[others], ref.at[others], ep_sem.at[sem]).wait()
    for copy in cache_out:
        copy.wait()
    last_copy.wait()
    done.wait()


def settle_kernel(half_h, ki_h, vi_h, out_h, ko_h, vo_h, out_v, k_v, v_v, sem):
    T, D = out_v.shape
    cols = [pl.ds(0, D // 2), pl.ds(D // 2, D // 2)]
    halves = [pltpu.make_async_copy(half_h.at[i], out_v.at[:, c], sem.at[i]) for i, c in enumerate(cols)]
    loads = [pltpu.make_async_copy(ki_h, k_v, sem.at[2]), pltpu.make_async_copy(vi_h, v_v, sem.at[3])]
    stores = [pltpu.make_async_copy(k_v, ko_h, sem.at[4]), pltpu.make_async_copy(v_v, vo_h, sem.at[5])]
    last = pltpu.make_async_copy(out_v, out_h, sem.at[6])
    for copy in loads + halves:
        copy.start()
    for load, store in zip(loads, stores):
        load.wait()
        store.start()
    for copy in halves:
        copy.wait()
    last.start()
    for copy in stores + [last]:
        copy.wait()


def settle(halves, k_rows, v_rows):
    hbm = pl.BlockSpec(memory_space=pl.ANY)
    T, D = halves.shape[1], 2 * halves.shape[2]
    shapes = ((T, D), k_rows.shape, v_rows.shape)
    return pl.pallas_call(
        settle_kernel,
        out_shape=tuple(jax.ShapeDtypeStruct(s, BF16) for s in shapes),
        in_specs=[hbm] * 3,
        out_specs=(hbm,) * 3,
        scratch_shapes=[pltpu.VMEM(s, BF16) for s in shapes] + [pltpu.SemaphoreType.DMA((7,))],
        compiler_params=pltpu.CompilerParams(vmem_limit_bytes=67043328),
        name='settle',
    )(halves, k_rows, v_rows)


def solution(mesh):
    EP = mesh.shape['ep']
    row_spec = P(('dp', 'ep'), None)
    cache_spec = P(('dp', 'ep'), None, 'tp', None)
    col_split = P(None, 'tp')
    row_split = P('tp', None)
    in_specs = (row_spec, P(('dp', 'ep')), row_spec, cache_spec, cache_spec, P(None), P(None), P(None), col_split, col_split, col_split, row_split, col_split, col_split, row_split, P(None, None), P('ep', None, 'tp'), P('ep', None, 'tp'), P('ep', 'tp', None))
    out_specs = (row_spec, cache_spec, cache_spec)

    def local_layer(hidden_in, positions, expert_ids, k_cache, v_cache, norm_in, norm_res, norm_post, w_q, w_k, w_v, w_o, w_gate, w_up, w_down, w_router, e_gate, e_up, e_down):
        T, D = hidden_in.shape
        _, L, KV, HD = k_cache.shape
        QH = w_q.shape[1] // HD
        F = w_gate.shape[1]
        EL, _, EF = e_gate.shape
        CAP = 4 * T // EP
        dims = (T, D, L, KV, HD, QH, F, EL, EF, EP, CAP, 512)
        slots = EP * CAP
        HALF = D // 2
        cache_rows = (T * L * KV, HD)
        args = (hidden_in, positions.reshape(1, T), expert_ids.T, k_cache.reshape(cache_rows), v_cache.reshape(cache_rows),
                norm_in.reshape(D // 128, 128), norm_res.reshape(D // 128, 128), norm_post.reshape(D // 128, 128),
                w_q, w_k, w_v, w_o, w_gate, w_up, w_down, w_router, e_gate, e_up, e_down)
        mirror = [pltpu.VMEM(a.shape, a.dtype) for i, a in enumerate(args) if i != 14]
        work = [
            pltpu.VMEM(cache_rows, BF16), pltpu.VMEM(cache_rows, BF16),
            pltpu.VMEM((T, D), BF16), pltpu.VMEM((T, D), BF16), pltpu.VMEM((T, QH * HD), F32), pltpu.VMEM((T, QH * HD), BF16),
            pltpu.VMEM((T, D), BF16), pltpu.VMEM((T, D), BF16), pltpu.VMEM((T, D), BF16), pltpu.VMEM((T, D), BF16),
            pltpu.VMEM((T, F), BF16), pltpu.VMEM((T, HALF), F32),
            pltpu.VMEM((EP, CAP, HALF + 128), BF16), pltpu.VMEM((EP, CAP, HALF + 128), BF16), pltpu.VMEM((EP, CAP, HALF + 128), BF16),
            pltpu.VMEM((slots, HALF + 128), BF16), pltpu.VMEM((slots, HALF), BF16), pltpu.VMEM((2 * EL, slots, EF), F32),
            pltpu.VMEM((slots, EL * EF), BF16), pltpu.VMEM((slots, HALF), BF16), pltpu.VMEM((slots, HALF), BF16), pltpu.VMEM((slots, HALF), F32),
            pltpu.VMEM((EP, CAP, HALF), BF16), pltpu.VMEM((EP, CAP, HALF), BF16), pltpu.VMEM((slots, HALF), BF16),
            pltpu.VMEM((T, HALF), BF16), pltpu.VMEM((T, HALF), BF16), pltpu.VMEM((T, HALF), BF16),
            pltpu.SemaphoreType.DMA((6,)), pltpu.SemaphoreType.DMA((14,)), pltpu.SemaphoreType.DMA((6,)), pltpu.SemaphoreType.DMA((3,)),
            pltpu.SemaphoreType.DMA((10,)), pltpu.SemaphoreType.DMA((4,)),
        ]
        hbm = pl.BlockSpec(memory_space=pl.ANY)
        out, k_out, v_out = pl.pallas_call(
            functools.partial(layer_kernel, dims),
            out_shape=(jax.ShapeDtypeStruct((2, T, HALF), BF16), jax.ShapeDtypeStruct(cache_rows, BF16), jax.ShapeDtypeStruct(cache_rows, BF16)),
            in_specs=[hbm] * len(args),
            out_specs=(hbm, hbm, hbm),
            scratch_shapes=mirror + work,
            compiler_params=pltpu.CompilerParams(collective_id=0, has_side_effects=True, vmem_limit_bytes=67043328),
            name='layer',
        )(*args)
        out, k_out, v_out = settle(out, k_out, v_out)
        return out, k_out.reshape(k_cache.shape), v_out.reshape(v_cache.shape)

    return jax.shard_map(local_layer, mesh=mesh, in_specs=in_specs, out_specs=out_specs, check_vma=False)
```

```python
import functools
import math
import random

import jax
import jax.numpy as jnp
from jax import lax
from jax.experimental import pallas as pl
from jax.experimental.pallas import tpu as pltpu
from jax.sharding import PartitionSpec as P

NORM_EPS = 1e-5
ROPE_BASE = 10000.0
MESH = pl.DeviceIdType.MESH
F32 = jnp.float32
BF16 = jnp.bfloat16


def iota(shape, axis):
    return lax.broadcasted_iota(jnp.int32, shape, axis)


def peer_steps(n):
    side = round(n ** (1 / 3))
    if side ** 3 != n:
        return n, [(0, 0, i) for i in range(1, n)]
    steps = [(a, b, c) for a in range(side) for b in range(side) for c in range(side)][1:]
    random.Random(1).shuffle(steps)
    return side, sorted(steps, key=lambda s: -sum(min(d, side - d) for d in s))


def entry_order(at, side):
    if side != 4:
        return at[2] < 0, at[2] < 0
    cost = 0
    for place, table in zip(at, ((0, 8, 17, 23), (0, 5, 10, 13), (0, 4, 9, 11))):
        for i in range(1, 4):
            cost = cost + jnp.where(place == i, table[i], 0)
    return cost <= 12, cost >= 30


def gain_row(ref):
    tile = ref[...].astype(F32)
    return jnp.concatenate([tile[i:i + 1, :] for i in range(tile.shape[0])], axis=1)


def inv_rms(wide):
    return lax.rsqrt(jnp.mean(wide * wide, axis=-1, keepdims=True) + NORM_EPS)


def silu_mul(gate, up):
    return ((gate * jax.nn.sigmoid(gate)) * up).astype(BF16)


def layer_kernel(dims, x_h, pos_h, ids_h, kc_h, vc_h, gin_h, gres_h, gpost_h, wq_h, wk_h, wv_h, wo_h, wg_h, wu_h, wd_h, wr_h,
                 eg_h, eu_h, ed_h, out_h, ko_h, vo_h,
                 x_v, pos_v, ids_v, kc_v, vc_v, gin_v, gres_v, gpost_v, wq_v, wk_v, wv_v, wo_v, wg_v, wu_v, wr_v,
                 eg_v, eu_v, ed_v, ko_v, vo_v, a_v, m_v, q_v, mix_v, as_v, ar_v, h_v, c_v, act_v, den_v,
                 ds_v, dr_v, dp_v, near_v, far_v, gu_v, z_v, xs_v, xr_v, own_v, rs_v, rr_v, ret_v, fs_v, fr_v, out_v,
                 small_sem, w_sem, ff_sem, out_sem, tp_sem, ep_sem):
    T, D, L, KV, HD, QH, F, EL, EF, EP, CAP, TILE = dims
    group = QH // KV
    slots = EP * CAP
    me = lax.axis_index('ep')
    mine = lax.axis_index('tp')
    other = 1 - mine
    HALF = D // 2

    barrier = pltpu.get_barrier_semaphore()

    side, steps = peer_steps(EP)
    at = (lax.div(me, side * side), lax.rem(lax.div(me, side), side), lax.rem(me, side))
    digit = [[lax.rem(p + d, side) * side ** (2 - axis) for d in range(side)] for axis, p in enumerate(at)]
    peers = [digit[0][i] + digit[1][j] + digit[2][k] for i, j, k in steps]

    small = [(x_h, x_v), (ids_h, ids_v), (gpost_h, gpost_v), (gin_h, gin_v), (pos_h, pos_v), (gres_h, gres_v)]
    for i, (src, dst) in enumerate(small):
        pltpu.make_async_copy(src, dst, small_sem.at[i]).start()

    def fetch(src, dst, sem, parts):
        step = dst.shape[0] // parts
        for i in range(parts):
            rows = pl.ds(i * step, step)
            pltpu.make_async_copy(src.at[rows], dst.at[rows], sem).start()

    def arrive(dst, sem):
        pltpu.make_async_copy(dst, dst, sem).wait()

    fetch(wk_h, wk_v, w_sem.at[1], 1)
    fetch(wv_h, wv_v, w_sem.at[2], 1)

    for peer in peers:
        pl.semaphore_signal(barrier, inc=1, device_id={'ep': peer}, device_id_type=MESH)
    pl.semaphore_signal(barrier, inc=1, device_id={'tp': other}, device_id_type=MESH)

    for i, (src, dst) in enumerate(small):
        pltpu.make_async_copy(src, dst, small_sem.at[i]).wait()

    fetch(wq_h, wq_v, w_sem.at[3], 2)

    wide = x_v[...].astype(F32)
    scaled = wide * inv_rms(wide)
    a_v[...] = (scaled * gain_row(gin_v)).astype(BF16)
    moe_in = (scaled * gain_row(gpost_v)).astype(BF16)
    m_v[...] = moe_in
    mine_half = pl.ds(pl.multiple_of(mine * HALF, HALF), HALF)
    other_half = pl.ds(pl.multiple_of(other * HALF, HALF), HALF)

    eye = iota((T, T), 0) == iota((T, T), 1)
    before = iota((T, T), 0) < iota((T, T), 1)

    def to_col(row):
        return jnp.sum(jnp.where(eye, row, 0.0), axis=1, keepdims=True)

    ids = ids_v[...]
    pos_row = pos_v[...].astype(F32)
    pos_col = to_col(pos_row)
    id_rows = [ids[k:k + 1, :].astype(F32) for k in range(2)]
    dest_rows = [jnp.floor(r * (1.0 / EL)) for r in id_rows]
    bit_rows = [r - EL * d for r, d in zip(id_rows, dest_rows)]
    dest_cols = [to_col(d) for d in dest_rows]
    rank0 = jnp.sum(jnp.where((dest_cols[0] == dest_rows[0]) & before, 1.0, 0.0), axis=0, keepdims=True)
    rank1 = (jnp.sum(jnp.where(dest_cols[0] == dest_rows[1], 1.0, 0.0), axis=0, keepdims=True)
             + jnp.sum(jnp.where((dest_cols[1] == dest_rows[1]) & before, 1.0, 0.0), axis=0, keepdims=True))
    slot_rows = [dest_rows[0] * CAP + rank0, dest_rows[1] * CAP + rank1]
    slot_cols = [to_col(s) for s in slot_rows]
    slot_iota = iota((slots, T), 0).astype(F32)
    hot = [jnp.where(slot_iota == s, 1.0, 0.0) for s in slot_rows]
    which = jnp.sum(hot[0] * bit_rows[0] + hot[1] * bit_rows[1], axis=1, keepdims=True)
    sent = jnp.dot((hot[0] + hot[1]).astype(BF16), m_v[:, mine_half], preferred_element_type=F32).astype(BF16)
    ds_v[:, :, :HALF] = sent.reshape(EP, CAP, HALF)
    ds_v[:, :, HALF:] = jnp.broadcast_to(which, (slots, 128)).astype(BF16).reshape(EP, CAP, 128)

    inv_freq = jnp.exp((iota((1, HD), 1) & (HD // 2 - 1)).astype(F32) * (-2.0 / HD * math.log(ROPE_BASE)))
    angles = pos_col * inv_freq
    cosine = jnp.cos(angles)
    sine = jnp.where(iota((1, HD), 1) < HD // 2, -1.0, 1.0) * jnp.sin(angles)

    def rope(head):
        return (head * cosine + pltpu.roll(head, HD // 2, 1) * sine).astype(BF16)

    arrive(wk_v, w_sem.at[1])
    k_proj = jnp.dot(a_v[...], wk_v[...], preferred_element_type=F32)
    k_new = jnp.concatenate([rope(k_proj[:, g * HD:(g + 1) * HD]) for g in range(KV)], axis=0)
    arrive(wv_v, w_sem.at[2])
    v_proj = jnp.dot(a_v[...], wv_v[...], preferred_element_type=F32).astype(BF16)
    v_new = jnp.concatenate([v_proj[:, g * HD:(g + 1) * HD] for g in range(KV)], axis=0)

    fetch(kc_h, kc_v, w_sem.at[4], 1)
    fetch(vc_h, vc_v, w_sem.at[5], 1)
    fetch(wo_h, wo_v, w_sem.at[6], 2)

    pl.semaphore_wait(barrier, EP)

    def exchange(src, dst, sem):
        for peer in peers:
            pltpu.make_async_remote_copy(src_ref=src.at[peer], dst_ref=dst.at[me], send_sem=ep_sem.at[sem], recv_sem=ep_sem.at[sem + 1],
                                         device_id={'ep': peer}, device_id_type=MESH).start()

    exchange(ds_v, dr_v, 0)
    dr_v[me] = ds_v[me]
    fetch(eg_h, eg_v, w_sem.at[7], 1)
    fetch(eu_h, eu_v, w_sem.at[8], 1)
    fetch(ed_h, ed_v, w_sem.at[9], 1)
    fetch(wr_h, wr_v, w_sem.at[0], 1)

    arrive(wq_v, w_sem.at[3])

    q_v[...] = jnp.dot(a_v[...], wq_v[...], preferred_element_type=F32)
    blocks = 3 if F % (3 * TILE) == 0 else 1
    ff_cols = [pl.ds(i * (F // blocks), F // blocks) for i in range(blocks)]
    for i, cols in enumerate(ff_cols):
        pltpu.make_async_copy(wg_h.at[:, cols], wg_v.at[:, cols], ff_sem.at[2 * i]).start()
        pltpu.make_async_copy(wu_h.at[:, cols], wu_v.at[:, cols], ff_sem.at[2 * i + 1]).start()
    half = min(wd_h.shape[0], wq_v.shape[0])
    rest = wd_h.shape[0] - half
    pltpu.make_async_copy(wd_h.at[pl.ds(0, half)], wq_v.at[pl.ds(0, half)], w_sem.at[12]).start()

    arrive(kc_v, w_sem.at[4])
    arrive(vc_v, w_sem.at[5])
    tok_i = iota((T, KV * T), 0)
    lane_j = iota((T, KV * T), 1)
    target = jnp.sum(jnp.where(lax.rem(lane_j, T) == tok_i, (tok_i.astype(F32) * L + pos_col) * KV, 0.0), axis=0, keepdims=True)
    target = target + jnp.floor(iota((1, KV * T), 1).astype(F32) * (1.0 / T))
    new_rows = jnp.concatenate([k_new, v_new, jnp.ones((KV * T, HD), BF16)], axis=1)
    q_heads = [rope(q_v[:, h * HD:(h + 1) * HD]) for h in range(QH)]
    TC = min(16, T)
    width = TC * L * KV
    for c in range(T // TC):
        rows = pl.ds(c * width, width)
        place = jnp.where(iota((width, KV * T), 0).astype(F32) + float(c * width) == target, 1.0, 0.0).astype(BF16)
        placed = jnp.dot(place, new_rows, preferred_element_type=F32)
        hit = placed[:, 2 * HD:] > 0.5
        k_all = jnp.where(hit, placed[:, :HD], kc_v[rows, :].astype(F32)).astype(BF16)
        v_all = jnp.where(hit, placed[:, HD:2 * HD], vc_v[rows, :].astype(F32)).astype(BF16)
        ko_v[rows, :] = k_all
        vo_v[rows, :] = v_all
        q_rows = jnp.concatenate([q[c * TC:(c + 1) * TC] for q in q_heads], axis=0)
        scores = lax.dot_general(q_rows, k_all, (((1,), (1,)), ((), ())), preferred_element_type=F32) * (HD ** -0.5)
        base = lax.rem(iota((QH * TC, 1), 0), TC) * (L * KV)
        pos_rows = jnp.concatenate([pos_col[c * TC:(c + 1) * TC]] * QH, axis=0).astype(jnp.int32)
        last = base + KV * pos_rows + (KV - 1)
        col = iota((1, width), 1)
        attn = []
        for g in range(KV):
            part = slice(g * group * TC, (g + 1) * group * TC)
            own_col = jnp.where(lax.rem(col, KV) == g, col, -1)
            visible = (own_col >= base[part]) & (own_col <= last[part])
            sub = jnp.where(visible, scores[part], -jnp.inf)
            expo = jnp.exp(sub - jnp.max(sub, axis=-1, keepdims=True))
            attn.append((expo * (1.0 / jnp.sum(expo, axis=-1, keepdims=True))).astype(BF16))
        attn = jnp.concatenate(attn, axis=0)
        mixed = jnp.dot(attn, v_all, preferred_element_type=F32).astype(BF16)
        mix_v[c * TC:(c + 1) * TC, :] = jnp.concatenate([mixed[h * TC:(h + 1) * TC] for h in range(QH)], axis=1)
    cache_out = [pltpu.make_async_copy(ko_v, ko_h, out_sem.at[0]), pltpu.make_async_copy(vo_v, vo_h, out_sem.at[1])]
    for copy in cache_out:
        copy.start()

    early, late = entry_order(at, side)
    attn_copy = pltpu.make_async_remote_copy(src_ref=as_v, dst_ref=ar_v, send_sem=tp_sem.at[0], recv_sem=tp_sem.at[1],
                                             device_id={'tp': other}, device_id_type=MESH)

    def project(cols):
        as_v[:, cols] = jnp.dot(mix_v[...], wo_v[:, cols], preferred_element_type=F32).astype(BF16)

    def finish_projection():
        project(pl.ds(HALF, HALF))
        if rest:
            pltpu.make_async_copy(wd_h.at[pl.ds(half, rest)], wo_v.at[pl.ds(0, rest)], w_sem.at[13]).start()
        attn_copy.start()

    def middle():
        attn_copy.wait()
        mid = (x_v[...].astype(F32) + (as_v[...].astype(F32) + ar_v[...].astype(F32))).astype(BF16)
        h_v[...] = mid
        mid = mid.astype(F32)
        c_v[...] = (mid * inv_rms(mid) * gain_row(gres_v)).astype(BF16)

    def gate_up(i):
        cols = ff_cols[i]
        arrive(wg_v.at[:, cols], ff_sem.at[2 * i])
        arrive(wu_v.at[:, cols], ff_sem.at[2 * i + 1])
        gate = jnp.dot(c_v[...], wg_v[:, cols], preferred_element_type=F32)
        up = jnp.dot(c_v[...], wu_v[:, cols], preferred_element_type=F32)
        act_v[:, cols] = silu_mul(gate, up)

    def gate_up_first():
        gate_up(0)

    arrive(wo_v, w_sem.at[6])
    project(pl.ds(0, HALF))

    others = pl.ds(0, EP - 1)
    pltpu.make_async_copy(dr_v.at[others], dr_v.at[others], ep_sem.at[1]).wait()
    rows_copy = pltpu.make_async_remote_copy(src_ref=dr_v, dst_ref=dp_v, send_sem=tp_sem.at[4], recv_sem=tp_sem.at[5],
                                             device_id={'tp': other}, device_id_type=MESH)
    rows_copy.start()

    pl.when(jnp.logical_not(late))(finish_projection)
    arrive(eg_v, w_sem.at[7])
    arrive(eu_v, w_sem.at[8])
    near_v[...] = dr_v[...].reshape(slots, HALF + 128)
    for e in range(EL):
        gu_v[2 * e] = jnp.dot(near_v[:, :HALF], eg_v[e, mine_half, :], preferred_element_type=F32)
        gu_v[2 * e + 1] = jnp.dot(near_v[:, :HALF], eu_v[e, mine_half, :], preferred_element_type=F32)
    rows_copy.wait()
    far_v[...] = dp_v[:, :, :HALF].reshape(slots, HALF)
    for e in range(EL):
        gate = gu_v[2 * e] + jnp.dot(far_v[...], eg_v[e, other_half, :], preferred_element_type=F32)
        up = gu_v[2 * e + 1] + jnp.dot(far_v[...], eu_v[e, other_half, :], preferred_element_type=F32)
        chosen = near_v[:, HALF:HALF + 1].astype(F32) == float(e)
        z_v[:, e * EF:(e + 1) * EF] = jnp.where(chosen, silu_mul(gate, up).astype(F32), 0.0).astype(BF16)
    arrive(ed_v, w_sem.at[9])

    def expert_down(half):
        part = jnp.dot(z_v[:, :EF], ed_v[0, :, half], preferred_element_type=F32)
        for e in range(1, EL):
            part += jnp.dot(z_v[:, e * EF:(e + 1) * EF], ed_v[e, :, half], preferred_element_type=F32)
        return part

    xs_v[...] = expert_down(other_half).astype(BF16)
    sum_copy = pltpu.make_async_remote_copy(src_ref=xs_v, dst_ref=xr_v, send_sem=tp_sem.at[6], recv_sem=tp_sem.at[7],
                                            device_id={'tp': other}, device_id_type=MESH)
    sum_copy.start()
    own_v[...] = expert_down(mine_half)
    pl.when(jnp.logical_not(late))(middle)

    arrive(wr_v, w_sem.at[0])
    logits = jnp.dot(m_v[...], wr_v[...], preferred_element_type=F32)
    expd = jnp.exp(logits - jnp.max(logits, axis=-1, keepdims=True))
    probs = expd / jnp.sum(expd, axis=-1, keepdims=True)
    lane = iota(logits.shape, 1).astype(F32)
    picked = [jnp.sum(jnp.where(lane == to_col(r), probs, 0.0), axis=1, keepdims=True) for r in id_rows]
    total = picked[0] + picked[1]
    weights = [pk / total for pk in picked]
    slot_lane = iota((T, slots), 1).astype(F32)
    take = [jnp.where(slot_lane == s, 1.0, 0.0).astype(BF16) for s in slot_cols]

    pl.when(early)(gate_up_first)
    sum_copy.wait()
    rs_v[...] = (own_v[...] + xr_v[...].astype(F32)).astype(BF16).reshape(EP, CAP, HALF)
    exchange(rs_v, rr_v, 2)
    rr_v[me] = rs_v[me]

    pl.when(late)(finish_projection)
    pl.when(late)(middle)
    pl.when(jnp.logical_not(early))(gate_up_first)
    for i in range(1, blocks):
        gate_up(i)

    arrive(wq_v.at[pl.ds(0, half)], w_sem.at[12])
    if rest:
        arrive(wo_v.at[pl.ds(0, rest)], w_sem.at[13])

    def down(cols):
        part = jnp.dot(act_v[:, :half], wq_v[:half, cols], preferred_element_type=F32)
        if rest:
            part += jnp.dot(act_v[:, half:], wo_v[:rest, cols], preferred_element_type=F32)
        return part

    fs_v[...] = down(other_half).astype(BF16)
    dense_copy = pltpu.make_async_remote_copy(src_ref=fs_v, dst_ref=fr_v, send_sem=tp_sem.at[2], recv_sem=tp_sem.at[3],
                                              device_id={'tp': other}, device_id_type=MESH)
    dense_copy.start()
    den_v[...] = h_v[:, mine_half].astype(F32) + down(mine_half)

    pltpu.make_async_copy(rr_v.at[others], rr_v.at[others], ep_sem.at[3]).wait()
    ret_v[...] = rr_v[...].reshape(slots, HALF)
    moe = weights[0] * jnp.dot(take[0], ret_v[...], preferred_element_type=F32)
    moe += weights[1] * jnp.dot(take[1], ret_v[...], preferred_element_type=F32)
    dense_copy.wait()
    out_v[...] = (den_v[...] + fr_v[...].astype(F32) + moe).astype(BF16)
    last_copy = pltpu.make_async_remote_copy(src_ref=out_v, dst_ref=out_h.at[mine], send_sem=tp_sem.at[8], recv_sem=tp_sem.at[9],
                                             device_id={'tp': other}, device_id_type=MESH)
    last_copy.start()
    done = pltpu.make_async_copy(out_v, out_h.at[mine], out_sem.at[2])
    done.start()
    for sem, ref in ((0, ds_v), (2, rs_v)):
        pltpu.make_async_copy(ref.at[others], ref.at[others], ep_sem.at[sem]).wait()
    for copy in cache_out:
        copy.wait()
    last_copy.wait()
    done.wait()


def settle_kernel(half_h, ki_h, vi_h, out_h, ko_h, vo_h, out_v, k_v, v_v, sem):
    T, D = out_v.shape
    cols = [pl.ds(0, D // 2), pl.ds(D // 2, D // 2)]
    halves = [pltpu.make_async_copy(half_h.at[i], out_v.at[:, c], sem.at[i]) for i, c in enumerate(cols)]
    loads = [pltpu.make_async_copy(ki_h, k_v, sem.at[2]), pltpu.make_async_copy(vi_h, v_v, sem.at[3])]
    stores = [pltpu.make_async_copy(k_v, ko_h, sem.at[4]), pltpu.make_async_copy(v_v, vo_h, sem.at[5])]
    last = pltpu.make_async_copy(out_v, out_h, sem.at[6])
    for copy in loads + halves:
        copy.start()
    for load, store in zip(loads, stores):
        load.wait()
        store.start()
    for copy in halves:
        copy.wait()
    last.start()
    for copy in stores + [last]:
        copy.wait()


def settle(halves, k_rows, v_rows):
    hbm = pl.BlockSpec(memory_space=pl.ANY)
    T, D = halves.shape[1], 2 * halves.shape[2]
    shapes = ((T, D), k_rows.shape, v_rows.shape)
    return pl.pallas_call(
        settle_kernel,
        out_shape=tuple(jax.ShapeDtypeStruct(s, BF16) for s in shapes),
        in_specs=[hbm] * 3,
        out_specs=(hbm,) * 3,
        scratch_shapes=[pltpu.VMEM(s, BF16) for s in shapes] + [pltpu.SemaphoreType.DMA((7,))],
        compiler_params=pltpu.CompilerParams(vmem_limit_bytes=67043328),
        name='settle',
    )(halves, k_rows, v_rows)


def solution(mesh):
    EP = mesh.shape['ep']
    row_spec = P(('dp', 'ep'), None)
    cache_spec = P(('dp', 'ep'), None, 'tp', None)
    col_split = P(None, 'tp')
    row_split = P('tp', None)
    in_specs = (row_spec, P(('dp', 'ep')), row_spec, cache_spec, cache_spec, P(None), P(None), P(None), col_split, col_split, col_split, row_split, col_split, col_split, row_split, P(None, None), P('ep', None, 'tp'), P('ep', None, 'tp'), P('ep', 'tp', None))
    out_specs = (row_spec, cache_spec, cache_spec)

    def local_layer(hidden_in, positions, expert_ids, k_cache, v_cache, norm_in, norm_res, norm_post, w_q, w_k, w_v, w_o, w_gate, w_up, w_down, w_router, e_gate, e_up, e_down):
        T, D = hidden_in.shape
        _, L, KV, HD = k_cache.shape
        QH = w_q.shape[1] // HD
        F = w_gate.shape[1]
        EL, _, EF = e_gate.shape
        CAP = 4 * T // EP
        dims = (T, D, L, KV, HD, QH, F, EL, EF, EP, CAP, 512)
        slots = EP * CAP
        HALF = D // 2
        cache_rows = (T * L * KV, HD)
        args = (hidden_in, positions.reshape(1, T), expert_ids.T, k_cache.reshape(cache_rows), v_cache.reshape(cache_rows),
                norm_in.reshape(D // 128, 128), norm_res.reshape(D // 128, 128), norm_post.reshape(D // 128, 128),
                w_q, w_k, w_v, w_o, w_gate, w_up, w_down, w_router, e_gate, e_up, e_down)
        mirror = [pltpu.VMEM(a.shape, a.dtype) for i, a in enumerate(args) if i != 14]
        work = [
            pltpu.VMEM(cache_rows, BF16), pltpu.VMEM(cache_rows, BF16),
            pltpu.VMEM((T, D), BF16), pltpu.VMEM((T, D), BF16), pltpu.VMEM((T, QH * HD), F32), pltpu.VMEM((T, QH * HD), BF16),
            pltpu.VMEM((T, D), BF16), pltpu.VMEM((T, D), BF16), pltpu.VMEM((T, D), BF16), pltpu.VMEM((T, D), BF16),
            pltpu.VMEM((T, F), BF16), pltpu.VMEM((T, HALF), F32),
            pltpu.VMEM((EP, CAP, HALF + 128), BF16), pltpu.VMEM((EP, CAP, HALF + 128), BF16), pltpu.VMEM((EP, CAP, HALF + 128), BF16),
            pltpu.VMEM((slots, HALF + 128), BF16), pltpu.VMEM((slots, HALF), BF16), pltpu.VMEM((2 * EL, slots, EF), F32),
            pltpu.VMEM((slots, EL * EF), BF16), pltpu.VMEM((slots, HALF), BF16), pltpu.VMEM((slots, HALF), BF16), pltpu.VMEM((slots, HALF), F32),
            pltpu.VMEM((EP, CAP, HALF), BF16), pltpu.VMEM((EP, CAP, HALF), BF16), pltpu.VMEM((slots, HALF), BF16),
            pltpu.VMEM((T, HALF), BF16), pltpu.VMEM((T, HALF), BF16), pltpu.VMEM((T, HALF), BF16),
            pltpu.SemaphoreType.DMA((6,)), pltpu.SemaphoreType.DMA((14,)), pltpu.SemaphoreType.DMA((6,)), pltpu.SemaphoreType.DMA((3,)),
            pltpu.SemaphoreType.DMA((10,)), pltpu.SemaphoreType.DMA((4,)),
        ]
        hbm = pl.BlockSpec(memory_space=pl.ANY)
        out, k_out, v_out = pl.pallas_call(
            functools.partial(layer_kernel, dims),
            out_shape=(jax.ShapeDtypeStruct((2, T, HALF), BF16), jax.ShapeDtypeStruct(cache_rows, BF16), jax.ShapeDtypeStruct(cache_rows, BF16)),
            in_specs=[hbm] * len(args),
            out_specs=(hbm, hbm, hbm),
            scratch_shapes=mirror + work,
            compiler_params=pltpu.CompilerParams(collective_id=0, has_side_effects=True, vmem_limit_bytes=67043328),
            name='layer',
        )(*args)
        out, k_out, v_out = settle(out, k_out, v_out)
        return out, k_out.reshape(k_cache.shape), v_out.reshape(v_cache.shape)

    return jax.shard_map(local_layer, mesh=mesh, in_specs=in_specs, out_specs=out_specs, check_vma=False)
```

```python
import functools
import math
import random

import jax
import jax.numpy as jnp
from jax import lax
from jax.experimental import pallas as pl
from jax.experimental.pallas import tpu as pltpu
from jax.sharding import PartitionSpec as P

NORM_EPS = 1e-5
ROPE_BASE = 10000.0
MESH = pl.DeviceIdType.MESH
F32 = jnp.float32
BF16 = jnp.bfloat16


def iota(shape, axis):
    return lax.broadcasted_iota(jnp.int32, shape, axis)


def peer_steps(n):
    side = round(n ** (1 / 3))
    if side ** 3 != n:
        return n, [(0, 0, i) for i in range(1, n)]
    steps = [(a, b, c) for a in range(side) for b in range(side) for c in range(side)][1:]
    random.Random(1).shuffle(steps)
    return side, sorted(steps, key=lambda s: -sum(min(d, side - d) for d in s))


def entry_order(at, side):
    if side != 4:
        return at[2] < 0, at[2] < 0
    cost = 0
    for place, table in zip(at, ((0, 8, 17, 23), (0, 5, 10, 13), (0, 4, 9, 11))):
        for i in range(1, 4):
            cost = cost + jnp.where(place == i, table[i], 0)
    return cost <= 12, cost >= 30


def gain_row(ref):
    tile = ref[...].astype(F32)
    return jnp.concatenate([tile[i:i + 1, :] for i in range(tile.shape[0])], axis=1)


def inv_rms(wide):
    return lax.rsqrt(jnp.mean(wide * wide, axis=-1, keepdims=True) + NORM_EPS)


def silu_mul(gate, up):
    return ((gate * jax.nn.sigmoid(gate)) * up).astype(BF16)


def layer_kernel(dims, x_h, pos_h, ids_h, kc_h, vc_h, gin_h, gres_h, gpost_h, wq_h, wk_h, wv_h, wo_h, wg_h, wu_h, wd_h, wr_h,
                 eg_h, eu_h, ed_h, out_h, ko_h, vo_h,
                 x_v, pos_v, ids_v, kc_v, vc_v, gin_v, gres_v, gpost_v, wq_v, wk_v, wv_v, wo_v, wg_v, wu_v, wr_v,
                 eg_v, eu_v, ed_v, ko_v, vo_v, a_v, m_v, q_v, mix_v, as_v, ar_v, h_v, c_v, act_v, den_v,
                 ds_v, dr_v, dp_v, near_v, far_v, gu_v, z_v, xs_v, xr_v, own_v, rs_v, rr_v, ret_v, fs_v, fr_v, out_v,
                 small_sem, w_sem, ff_sem, out_sem, tp_sem, ep_sem):
    T, D, L, KV, HD, QH, F, EL, EF, EP, CAP, TILE = dims
    group = QH // KV
    slots = EP * CAP
    me = lax.axis_index('ep')
    mine = lax.axis_index('tp')
    other = 1 - mine
    HALF = D // 2

    barrier = pltpu.get_barrier_semaphore()

    side, steps = peer_steps(EP)
    at = (lax.div(me, side * side), lax.rem(lax.div(me, side), side), lax.rem(me, side))
    digit = [[lax.rem(p + d, side) * side ** (2 - axis) for d in range(side)] for axis, p in enumerate(at)]
    peers = [digit[0][i] + digit[1][j] + digit[2][k] for i, j, k in steps]

    small = [(x_h, x_v), (ids_h, ids_v), (gpost_h, gpost_v), (gin_h, gin_v), (pos_h, pos_v), (gres_h, gres_v)]
    for i, (src, dst) in enumerate(small):
        pltpu.make_async_copy(src, dst, small_sem.at[i]).start()

    def fetch(src, dst, sem, parts):
        step = dst.shape[0] // parts
        for i in range(parts):
            rows = pl.ds(i * step, step)
            pltpu.make_async_copy(src.at[rows], dst.at[rows], sem).start()

    def arrive(dst, sem):
        pltpu.make_async_copy(dst, dst, sem).wait()

    fetch(wk_h, wk_v, w_sem.at[1], 1)
    fetch(wv_h, wv_v, w_sem.at[2], 1)

    for peer in peers:
        pl.semaphore_signal(barrier, inc=1, device_id={'ep': peer}, device_id_type=MESH)
    pl.semaphore_signal(barrier, inc=1, device_id={'tp': other}, device_id_type=MESH)

    for i, (src, dst) in enumerate(small):
        pltpu.make_async_copy(src, dst, small_sem.at[i]).wait()

    fetch(wq_h, wq_v, w_sem.at[3], 1)

    wide = x_v[...].astype(F32)
    scaled = wide * inv_rms(wide)
    a_v[...] = (scaled * gain_row(gin_v)).astype(BF16)
    moe_in = (scaled * gain_row(gpost_v)).astype(BF16)
    m_v[...] = moe_in
    mine_half = pl.ds(pl.multiple_of(mine * HALF, HALF), HALF)
    other_half = pl.ds(pl.multiple_of(other * HALF, HALF), HALF)

    eye = iota((T, T), 0) == iota((T, T), 1)
    before = iota((T, T), 0) < iota((T, T), 1)

    def to_col(row):
        return jnp.sum(jnp.where(eye, row, 0.0), axis=1, keepdims=True)

    ids = ids_v[...]
    pos_row = pos_v[...].astype(F32)
    pos_col = to_col(pos_row)
    id_rows = [ids[k:k + 1, :].astype(F32) for k in range(2)]
    dest_rows = [jnp.floor(r * (1.0 / EL)) for r in id_rows]
    bit_rows = [r - EL * d for r, d in zip(id_rows, dest_rows)]
    dest_cols = [to_col(d) for d in dest_rows]
    rank0 = jnp.sum(jnp.where((dest_cols[0] == dest_rows[0]) & before, 1.0, 0.0), axis=0, keepdims=True)
    rank1 = (jnp.sum(jnp.where(dest_cols[0] == dest_rows[1], 1.0, 0.0), axis=0, keepdims=True)
             + jnp.sum(jnp.where((dest_cols[1] == dest_rows[1]) & before, 1.0, 0.0), axis=0, keepdims=True))
    slot_rows = [dest_rows[0] * CAP + rank0, dest_rows[1] * CAP + rank1]
    slot_cols = [to_col(s) for s in slot_rows]
    slot_iota = iota((slots, T), 0).astype(F32)
    hot = [jnp.where(slot_iota == s, 1.0, 0.0) for s in slot_rows]
    which = jnp.sum(hot[0] * bit_rows[0] + hot[1] * bit_rows[1], axis=1, keepdims=True)
    sent = jnp.dot((hot[0] + hot[1]).astype(BF16), m_v[:, mine_half], preferred_element_type=F32).astype(BF16)
    ds_v[:, :, :HALF] = sent.reshape(EP, CAP, HALF)
    ds_v[:, :, HALF:] = jnp.broadcast_to(which, (slots, 128)).astype(BF16).reshape(EP, CAP, 128)

    inv_freq = jnp.exp((iota((1, HD), 1) & (HD // 2 - 1)).astype(F32) * (-2.0 / HD * math.log(ROPE_BASE)))
    angles = pos_col * inv_freq
    cosine = jnp.cos(angles)
    sine = jnp.where(iota((1, HD), 1) < HD // 2, -1.0, 1.0) * jnp.sin(angles)

    def rope(head):
        return (head * cosine + pltpu.roll(head, HD // 2, 1) * sine).astype(BF16)

    arrive(wk_v, w_sem.at[1])
    k_proj = jnp.dot(a_v[...], wk_v[...], preferred_element_type=F32)
    k_new = jnp.concatenate([rope(k_proj[:, g * HD:(g + 1) * HD]) for g in range(KV)], axis=0)
    arrive(wv_v, w_sem.at[2])
    v_proj = jnp.dot(a_v[...], wv_v[...], preferred_element_type=F32).astype(BF16)
    v_new = jnp.concatenate([v_proj[:, g * HD:(g + 1) * HD] for g in range(KV)], axis=0)

    fetch(kc_h, kc_v, w_sem.at[4], 1)
    fetch(vc_h, vc_v, w_sem.at[5], 1)
    fetch(wo_h, wo_v, w_sem.at[6], 1)
    fetch(eg_h, eg_v, w_sem.at[7], 1)
    fetch(eu_h, eu_v, w_sem.at[8], 1)
    fetch(ed_h, ed_v, w_sem.at[9], 1)
    blocks = 3 if F % (3 * TILE) == 0 else 1
    ff_cols = [pl.ds(i * (F // blocks), F // blocks) for i in range(blocks)]

    def fetch_gate_up(i):
        for w, (src, dst) in enumerate(((wg_h, wg_v), (wu_h, wu_v))):
            pltpu.make_async_copy(src.at[:, ff_cols[i]], dst.at[:, ff_cols[i]], ff_sem.at[2 * i + w]).start()

    for i in range(min(2, blocks)):
        fetch_gate_up(i)

    pl.semaphore_wait(barrier, EP)

    def exchange(src, dst, sem):
        for peer in peers:
            pltpu.make_async_remote_copy(src_ref=src.at[peer], dst_ref=dst.at[me], send_sem=ep_sem.at[sem], recv_sem=ep_sem.at[sem + 1],
                                         device_id={'ep': peer}, device_id_type=MESH).start()

    exchange(ds_v, dr_v, 0)
    dr_v[me] = ds_v[me]

    arrive(wq_v, w_sem.at[3])
    for i in range(2, blocks):
        fetch_gate_up(i)
    fetch(wr_h, wr_v, w_sem.at[0], 1)

    q_v[...] = jnp.dot(a_v[...], wq_v[...], preferred_element_type=F32)
    half = min(wd_h.shape[0], wq_v.shape[0])
    rest = wd_h.shape[0] - half
    pltpu.make_async_copy(wd_h.at[pl.ds(0, half)], wq_v.at[pl.ds(0, half)], w_sem.at[12]).start()

    arrive(kc_v, w_sem.at[4])
    arrive(vc_v, w_sem.at[5])
    tok_i = iota((T, KV * T), 0)
    lane_j = iota((T, KV * T), 1)
    target = jnp.sum(jnp.where(lax.rem(lane_j, T) == tok_i, (tok_i.astype(F32) * L + pos_col) * KV, 0.0), axis=0, keepdims=True)
    target = target + jnp.floor(iota((1, KV * T), 1).astype(F32) * (1.0 / T))
    new_rows = jnp.concatenate([k_new, v_new, jnp.ones((KV * T, HD), BF16)], axis=1)
    q_heads = [rope(q_v[:, h * HD:(h + 1) * HD]) for h in range(QH)]
    TC = min(16, T)
    width = TC * L * KV
    for c in range(T // TC):
        rows = pl.ds(c * width, width)
        place = jnp.where(iota((width, KV * T), 0).astype(F32) + float(c * width) == target, 1.0, 0.0).astype(BF16)
        placed = jnp.dot(place, new_rows, preferred_element_type=F32)
        hit = placed[:, 2 * HD:] > 0.5
        k_all = jnp.where(hit, placed[:, :HD], kc_v[rows, :].astype(F32)).astype(BF16)
        v_all = jnp.where(hit, placed[:, HD:2 * HD], vc_v[rows, :].astype(F32)).astype(BF16)
        ko_v[rows, :] = k_all
        vo_v[rows, :] = v_all
        q_rows = jnp.concatenate([q[c * TC:(c + 1) * TC] for q in q_heads], axis=0)
        scores = lax.dot_general(q_rows, k_all, (((1,), (1,)), ((), ())), preferred_element_type=F32) * (HD ** -0.5)
        base = lax.rem(iota((QH * TC, 1), 0), TC) * (L * KV)
        pos_rows = jnp.concatenate([pos_col[c * TC:(c + 1) * TC]] * QH, axis=0).astype(jnp.int32)
        last = base + KV * pos_rows + (KV - 1)
        col = iota((1, width), 1)
        attn = []
        for g in range(KV):
            part = slice(g * group * TC, (g + 1) * group * TC)
            own_col = jnp.where(lax.rem(col, KV) == g, col, -1)
            visible = (own_col >= base[part]) & (own_col <= last[part])
            sub = jnp.where(visible, scores[part], -jnp.inf)
            expo = jnp.exp(sub - jnp.max(sub, axis=-1, keepdims=True))
            attn.append((expo * (1.0 / jnp.sum(expo, axis=-1, keepdims=True))).astype(BF16))
        attn = jnp.concatenate(attn, axis=0)
        mixed = jnp.dot(attn, v_all, preferred_element_type=F32).astype(BF16)
        mix_v[c * TC:(c + 1) * TC, :] = jnp.concatenate([mixed[h * TC:(h + 1) * TC] for h in range(QH)], axis=1)
    cache_out = [pltpu.make_async_copy(ko_v, ko_h, out_sem.at[0]), pltpu.make_async_copy(vo_v, vo_h, out_sem.at[1])]
    for copy in cache_out:
        copy.start()

    early, late = entry_order(at, side)
    attn_copy = pltpu.make_async_remote_copy(src_ref=as_v, dst_ref=ar_v, send_sem=tp_sem.at[0], recv_sem=tp_sem.at[1],
                                             device_id={'tp': other}, device_id_type=MESH)

    def project(cols):
        as_v[:, cols] = jnp.dot(mix_v[...], wo_v[:, cols], preferred_element_type=F32).astype(BF16)

    def finish_projection():
        project(pl.ds(HALF, HALF))
        if rest:
            pltpu.make_async_copy(wd_h.at[pl.ds(half, rest)], wo_v.at[pl.ds(0, rest)], w_sem.at[13]).start()
        attn_copy.start()

    def middle():
        attn_copy.wait()
        mid = (x_v[...].astype(F32) + (as_v[...].astype(F32) + ar_v[...].astype(F32))).astype(BF16)
        h_v[...] = mid
        mid = mid.astype(F32)
        c_v[...] = (mid * inv_rms(mid) * gain_row(gres_v)).astype(BF16)

    def gate_up(i):
        cols = ff_cols[i]
        arrive(wg_v.at[:, cols], ff_sem.at[2 * i])
        arrive(wu_v.at[:, cols], ff_sem.at[2 * i + 1])
        gate = jnp.dot(c_v[...], wg_v[:, cols], preferred_element_type=F32)
        up = jnp.dot(c_v[...], wu_v[:, cols], preferred_element_type=F32)
        act_v[:, cols] = silu_mul(gate, up)

    def gate_up_first():
        gate_up(0)

    arrive(wo_v, w_sem.at[6])
    project(pl.ds(0, HALF))

    others = pl.ds(0, EP - 1)
    pltpu.make_async_copy(dr_v.at[others], dr_v.at[others], ep_sem.at[1]).wait()
    rows_copy = pltpu.make_async_remote_copy(src_ref=dr_v, dst_ref=dp_v, send_sem=tp_sem.at[4], recv_sem=tp_sem.at[5],
                                             device_id={'tp': other}, device_id_type=MESH)
    rows_copy.start()

    pl.when(jnp.logical_not(late))(finish_projection)
    arrive(eg_v, w_sem.at[7])
    arrive(eu_v, w_sem.at[8])
    near_v[...] = dr_v[...].reshape(slots, HALF + 128)
    for e in range(EL):
        gu_v[2 * e] = jnp.dot(near_v[:, :HALF], eg_v[e, mine_half, :], preferred_element_type=F32)
        gu_v[2 * e + 1] = jnp.dot(near_v[:, :HALF], eu_v[e, mine_half, :], preferred_element_type=F32)
    rows_copy.wait()
    far_v[...] = dp_v[:, :, :HALF].reshape(slots, HALF)
    for e in range(EL):
        gate = gu_v[2 * e] + jnp.dot(far_v[...], eg_v[e, other_half, :], preferred_element_type=F32)
        up = gu_v[2 * e + 1] + jnp.dot(far_v[...], eu_v[e, other_half, :], preferred_element_type=F32)
        chosen = near_v[:, HALF:HALF + 1].astype(F32) == float(e)
        z_v[:, e * EF:(e + 1) * EF] = jnp.where(chosen, silu_mul(gate, up).astype(F32), 0.0).astype(BF16)
    arrive(ed_v, w_sem.at[9])

    def expert_down(half):
        part = jnp.dot(z_v[:, :EF], ed_v[0, :, half], preferred_element_type=F32)
        for e in range(1, EL):
            part += jnp.dot(z_v[:, e * EF:(e + 1) * EF], ed_v[e, :, half], preferred_element_type=F32)
        return part

    xs_v[...] = expert_down(other_half).astype(BF16)
    sum_copy = pltpu.make_async_remote_copy(src_ref=xs_v, dst_ref=xr_v, send_sem=tp_sem.at[6], recv_sem=tp_sem.at[7],
                                            device_id={'tp': other}, device_id_type=MESH)
    sum_copy.start()
    own_v[...] = expert_down(mine_half)
    pl.when(jnp.logical_not(late))(middle)

    arrive(wr_v, w_sem.at[0])
    logits = jnp.dot(m_v[...], wr_v[...], preferred_element_type=F32)
    expd = jnp.exp(logits - jnp.max(logits, axis=-1, keepdims=True))
    probs = expd / jnp.sum(expd, axis=-1, keepdims=True)
    lane = iota(logits.shape, 1).astype(F32)
    picked = [jnp.sum(jnp.where(lane == to_col(r), probs, 0.0), axis=1, keepdims=True) for r in id_rows]
    total = picked[0] + picked[1]
    weights = [pk / total for pk in picked]
    slot_lane = iota((T, slots), 1).astype(F32)
    take = [jnp.where(slot_lane == s, 1.0, 0.0).astype(BF16) for s in slot_cols]

    pl.when(early)(gate_up_first)
    sum_copy.wait()
    rs_v[...] = (own_v[...] + xr_v[...].astype(F32)).astype(BF16).reshape(EP, CAP, HALF)
    exchange(rs_v, rr_v, 2)
    rr_v[me] = rs_v[me]

    pl.when(late)(finish_projection)
    pl.when(late)(middle)
    pl.when(jnp.logical_not(early))(gate_up_first)
    for i in range(1, blocks):
        gate_up(i)

    arrive(wq_v.at[pl.ds(0, half)], w_sem.at[12])
    if rest:
        arrive(wo_v.at[pl.ds(0, rest)], w_sem.at[13])

    def down(cols):
        part = jnp.dot(act_v[:, :half], wq_v[:half, cols], preferred_element_type=F32)
        if rest:
            part += jnp.dot(act_v[:, half:], wo_v[:rest, cols], preferred_element_type=F32)
        return part

    fs_v[...] = down(other_half).astype(BF16)
    dense_copy = pltpu.make_async_remote_copy(src_ref=fs_v, dst_ref=fr_v, send_sem=tp_sem.at[2], recv_sem=tp_sem.at[3],
                                              device_id={'tp': other}, device_id_type=MESH)
    dense_copy.start()
    den_v[...] = h_v[:, mine_half].astype(F32) + down(mine_half)

    pltpu.make_async_copy(rr_v.at[others], rr_v.at[others], ep_sem.at[3]).wait()
    ret_v[...] = rr_v[...].reshape(slots, HALF)
    moe = weights[0] * jnp.dot(take[0], ret_v[...], preferred_element_type=F32)
    moe += weights[1] * jnp.dot(take[1], ret_v[...], preferred_element_type=F32)
    dense_copy.wait()
    out_v[...] = (den_v[...] + fr_v[...].astype(F32) + moe).astype(BF16)
    last_copy = pltpu.make_async_remote_copy(src_ref=out_v, dst_ref=out_h.at[mine], send_sem=tp_sem.at[8], recv_sem=tp_sem.at[9],
                                             device_id={'tp': other}, device_id_type=MESH)
    last_copy.start()
    done = pltpu.make_async_copy(out_v, out_h.at[mine], out_sem.at[2])
    done.start()
    for sem, ref in ((0, ds_v), (2, rs_v)):
        pltpu.make_async_copy(ref.at[others], ref.at[others], ep_sem.at[sem]).wait()
    for copy in cache_out:
        copy.wait()
    last_copy.wait()
    done.wait()


def settle_kernel(half_h, ki_h, vi_h, out_h, ko_h, vo_h, out_v, k_v, v_v, sem):
    T, D = out_v.shape
    cols = [pl.ds(0, D // 2), pl.ds(D // 2, D // 2)]
    halves = [pltpu.make_async_copy(half_h.at[i], out_v.at[:, c], sem.at[i]) for i, c in enumerate(cols)]
    loads = [pltpu.make_async_copy(ki_h, k_v, sem.at[2]), pltpu.make_async_copy(vi_h, v_v, sem.at[3])]
    stores = [pltpu.make_async_copy(k_v, ko_h, sem.at[4]), pltpu.make_async_copy(v_v, vo_h, sem.at[5])]
    last = pltpu.make_async_copy(out_v, out_h, sem.at[6])
    for copy in loads + halves:
        copy.start()
    for load, store in zip(loads, stores):
        load.wait()
        store.start()
    for copy in halves:
        copy.wait()
    last.start()
    for copy in stores + [last]:
        copy.wait()


def settle(halves, k_rows, v_rows):
    hbm = pl.BlockSpec(memory_space=pl.ANY)
    T, D = halves.shape[1], 2 * halves.shape[2]
    shapes = ((T, D), k_rows.shape, v_rows.shape)
    return pl.pallas_call(
        settle_kernel,
        out_shape=tuple(jax.ShapeDtypeStruct(s, BF16) for s in shapes),
        in_specs=[hbm] * 3,
        out_specs=(hbm,) * 3,
        scratch_shapes=[pltpu.VMEM(s, BF16) for s in shapes] + [pltpu.SemaphoreType.DMA((7,))],
        compiler_params=pltpu.CompilerParams(vmem_limit_bytes=67043328),
        name='settle',
    )(halves, k_rows, v_rows)


def solution(mesh):
    EP = mesh.shape['ep']
    row_spec = P(('dp', 'ep'), None)
    cache_spec = P(('dp', 'ep'), None, 'tp', None)
    col_split = P(None, 'tp')
    row_split = P('tp', None)
    in_specs = (row_spec, P(('dp', 'ep')), row_spec, cache_spec, cache_spec, P(None), P(None), P(None), col_split, col_split, col_split, row_split, col_split, col_split, row_split, P(None, None), P('ep', None, 'tp'), P('ep', None, 'tp'), P('ep', 'tp', None))
    out_specs = (row_spec, cache_spec, cache_spec)

    def local_layer(hidden_in, positions, expert_ids, k_cache, v_cache, norm_in, norm_res, norm_post, w_q, w_k, w_v, w_o, w_gate, w_up, w_down, w_router, e_gate, e_up, e_down):
        T, D = hidden_in.shape
        _, L, KV, HD = k_cache.shape
        QH = w_q.shape[1] // HD
        F = w_gate.shape[1]
        EL, _, EF = e_gate.shape
        CAP = 4 * T // EP
        dims = (T, D, L, KV, HD, QH, F, EL, EF, EP, CAP, 512)
        slots = EP * CAP
        HALF = D // 2
        cache_rows = (T * L * KV, HD)
        args = (hidden_in, positions.reshape(1, T), expert_ids.T, k_cache.reshape(cache_rows), v_cache.reshape(cache_rows),
                norm_in.reshape(D // 128, 128), norm_res.reshape(D // 128, 128), norm_post.reshape(D // 128, 128),
                w_q, w_k, w_v, w_o, w_gate, w_up, w_down, w_router, e_gate, e_up, e_down)
        mirror = [pltpu.VMEM(a.shape, a.dtype) for i, a in enumerate(args) if i != 14]
        work = [
            pltpu.VMEM(cache_rows, BF16), pltpu.VMEM(cache_rows, BF16),
            pltpu.VMEM((T, D), BF16), pltpu.VMEM((T, D), BF16), pltpu.VMEM((T, QH * HD), F32), pltpu.VMEM((T, QH * HD), BF16),
            pltpu.VMEM((T, D), BF16), pltpu.VMEM((T, D), BF16), pltpu.VMEM((T, D), BF16), pltpu.VMEM((T, D), BF16),
            pltpu.VMEM((T, F), BF16), pltpu.VMEM((T, HALF), F32),
            pltpu.VMEM((EP, CAP, HALF + 128), BF16), pltpu.VMEM((EP, CAP, HALF + 128), BF16), pltpu.VMEM((EP, CAP, HALF + 128), BF16),
            pltpu.VMEM((slots, HALF + 128), BF16), pltpu.VMEM((slots, HALF), BF16), pltpu.VMEM((2 * EL, slots, EF), F32),
            pltpu.VMEM((slots, EL * EF), BF16), pltpu.VMEM((slots, HALF), BF16), pltpu.VMEM((slots, HALF), BF16), pltpu.VMEM((slots, HALF), F32),
            pltpu.VMEM((EP, CAP, HALF), BF16), pltpu.VMEM((EP, CAP, HALF), BF16), pltpu.VMEM((slots, HALF), BF16),
            pltpu.VMEM((T, HALF), BF16), pltpu.VMEM((T, HALF), BF16), pltpu.VMEM((T, HALF), BF16),
            pltpu.SemaphoreType.DMA((6,)), pltpu.SemaphoreType.DMA((14,)), pltpu.SemaphoreType.DMA((6,)), pltpu.SemaphoreType.DMA((3,)),
            pltpu.SemaphoreType.DMA((10,)), pltpu.SemaphoreType.DMA((4,)),
        ]
        hbm = pl.BlockSpec(memory_space=pl.ANY)
        out, k_out, v_out = pl.pallas_call(
            functools.partial(layer_kernel, dims),
            out_shape=(jax.ShapeDtypeStruct((2, T, HALF), BF16), jax.ShapeDtypeStruct(cache_rows, BF16), jax.ShapeDtypeStruct(cache_rows, BF16)),
            in_specs=[hbm] * len(args),
            out_specs=(hbm, hbm, hbm),
            scratch_shapes=mirror + work,
            compiler_params=pltpu.CompilerParams(collective_id=0, has_side_effects=True, vmem_limit_bytes=67043328),
            name='layer',
        )(*args)
        out, k_out, v_out = settle(out, k_out, v_out)
        return out, k_out.reshape(k_cache.shape), v_out.reshape(v_cache.shape)

    return jax.shard_map(local_layer, mesh=mesh, in_specs=in_specs, out_specs=out_specs, check_vma=False)
```

```python
import functools
import math
import random

import jax
import jax.numpy as jnp
from jax import lax
from jax.experimental import pallas as pl
from jax.experimental.pallas import tpu as pltpu
from jax.sharding import PartitionSpec as P

NORM_EPS = 1e-5
ROPE_BASE = 10000.0
MESH = pl.DeviceIdType.MESH
F32 = jnp.float32
BF16 = jnp.bfloat16


def iota(shape, axis):
    return lax.broadcasted_iota(jnp.int32, shape, axis)


def peer_steps(n):
    side = round(n ** (1 / 3))
    if side ** 3 != n:
        return n, [(0, 0, i) for i in range(1, n)]
    steps = [(a, b, c) for a in range(side) for b in range(side) for c in range(side)][1:]
    random.Random(1).shuffle(steps)
    return side, sorted(steps, key=lambda s: -sum(min(d, side - d) for d in s))


def entry_order(at, side):
    if side != 4:
        return at[2] < 0, at[2] < 0
    cost = 0
    for place, table in zip(at, ((0, 8, 17, 23), (0, 5, 10, 13), (0, 4, 9, 11))):
        for i in range(1, 4):
            cost = cost + jnp.where(place == i, table[i], 0)
    return cost <= 12, cost >= 30


def gain_row(ref):
    tile = ref[...].astype(F32)
    return jnp.concatenate([tile[i:i + 1, :] for i in range(tile.shape[0])], axis=1)


def inv_rms(wide):
    return lax.rsqrt(jnp.mean(wide * wide, axis=-1, keepdims=True) + NORM_EPS)


def silu_mul(gate, up):
    return ((gate * jax.nn.sigmoid(gate)) * up).astype(BF16)


def layer_kernel(dims, x_h, pos_h, ids_h, kc_h, vc_h, gin_h, gres_h, gpost_h, wq_h, wk_h, wv_h, wo_h, wg_h, wu_h, wd_h, wr_h,
                 eg_h, eu_h, ed_h, out_h, ko_h, vo_h,
                 x_v, pos_v, ids_v, kc_v, vc_v, gin_v, gres_v, gpost_v, wq_v, wk_v, wv_v, wo_v, wg_v, wu_v, wr_v,
                 eg_v, eu_v, ed_v, ko_v, vo_v, a_v, m_v, q_v, mix_v, as_v, ar_v, h_v, c_v, act_v, den_v,
                 ds_v, dr_v, dp_v, near_v, far_v, gu_v, z_v, xs_v, xr_v, own_v, rs_v, rr_v, ret_v, fs_v, fr_v, out_v,
                 small_sem, w_sem, ff_sem, out_sem, tp_sem, ep_sem):
    T, D, L, KV, HD, QH, F, EL, EF, EP, CAP, TILE = dims
    group = QH // KV
    slots = EP * CAP
    me = lax.axis_index('ep')
    mine = lax.axis_index('tp')
    other = 1 - mine
    HALF = D // 2

    barrier = pltpu.get_barrier_semaphore()

    side, steps = peer_steps(EP)
    at = (lax.div(me, side * side), lax.rem(lax.div(me, side), side), lax.rem(me, side))
    digit = [[lax.rem(p + d, side) * side ** (2 - axis) for d in range(side)] for axis, p in enumerate(at)]
    peers = [digit[0][i] + digit[1][j] + digit[2][k] for i, j, k in steps]

    small = [(x_h, x_v), (ids_h, ids_v), (gpost_h, gpost_v), (gin_h, gin_v), (pos_h, pos_v), (gres_h, gres_v)]
    for i, (src, dst) in enumerate(small):
        pltpu.make_async_copy(src, dst, small_sem.at[i]).start()

    def fetch(src, dst, sem, parts):
        step = dst.shape[0] // parts
        for i in range(parts):
            rows = pl.ds(i * step, step)
            pltpu.make_async_copy(src.at[rows], dst.at[rows], sem).start()

    def arrive(dst, sem):
        pltpu.make_async_copy(dst, dst, sem).wait()

    fetch(wk_h, wk_v, w_sem.at[1], 1)
    fetch(wv_h, wv_v, w_sem.at[2], 1)

    for peer in peers:
        pl.semaphore_signal(barrier, inc=1, device_id={'ep': peer}, device_id_type=MESH)
    pl.semaphore_signal(barrier, inc=1, device_id={'tp': other}, device_id_type=MESH)

    for i, (src, dst) in enumerate(small):
        pltpu.make_async_copy(src, dst, small_sem.at[i]).wait()

    fetch(wq_h, wq_v, w_sem.at[3], 2)

    wide = x_v[...].astype(F32)
    scaled = wide * inv_rms(wide)
    a_v[...] = (scaled * gain_row(gin_v)).astype(BF16)
    moe_in = (scaled * gain_row(gpost_v)).astype(BF16)
    m_v[...] = moe_in
    mine_half = pl.ds(pl.multiple_of(mine * HALF, HALF), HALF)
    other_half = pl.ds(pl.multiple_of(other * HALF, HALF), HALF)

    eye = iota((T, T), 0) == iota((T, T), 1)
    before = iota((T, T), 0) < iota((T, T), 1)

    def to_col(row):
        return jnp.sum(jnp.where(eye, row, 0.0), axis=1, keepdims=True)

    ids = ids_v[...]
    pos_row = pos_v[...].astype(F32)
    pos_col = to_col(pos_row)
    id_rows = [ids[k:k + 1, :].astype(F32) for k in range(2)]
    dest_rows = [jnp.floor(r * (1.0 / EL)) for r in id_rows]
    bit_rows = [r - EL * d for r, d in zip(id_rows, dest_rows)]
    dest_cols = [to_col(d) for d in dest_rows]
    rank0 = jnp.sum(jnp.where((dest_cols[0] == dest_rows[0]) & before, 1.0, 0.0), axis=0, keepdims=True)
    rank1 = (jnp.sum(jnp.where(dest_cols[0] == dest_rows[1], 1.0, 0.0), axis=0, keepdims=True)
             + jnp.sum(jnp.where((dest_cols[1] == dest_rows[1]) & before, 1.0, 0.0), axis=0, keepdims=True))
    slot_rows = [dest_rows[0] * CAP + rank0, dest_rows[1] * CAP + rank1]
    slot_cols = [to_col(s) for s in slot_rows]
    slot_iota = iota((slots, T), 0).astype(F32)
    hot = [jnp.where(slot_iota == s, 1.0, 0.0) for s in slot_rows]
    which = jnp.sum(hot[0] * bit_rows[0] + hot[1] * bit_rows[1], axis=1, keepdims=True)
    sent = jnp.dot((hot[0] + hot[1]).astype(BF16), m_v[:, mine_half], preferred_element_type=F32).astype(BF16)
    ds_v[:, :, :HALF] = sent.reshape(EP, CAP, HALF)
    ds_v[:, :, HALF:] = jnp.broadcast_to(which, (slots, 128)).astype(BF16).reshape(EP, CAP, 128)

    inv_freq = jnp.exp((iota((1, HD), 1) & (HD // 2 - 1)).astype(F32) * (-2.0 / HD * math.log(ROPE_BASE)))
    angles = pos_col * inv_freq
    cosine = jnp.cos(angles)
    sine = jnp.where(iota((1, HD), 1) < HD // 2, -1.0, 1.0) * jnp.sin(angles)

    def rope(head):
        return (head * cosine + pltpu.roll(head, HD // 2, 1) * sine).astype(BF16)

    arrive(wk_v, w_sem.at[1])
    k_proj = jnp.dot(a_v[...], wk_v[...], preferred_element_type=F32)
    k_new = jnp.concatenate([rope(k_proj[:, g * HD:(g + 1) * HD]) for g in range(KV)], axis=0)
    arrive(wv_v, w_sem.at[2])
    v_proj = jnp.dot(a_v[...], wv_v[...], preferred_element_type=F32).astype(BF16)
    v_new = jnp.concatenate([v_proj[:, g * HD:(g + 1) * HD] for g in range(KV)], axis=0)

    fetch(kc_h, kc_v, w_sem.at[4], 1)
    fetch(vc_h, vc_v, w_sem.at[5], 1)
    fetch(wo_h, wo_v, w_sem.at[6], 2)

    early, late = entry_order(at, side)
    blocks = 3 if F % (3 * TILE) == 0 else 1
    ff_cols = [pl.ds(i * (F // blocks), F // blocks) for i in range(blocks)]

    def stream_ahead():
        arrive(wq_v, w_sem.at[3])
        fetch(eg_h, eg_v, w_sem.at[7], 1)
        fetch(eu_h, eu_v, w_sem.at[8], 1)
        fetch(ed_h, ed_v, w_sem.at[9], 1)
        fetch(wr_h, wr_v, w_sem.at[0], 1)
        for i, cols in enumerate(ff_cols):
            pltpu.make_async_copy(wg_h.at[:, cols], wg_v.at[:, cols], ff_sem.at[2 * i]).start()
            pltpu.make_async_copy(wu_h.at[:, cols], wu_v.at[:, cols], ff_sem.at[2 * i + 1]).start()

    pl.when(jnp.logical_not(late))(stream_ahead)

    pl.semaphore_wait(barrier, EP)

    def exchange(src, dst, sem):
        for peer in peers:
            pltpu.make_async_remote_copy(src_ref=src.at[peer], dst_ref=dst.at[me], send_sem=ep_sem.at[sem], recv_sem=ep_sem.at[sem + 1],
                                         device_id={'ep': peer}, device_id_type=MESH).start()

    exchange(ds_v, dr_v, 0)
    dr_v[me] = ds_v[me]
    pl.when(late)(stream_ahead)


    q_v[...] = jnp.dot(a_v[...], wq_v[...], preferred_element_type=F32)
    half = min(wd_h.shape[0], wq_v.shape[0])
    rest = wd_h.shape[0] - half
    pltpu.make_async_copy(wd_h.at[pl.ds(0, half)], wq_v.at[pl.ds(0, half)], w_sem.at[12]).start()

    arrive(kc_v, w_sem.at[4])
    arrive(vc_v, w_sem.at[5])
    tok_i = iota((T, KV * T), 0)
    lane_j = iota((T, KV * T), 1)
    target = jnp.sum(jnp.where(lax.rem(lane_j, T) == tok_i, (tok_i.astype(F32) * L + pos_col) * KV, 0.0), axis=0, keepdims=True)
    target = target + jnp.floor(iota((1, KV * T), 1).astype(F32) * (1.0 / T))
    new_rows = jnp.concatenate([k_new, v_new, jnp.ones((KV * T, HD), BF16)], axis=1)
    q_heads = [rope(q_v[:, h * HD:(h + 1) * HD]) for h in range(QH)]
    TC = min(16, T)
    width = TC * L * KV
    for c in range(T // TC):
        rows = pl.ds(c * width, width)
        place = jnp.where(iota((width, KV * T), 0).astype(F32) + float(c * width) == target, 1.0, 0.0).astype(BF16)
        placed = jnp.dot(place, new_rows, preferred_element_type=F32)
        hit = placed[:, 2 * HD:] > 0.5
        k_all = jnp.where(hit, placed[:, :HD], kc_v[rows, :].astype(F32)).astype(BF16)
        v_all = jnp.where(hit, placed[:, HD:2 * HD], vc_v[rows, :].astype(F32)).astype(BF16)
        ko_v[rows, :] = k_all
        vo_v[rows, :] = v_all
        q_rows = jnp.concatenate([q[c * TC:(c + 1) * TC] for q in q_heads], axis=0)
        scores = lax.dot_general(q_rows, k_all, (((1,), (1,)), ((), ())), preferred_element_type=F32) * (HD ** -0.5)
        base = lax.rem(iota((QH * TC, 1), 0), TC) * (L * KV)
        pos_rows = jnp.concatenate([pos_col[c * TC:(c + 1) * TC]] * QH, axis=0).astype(jnp.int32)
        last = base + KV * pos_rows + (KV - 1)
        col = iota((1, width), 1)
        attn = []
        for g in range(KV):
            part = slice(g * group * TC, (g + 1) * group * TC)
            own_col = jnp.where(lax.rem(col, KV) == g, col, -1)
            visible = (own_col >= base[part]) & (own_col <= last[part])
            sub = jnp.where(visible, scores[part], -jnp.inf)
            expo = jnp.exp(sub - jnp.max(sub, axis=-1, keepdims=True))
            attn.append((expo * (1.0 / jnp.sum(expo, axis=-1, keepdims=True))).astype(BF16))
        attn = jnp.concatenate(attn, axis=0)
        mixed = jnp.dot(attn, v_all, preferred_element_type=F32).astype(BF16)
        mix_v[c * TC:(c + 1) * TC, :] = jnp.concatenate([mixed[h * TC:(h + 1) * TC] for h in range(QH)], axis=1)
    cache_out = [pltpu.make_async_copy(ko_v, ko_h, out_sem.at[0]), pltpu.make_async_copy(vo_v, vo_h, out_sem.at[1])]
    for copy in cache_out:
        copy.start()

    attn_copy = pltpu.make_async_remote_copy(src_ref=as_v, dst_ref=ar_v, send_sem=tp_sem.at[0], recv_sem=tp_sem.at[1],
                                             device_id={'tp': other}, device_id_type=MESH)

    def project(cols):
        as_v[:, cols] = jnp.dot(mix_v[...], wo_v[:, cols], preferred_element_type=F32).astype(BF16)

    def finish_projection():
        project(pl.ds(HALF, HALF))
        if rest:
            pltpu.make_async_copy(wd_h.at[pl.ds(half, rest)], wo_v.at[pl.ds(0, rest)], w_sem.at[13]).start()
        attn_copy.start()

    def middle():
        attn_copy.wait()
        mid = (x_v[...].astype(F32) + (as_v[...].astype(F32) + ar_v[...].astype(F32))).astype(BF16)
        h_v[...] = mid
        mid = mid.astype(F32)
        c_v[...] = (mid * inv_rms(mid) * gain_row(gres_v)).astype(BF16)

    def gate_up(i):
        cols = ff_cols[i]
        arrive(wg_v.at[:, cols], ff_sem.at[2 * i])
        arrive(wu_v.at[:, cols], ff_sem.at[2 * i + 1])
        gate = jnp.dot(c_v[...], wg_v[:, cols], preferred_element_type=F32)
        up = jnp.dot(c_v[...], wu_v[:, cols], preferred_element_type=F32)
        act_v[:, cols] = silu_mul(gate, up)

    def gate_up_first():
        gate_up(0)

    arrive(wo_v, w_sem.at[6])
    project(pl.ds(0, HALF))

    others = pl.ds(0, EP - 1)
    pltpu.make_async_copy(dr_v.at[others], dr_v.at[others], ep_sem.at[1]).wait()
    rows_copy = pltpu.make_async_remote_copy(src_ref=dr_v, dst_ref=dp_v, send_sem=tp_sem.at[4], recv_sem=tp_sem.at[5],
                                             device_id={'tp': other}, device_id_type=MESH)
    rows_copy.start()

    pl.when(jnp.logical_not(late))(finish_projection)
    arrive(eg_v, w_sem.at[7])
    arrive(eu_v, w_sem.at[8])
    near_v[...] = dr_v[...].reshape(slots, HALF + 128)
    for e in range(EL):
        gu_v[2 * e] = jnp.dot(near_v[:, :HALF], eg_v[e, mine_half, :], preferred_element_type=F32)
        gu_v[2 * e + 1] = jnp.dot(near_v[:, :HALF], eu_v[e, mine_half, :], preferred_element_type=F32)
    rows_copy.wait()
    far_v[...] = dp_v[:, :, :HALF].reshape(slots, HALF)
    for e in range(EL):
        gate = gu_v[2 * e] + jnp.dot(far_v[...], eg_v[e, other_half, :], preferred_element_type=F32)
        up = gu_v[2 * e + 1] + jnp.dot(far_v[...], eu_v[e, other_half, :], preferred_element_type=F32)
        chosen = near_v[:, HALF:HALF + 1].astype(F32) == float(e)
        z_v[:, e * EF:(e + 1) * EF] = jnp.where(chosen, silu_mul(gate, up).astype(F32), 0.0).astype(BF16)
    arrive(ed_v, w_sem.at[9])

    def expert_down(half):
        part = jnp.dot(z_v[:, :EF], ed_v[0, :, half], preferred_element_type=F32)
        for e in range(1, EL):
            part += jnp.dot(z_v[:, e * EF:(e + 1) * EF], ed_v[e, :, half], preferred_element_type=F32)
        return part

    xs_v[...] = expert_down(other_half).astype(BF16)
    sum_copy = pltpu.make_async_remote_copy(src_ref=xs_v, dst_ref=xr_v, send_sem=tp_sem.at[6], recv_sem=tp_sem.at[7],
                                            device_id={'tp': other}, device_id_type=MESH)
    sum_copy.start()
    own_v[...] = expert_down(mine_half)
    pl.when(jnp.logical_not(late))(middle)

    arrive(wr_v, w_sem.at[0])
    logits = jnp.dot(m_v[...], wr_v[...], preferred_element_type=F32)
    expd = jnp.exp(logits - jnp.max(logits, axis=-1, keepdims=True))
    probs = expd / jnp.sum(expd, axis=-1, keepdims=True)
    lane = iota(logits.shape, 1).astype(F32)
    picked = [jnp.sum(jnp.where(lane == to_col(r), probs, 0.0), axis=1, keepdims=True) for r in id_rows]
    total = picked[0] + picked[1]
    weights = [pk / total for pk in picked]
    slot_lane = iota((T, slots), 1).astype(F32)
    take = [jnp.where(slot_lane == s, 1.0, 0.0).astype(BF16) for s in slot_cols]

    pl.when(early)(gate_up_first)
    sum_copy.wait()
    rs_v[...] = (own_v[...] + xr_v[...].astype(F32)).astype(BF16).reshape(EP, CAP, HALF)
    exchange(rs_v, rr_v, 2)
    rr_v[me] = rs_v[me]

    pl.when(late)(finish_projection)
    pl.when(late)(middle)
    pl.when(jnp.logical_not(early))(gate_up_first)
    for i in range(1, blocks):
        gate_up(i)

    arrive(wq_v.at[pl.ds(0, half)], w_sem.at[12])
    if rest:
        arrive(wo_v.at[pl.ds(0, rest)], w_sem.at[13])

    def down(cols):
        part = jnp.dot(act_v[:, :half], wq_v[:half, cols], preferred_element_type=F32)
        if rest:
            part += jnp.dot(act_v[:, half:], wo_v[:rest, cols], preferred_element_type=F32)
        return part

    fs_v[...] = down(other_half).astype(BF16)
    dense_copy = pltpu.make_async_remote_copy(src_ref=fs_v, dst_ref=fr_v, send_sem=tp_sem.at[2], recv_sem=tp_sem.at[3],
                                              device_id={'tp': other}, device_id_type=MESH)
    dense_copy.start()
    den_v[...] = h_v[:, mine_half].astype(F32) + down(mine_half)

    pltpu.make_async_copy(rr_v.at[others], rr_v.at[others], ep_sem.at[3]).wait()
    ret_v[...] = rr_v[...].reshape(slots, HALF)
    moe = weights[0] * jnp.dot(take[0], ret_v[...], preferred_element_type=F32)
    moe += weights[1] * jnp.dot(take[1], ret_v[...], preferred_element_type=F32)
    dense_copy.wait()
    out_v[...] = (den_v[...] + fr_v[...].astype(F32) + moe).astype(BF16)
    last_copy = pltpu.make_async_remote_copy(src_ref=out_v, dst_ref=out_h.at[mine], send_sem=tp_sem.at[8], recv_sem=tp_sem.at[9],
                                             device_id={'tp': other}, device_id_type=MESH)
    last_copy.start()
    done = pltpu.make_async_copy(out_v, out_h.at[mine], out_sem.at[2])
    done.start()
    for sem, ref in ((0, ds_v), (2, rs_v)):
        pltpu.make_async_copy(ref.at[others], ref.at[others], ep_sem.at[sem]).wait()
    for copy in cache_out:
        copy.wait()
    last_copy.wait()
    done.wait()


def settle_kernel(half_h, ki_h, vi_h, out_h, ko_h, vo_h, out_v, k_v, v_v, sem):
    T, D = out_v.shape
    cols = [pl.ds(0, D // 2), pl.ds(D // 2, D // 2)]
    halves = [pltpu.make_async_copy(half_h.at[i], out_v.at[:, c], sem.at[i]) for i, c in enumerate(cols)]
    loads = [pltpu.make_async_copy(ki_h, k_v, sem.at[2]), pltpu.make_async_copy(vi_h, v_v, sem.at[3])]
    stores = [pltpu.make_async_copy(k_v, ko_h, sem.at[4]), pltpu.make_async_copy(v_v, vo_h, sem.at[5])]
    last = pltpu.make_async_copy(out_v, out_h, sem.at[6])
    for copy in loads + halves:
        copy.start()
    for load, store in zip(loads, stores):
        load.wait()
        store.start()
    for copy in halves:
        copy.wait()
    last.start()
    for copy in stores + [last]:
        copy.wait()


def settle(halves, k_rows, v_rows):
    hbm = pl.BlockSpec(memory_space=pl.ANY)
    T, D = halves.shape[1], 2 * halves.shape[2]
    shapes = ((T, D), k_rows.shape, v_rows.shape)
    return pl.pallas_call(
        settle_kernel,
        out_shape=tuple(jax.ShapeDtypeStruct(s, BF16) for s in shapes),
        in_specs=[hbm] * 3,
        out_specs=(hbm,) * 3,
        scratch_shapes=[pltpu.VMEM(s, BF16) for s in shapes] + [pltpu.SemaphoreType.DMA((7,))],
        compiler_params=pltpu.CompilerParams(vmem_limit_bytes=67043328),
        name='settle',
    )(halves, k_rows, v_rows)


def solution(mesh):
    EP = mesh.shape['ep']
    row_spec = P(('dp', 'ep'), None)
    cache_spec = P(('dp', 'ep'), None, 'tp', None)
    col_split = P(None, 'tp')
    row_split = P('tp', None)
    in_specs = (row_spec, P(('dp', 'ep')), row_spec, cache_spec, cache_spec, P(None), P(None), P(None), col_split, col_split, col_split, row_split, col_split, col_split, row_split, P(None, None), P('ep', None, 'tp'), P('ep', None, 'tp'), P('ep', 'tp', None))
    out_specs = (row_spec, cache_spec, cache_spec)

    def local_layer(hidden_in, positions, expert_ids, k_cache, v_cache, norm_in, norm_res, norm_post, w_q, w_k, w_v, w_o, w_gate, w_up, w_down, w_router, e_gate, e_up, e_down):
        T, D = hidden_in.shape
        _, L, KV, HD = k_cache.shape
        QH = w_q.shape[1] // HD
        F = w_gate.shape[1]
        EL, _, EF = e_gate.shape
        CAP = 4 * T // EP
        dims = (T, D, L, KV, HD, QH, F, EL, EF, EP, CAP, 512)
        slots = EP * CAP
        HALF = D // 2
        cache_rows = (T * L * KV, HD)
        args = (hidden_in, positions.reshape(1, T), expert_ids.T, k_cache.reshape(cache_rows), v_cache.reshape(cache_rows),
                norm_in.reshape(D // 128, 128), norm_res.reshape(D // 128, 128), norm_post.reshape(D // 128, 128),
                w_q, w_k, w_v, w_o, w_gate, w_up, w_down, w_router, e_gate, e_up, e_down)
        mirror = [pltpu.VMEM(a.shape, a.dtype) for i, a in enumerate(args) if i != 14]
        work = [
            pltpu.VMEM(cache_rows, BF16), pltpu.VMEM(cache_rows, BF16),
            pltpu.VMEM((T, D), BF16), pltpu.VMEM((T, D), BF16), pltpu.VMEM((T, QH * HD), F32), pltpu.VMEM((T, QH * HD), BF16),
            pltpu.VMEM((T, D), BF16), pltpu.VMEM((T, D), BF16), pltpu.VMEM((T, D), BF16), pltpu.VMEM((T, D), BF16),
            pltpu.VMEM((T, F), BF16), pltpu.VMEM((T, HALF), F32),
            pltpu.VMEM((EP, CAP, HALF + 128), BF16), pltpu.VMEM((EP, CAP, HALF + 128), BF16), pltpu.VMEM((EP, CAP, HALF + 128), BF16),
            pltpu.VMEM((slots, HALF + 128), BF16), pltpu.VMEM((slots, HALF), BF16), pltpu.VMEM((2 * EL, slots, EF), F32),
            pltpu.VMEM((slots, EL * EF), BF16), pltpu.VMEM((slots, HALF), BF16), pltpu.VMEM((slots, HALF), BF16), pltpu.VMEM((slots, HALF), F32),
            pltpu.VMEM((EP, CAP, HALF), BF16), pltpu.VMEM((EP, CAP, HALF), BF16), pltpu.VMEM((slots, HALF), BF16),
            pltpu.VMEM((T, HALF), BF16), pltpu.VMEM((T, HALF), BF16), pltpu.VMEM((T, HALF), BF16),
            pltpu.SemaphoreType.DMA((6,)), pltpu.SemaphoreType.DMA((14,)), pltpu.SemaphoreType.DMA((6,)), pltpu.SemaphoreType.DMA((3,)),
            pltpu.SemaphoreType.DMA((10,)), pltpu.SemaphoreType.DMA((4,)),
        ]
        hbm = pl.BlockSpec(memory_space=pl.ANY)
        out, k_out, v_out = pl.pallas_call(
            functools.partial(layer_kernel, dims),
            out_shape=(jax.ShapeDtypeStruct((2, T, HALF), BF16), jax.ShapeDtypeStruct(cache_rows, BF16), jax.ShapeDtypeStruct(cache_rows, BF16)),
            in_specs=[hbm] * len(args),
            out_specs=(hbm, hbm, hbm),
            scratch_shapes=mirror + work,
            compiler_params=pltpu.CompilerParams(collective_id=0, has_side_effects=True, vmem_limit_bytes=67043328),
            name='layer',
        )(*args)
        out, k_out, v_out = settle(out, k_out, v_out)
        return out, k_out.reshape(k_cache.shape), v_out.reshape(v_cache.shape)

    return jax.shard_map(local_layer, mesh=mesh, in_specs=in_specs, out_specs=out_specs, check_vma=False)
```
